32 devices in a mesh: ep: 4 (over z), tp: 8 (over y, x, core).
Axes of the slice: x: 2, y: 2, z: 4, core: 2. Of those that a mesh axis runs over, the one named last changes fastest.
Arguments:
- tokens: bfloat16 [384, 3072], P('ep', 'tp'), may hold values from -6 to 6
- cotangent: bfloat16 [384, 3072], P('ep', 'tp'), may hold values from -6 to 6
- expert_ids: int32 [384, 2], P('ep'), may hold values from 0 to 3, all different within a row; in each aligned block of 96 rows (0 to 95, 96 to 191, ...) at most 80 rows name the same one
- combine_weights: float32 [384, 2], P('ep'), may hold values from 0.1 to 1
- w_gate: bfloat16 [4, 3072, 8192], P('ep', None, 'tp'), may hold values from -0.15625 to 0.15625
- w_up: bfloat16 [4, 3072, 8192], P('ep', None, 'tp'), may hold values from -0.109375 to 0.109375
- w_down: bfloat16 [4, 8192, 3072], P('ep', 'tp'), may hold values from -0.09375 to 0.09375
Outputs:
- mixed: bfloat16 [384, 3072], P('ep', 'tp')
- grad_tokens: bfloat16 [384, 3072], P('ep', 'tp')
- grad_combine: float32 [384, 2], P('ep')
- grad_gate: bfloat16 [4, 3072, 8192], P('ep', 'tp')
- grad_up: bfloat16 [4, 3072, 8192], P('ep', 'tp')
- grad_down: bfloat16 [4, 8192, 3072], P('ep', None, 'tp')
The draws below stay inside these ranges and needn't reach their ends.
Inputs may be any that keep to these rules, and one draw needn't show every extreme that they name: `expert_ids`: each row names 2 different experts. Among the 96 rows of one index of ep, no expert is named more than 80 times, and in some such blocks one expert is named exactly 80 times.
All inputs are finite; a program needn't handle non-finite values.
Results may differ from the reference program's by a relative error of at most 0.019.
Values may be sent and summed in bfloat16 or wider, within the bound.
A program may use at most 128 MiB of HBM per device.

```python
import math
import jax
import jax.numpy as jnp
import numpy as np
from jax import lax

D = 3072
FF = 8192
TOP = 2
TOK_EP = 96
EXPERTS = 4
CAP = 80
TOKENS = 384
N_EP = 4
N_TP = 8


def with_spikes(drawn, stream_key, source, target, parts, factor):
    def block_of(axis_at):
        return (jnp.arange(drawn.shape[axis_at]) // (drawn.shape[axis_at] // parts)).reshape((-1,) + (1,) * (drawn.ndim - 1 - axis_at))

    first = jax.random.permutation(stream_key, parts)[block_of(target)]
    other_side = (block_of(target) + parts // 2) % parts
    return jnp.where((block_of(source) == first) | (block_of(source) == other_side), factor * drawn, drawn)


def level_of(stream_key, shape, shards, least, largest):
    def one(position, parts):
        draws = jax.random.uniform(jax.random.fold_in(jax.random.fold_in(stream_key, 6), position), (parts,), jnp.float32, least / len(shards), largest / len(shards))
        return jnp.repeat(jnp.exp(draws), shape[position] // parts).reshape((-1,) + (1,) * (len(shape) - position - 1))

    loudness = one(*shards[0])
    for cut in shards[1:]:
        loudness = loudness * one(*cut)
    return loudness


def assign_block(key, own, number, rows, amount, top, most, skew):
    ranking = jax.random.permutation(key, amount)
    packed, usual = shares(amount, rows * top, most, skew, True), shares(amount, rows * top, most, skew, False)
    places = jnp.arange(amount)

    def named(tallies, rotation):
        used = int((tallies > 0).sum())
        fixed = max(1, used // 4)
        passed = fixed + (places - fixed + rotation * (used - fixed)) % max(1, amount - fixed)
        return jnp.zeros((amount,), jnp.int32).at[ranking[jnp.where(places < fixed, places, passed)]].set(jnp.asarray(tallies, jnp.int32))

    tallies = jnp.where(number % 4 == 0, named(packed, number // 4), named(usual, number - number // 4 - 1))
    mixed = jax.random.permutation(jax.random.fold_in(own, 3), amount)
    giver, receiver = mixed[0:amount // 2 * 2:2], mixed[1:amount // 2 * 2:2]
    margin = jnp.minimum(tallies[giver] - 1, most - tallies[receiver]) // 2
    margin = jnp.where((giver == ranking[0]) | (receiver == ranking[0]) | (tallies[receiver] == 0), 0, jnp.maximum(margin, 0))
    passed = jax.random.randint(jax.random.fold_in(own, 4), (amount // 2,), 0, 1 << 20) % (margin + 1)
    tallies = tallies.at[giver].add(-passed).at[receiver].add(passed)
    members = jnp.searchsorted(jnp.cumsum(tallies), jnp.arange(rows * top), side="right").astype(jnp.int32)
    grid = members.reshape(top, rows).T
    grid = grid[jax.random.permutation(jax.random.fold_in(own, 1), rows)]
    rotation = jax.random.randint(jax.random.fold_in(own, 2), (rows, 1), 0, top)
    return jnp.take_along_axis(grid, (jnp.arange(top)[None, :] + rotation) % top, axis=1)


def shares(count, total, bound, lean, full):
    portions = [(1 << 20) // math.isqrt(standing ** lean) + 1 for standing in range(1, count + 1)]
    largest = bound if full else min(bound, max(-(-total // count), total * portions[0] // sum(portions)))
    least = 1 if total - largest >= count - 1 else 0
    given, spare = [largest] + [least] * (count - 1), total - largest - least * (count - 1)
    while spare > 0:
        candidates = [i for i in range(1, count) if given[i] < largest] or [i for i in range(1, count) if given[i] < bound]
        mass, left = sum([portions[i] for i in candidates]), spare
        for i in candidates:
            extra = min(bound - given[i], max(1, left * portions[i] // mass), spare)
            given[i] = given[i] + extra
            spare = spare - extra
    return np.array(given)


def noise(key, extent, scale, limit, cuts=(), held_as=jnp.bfloat16):
    result = scale * jax.random.normal(key, extent, jnp.float32)
    if cuts:
        result = result * level_of(key, extent, cuts, -0.22, 0.18)
    return jnp.clip(result, -limit, limit).astype(held_as)


def heavy_noise(own_key, dims, spread, bound, shards, heavy, kind=jnp.bfloat16):
    values = spread * jax.random.normal(own_key, dims, jnp.float32)
    if shards:
        values = values * level_of(own_key, dims, shards, -0.22, 0.18)
    return jnp.clip(with_spikes(values, jax.random.fold_in(own_key, 3), *heavy), -bound, bound).astype(kind)


def setup_inputs(seed: int = 0) -> dict:
    key_of = jax.random.split(jax.random.key(seed), 8)
    tokens = noise(key_of[0], (TOKENS, D), 1.0, 6.0, ((0, 4), (1, 8)))
    cotangent = noise(key_of[1], (TOKENS, D), 1.0, 6.0, ((0, 4), (1, 8)))
    expert_ids_keys = jax.random.split(jax.random.fold_in(key_of[2], 1), TOKENS // TOK_EP)
    expert_ids_turns = jax.random.permutation(jax.random.fold_in(key_of[2], 3), TOKENS // TOK_EP)
    expert_ids = jax.vmap(lambda own, number: assign_block(jax.random.fold_in(key_of[2], 2), own, number, TOK_EP, N_EP, TOP, CAP, 2))(expert_ids_keys, expert_ids_turns).reshape((TOKENS, TOP))
    combine_weights = jnp.clip(jnp.exp(math.log(1.0) - 2.3025851 * jax.random.uniform(key_of[3], (TOKENS, TOP), jnp.float32) ** level_of(key_of[3], (TOKENS, TOP), ((0, 4),), -0.2, 0.2)), 0.1, 1.0)
    w_gate = heavy_noise(key_of[4], (EXPERTS, D, FF), D ** -0.5, 0.15625, ((0, 4), (2, 8)), (2, 1, 8, 2.0))
    w_up = noise(key_of[5], (EXPERTS, D, FF), D ** -0.5, 0.109375, ((0, 4), (2, 8)))
    w_down = heavy_noise(key_of[6], (EXPERTS, FF, D), FF ** -0.5, 0.09375, ((0, 4), (1, 8)), (1, 2, 8, 2.0))
    return {"tokens": tokens, "cotangent": cotangent, "expert_ids": expert_ids, "combine_weights": combine_weights, "w_gate": w_gate, "w_up": w_up, "w_down": w_down}


def silu_parts(gate_pre):
    sigma = jax.nn.sigmoid(gate_pre)
    return gate_pre * sigma, sigma * (1.0 + gate_pre * (1.0 - sigma))


def slot_rows(expert_ids):
    groups = expert_ids.reshape(N_EP, TOK_EP * TOP)
    onehot = (groups[:, :, None] == jnp.arange(N_EP, dtype=jnp.int32)[None, None, :]).astype(jnp.int32)
    before = jnp.cumsum(onehot, axis=1) - onehot
    rank = jnp.sum(before * onehot, axis=2)
    source = jnp.arange(N_EP, dtype=jnp.int32)[:, None]
    return (source * CAP + rank).reshape(-1).astype(jnp.int32)


def rounded_blocks(pairs, rows):
    width = FF // N_TP

    def step(total, index):
        start = index * width
        part = jnp.zeros((rows, D), jnp.float32)
        for left, right in pairs:
            left_block = lax.dynamic_slice_in_dim(left, start, width, 1)
            right_block = lax.dynamic_slice_in_dim(right, start, width, 0)
            part = part + jnp.dot(left_block, right_block, preferred_element_type=jnp.float32)
        rounded = lax.optimization_barrier(part.astype(jnp.bfloat16))
        return total + rounded.astype(jnp.float32), None

    total, _ = lax.scan(step, jnp.zeros((rows, D), jnp.float32), jnp.arange(N_TP, dtype=jnp.int32))
    return total.astype(jnp.bfloat16)


def reference(tokens, cotangent, expert_ids, combine_weights, w_gate, w_up, w_down):
    flat_ids = expert_ids.reshape(-1)
    rows = slot_rows(expert_ids)
    owner = jnp.repeat(jnp.arange(TOKENS, dtype=jnp.int32), TOP)
    weight_flat = combine_weights.reshape(-1)
    buffer_rows = N_EP * CAP
    x_buffer = jnp.zeros((N_EP, buffer_rows, D), jnp.bfloat16).at[flat_ids, rows].set(tokens[owner])
    grad_out = (weight_flat[:, None] * cotangent[owner].astype(jnp.float32)).astype(jnp.bfloat16)
    dy_buffer = jnp.zeros((N_EP, buffer_rows, D), jnp.bfloat16).at[flat_ids, rows].set(grad_out)
    outs_list, ins_list, gates_list, ups_list, downs_list = [], [], [], [], []
    for expert in range(N_EP):
        x_rows = x_buffer[expert]
        dy_rows = dy_buffer[expert]
        gate_pre = jnp.dot(x_rows, w_gate[expert], preferred_element_type=jnp.float32)
        up_pre = jnp.dot(x_rows, w_up[expert], preferred_element_type=jnp.float32)
        active, slope = silu_parts(gate_pre)
        hidden = (active * up_pre).astype(jnp.bfloat16)
        outs_list.append(rounded_blocks([(hidden, w_down[expert])], buffer_rows))
        grad_hidden = jnp.dot(dy_rows, w_down[expert].T, preferred_element_type=jnp.float32)
        grad_gate_pre = (grad_hidden * up_pre * slope).astype(jnp.bfloat16)
        grad_up_pre = (grad_hidden * active).astype(jnp.bfloat16)
        ins_list.append(rounded_blocks([(grad_gate_pre, w_gate[expert].T), (grad_up_pre, w_up[expert].T)], buffer_rows))
        gates_list.append(jnp.dot(x_rows.T, grad_gate_pre, preferred_element_type=jnp.float32).astype(jnp.bfloat16))
        ups_list.append(jnp.dot(x_rows.T, grad_up_pre, preferred_element_type=jnp.float32).astype(jnp.bfloat16))
        downs_list.append(jnp.dot(hidden.T, dy_rows, preferred_element_type=jnp.float32).astype(jnp.bfloat16))
    expert_out = jnp.stack(outs_list)[flat_ids, rows].reshape(TOKENS, TOP, D).astype(jnp.float32)
    grad_in = jnp.stack(ins_list)[flat_ids, rows].reshape(TOKENS, TOP, D).astype(jnp.float32)
    mixed = jnp.sum(combine_weights[:, :, None] * expert_out, axis=1).astype(jnp.bfloat16)
    grad_combine = jnp.sum(cotangent.astype(jnp.float32)[:, None, :] * expert_out, axis=2)
    grad_tokens = jnp.sum(grad_in, axis=1).astype(jnp.bfloat16)
    return (mixed, grad_tokens, grad_combine, jnp.stack(gates_list), jnp.stack(ups_list), jnp.stack(downs_list))
```

```python
import functools
import math

import jax
import jax.numpy as jnp
from jax import lax
from jax.experimental import pallas as pl
from jax.experimental.pallas import tpu as pltpu
from jax.sharding import PartitionSpec as P

MESH = pl.DeviceIdType.MESH
BF = jnp.bfloat16


def ring_order(chips):
    side_x = math.isqrt(chips)
    side_x = side_x if side_x * side_x == chips else chips // 2
    side_y = chips // side_x
    order = [x for x in range(side_x)]
    for y in range(1, side_y):
        xs = range(side_x - 1, 0, -1) if y % 2 else range(1, side_x)
        order += [y * side_x + x for x in xs]
    order += [y * side_x for y in range(side_y - 1, 0, -1)]
    return order


def pick(table, index):
    value = jnp.int32(table[0])
    for i in range(1, len(table)):
        value = jnp.where(index == i, jnp.int32(table[i]), value)
    return value


def remote(src, dst, send, recv, device):
    return pltpu.make_async_remote_copy(
        src_ref=src,
        dst_ref=dst,
        send_sem=send,
        recv_sem=recv,
        device_id={"tp": device},
        device_id_type=MESH,
    )


def greet(devices):
    barrier = pltpu.get_barrier_semaphore()
    for device in devices:
        pl.semaphore_signal(barrier, inc=1, device_id={"tp": device}, device_id_type=MESH)
    pl.semaphore_wait(barrier, len(devices))


def gather_kernel(count, chips, *refs):
    own, out = refs[:count], refs[count : 2 * count]
    ring_send, ring_recv, core_send, core_recv, keep = refs[2 * count :]
    order = ring_order(chips)
    place = [order.index(chip) for chip in range(chips)]
    me = lax.axis_index("tp")
    chip, core = me // 2, me % 2
    spot = pick(place, chip)
    partner = chip * 2 + 1 - core
    steps = chips // 2
    rows = own[0].shape[0]
    half = rows // 2

    def at(offset):
        return pick(order, (spot + offset + chips) % chips) * 2 + core

    right, left = at(1), at(-1)
    greet([right, left, partner])

    def part(ref, way, step):
        if step < steps - 1:
            return ref
        return ref.at[pl.ds(way * half, half)]

    def hop(k, way, step):
        index = at(-step if way == 0 else step)
        source = own[k] if step == 0 else out[k].at[index]
        return remote(
            part(source, way, step),
            part(out[k].at[index], way, step),
            ring_send.at[k, way, step],
            ring_recv.at[k, way, step],
            right if way == 0 else left,
        )

    def arrived(k, way, step):
        index = at(-(step + 1) if way == 0 else step + 1)
        block = part(out[k].at[index], way, step)
        return remote(
            block, block, ring_send.at[k, way, step], ring_recv.at[k, way, step], right if way == 0 else left
        ), remote(
            block, block, core_send.at[k, way, step], core_recv.at[k, way, step], partner
        )

    def own_pass(k):
        return remote(
            own[k], out[k].at[me], core_send.at[k, 2, 0], core_recv.at[k, 2, 0], partner
        )

    def own_keep(k):
        return pltpu.make_async_copy(own[k], out[k].at[me], keep.at[k])

    for k in range(count):
        for way in range(2):
            hop(k, way, 0).start()
    for k in range(count):
        own_pass(k).start()
        own_keep(k).start()
    for step in range(steps):
        for k in range(count):
            for way in range(2):
                landed, handed = arrived(k, way, step)
                landed.wait_recv()
                if step + 1 < steps:
                    hop(k, way, step + 1).start()
                handed.start()
    for k in range(count):
        own_keep(k).wait()
        own_pass(k).wait_send()
        other = remote(
            own[k], out[k].at[partner], core_send.at[k, 2, 0], core_recv.at[k, 2, 0], partner
        )
        other.wait_recv()
        for way in range(2):
            for step in range(steps):
                hop(k, way, step).wait_send()
                handed = arrived(k, way, step)[1]
                handed.wait_send()
                index = at(-(step + 1) if way == 0 else step + 1) // 2 * 2 + 1 - core
                block = part(out[k].at[index], way, step)
                remote(
                    block, block, core_send.at[k, way, step], core_recv.at[k, way, step], partner
                ).wait_recv()


def gather(arrays, ident):
    size = lax.axis_size("tp")
    chips, count = size // 2, len(arrays)
    ring = pltpu.SemaphoreType.DMA((count, 2, chips // 2))
    cores = pltpu.SemaphoreType.DMA((count, 3, chips // 2))
    return pl.pallas_call(
        functools.partial(gather_kernel, count, chips),
        out_shape=[jax.ShapeDtypeStruct((size,) + a.shape, a.dtype) for a in arrays],
        in_specs=[pl.BlockSpec(memory_space=pltpu.VMEM)] * count,
        out_specs=[pl.BlockSpec(memory_space=pl.ANY)] * count,
        scratch_shapes=[ring, ring, cores, cores, pltpu.SemaphoreType.DMA((count,))],
        compiler_params=pltpu.CompilerParams(collective_id=ident, has_side_effects=True),
        name=f"gather_{ident}",
    )(*arrays)


def reduce_kernel(count, chips, *refs):
    part, out = refs[:count], refs[count : 2 * count]
    pre, stage, got = refs[2 * count : 5 * count : 3], refs[2 * count + 1 : 5 * count : 3], refs[2 * count + 2 : 5 * count : 3]
    core_send, core_recv, chip_send, chip_recv = refs[5 * count :]
    me = lax.axis_index("tp")
    chip, core = me // 2, me % 2
    partner = chip * 2 + 1 - core
    away = [(chip + o) % chips for o in range(1, chips)]
    greet([partner] + [other * 2 + core for other in away])

    def swap(k):
        return remote(part[k].at[1 - core], pre[k], core_send.at[k], core_recv.at[k], partner)

    def ship(k, o):
        return remote(
            stage[k].at[away[o]], got[k].at[o], chip_send.at[k, o], chip_recv.at[k, o], away[o] * 2 + core
        )

    for k in range(count):
        swap(k).start()
    for k in range(count):
        swap(k).wait()

        def add(q, _):
            stage[k][q] = (
                part[k][core, q].astype(jnp.float32) + pre[k][q].astype(jnp.float32)
            ).astype(BF)
            return 0

        lax.fori_loop(0, chips, add, 0)
        for o in range(chips - 1):
            ship(k, o).start()
    for k in range(count):
        for o in range(chips - 1):
            ship(k, o).wait()
        total = stage[k][chip].astype(jnp.float32)
        for o in range(chips - 1):
            total = total + got[k][o].astype(jnp.float32)
        out[k][...] = total.astype(BF)


def reduce_pieces(partials, ident):
    size = lax.axis_size("tp")
    chips, count = size // 2, len(partials)
    rows, width = partials[0].shape[0], partials[0].shape[1] // size
    cut = [p.reshape(rows, chips, 2, width).transpose(2, 1, 0, 3) for p in partials]
    held = pltpu.VMEM((chips, rows, width), BF)
    got = pltpu.VMEM((chips - 1, rows, width), BF)
    return pl.pallas_call(
        functools.partial(reduce_kernel, count, chips),
        out_shape=[jax.ShapeDtypeStruct((rows, width), BF)] * count,
        in_specs=[pl.BlockSpec(memory_space=pltpu.VMEM)] * count,
        out_specs=[pl.BlockSpec(memory_space=pltpu.VMEM)] * count,
        scratch_shapes=[held, held, got] * count
        + [pltpu.SemaphoreType.DMA((count,))] * 2
        + [pltpu.SemaphoreType.DMA((count, chips - 1))] * 2,
        compiler_params=pltpu.CompilerParams(
            collective_id=ident, has_side_effects=True, vmem_limit_bytes=48 << 20
        ),
        name=f"reduce_{ident}",
    )(*cut)


def rows_kernel(x_ref, g_ref, o_ref):
    o_ref[...] = jnp.dot(x_ref[...], g_ref[0], preferred_element_type=jnp.float32).astype(BF)


def row_grads(x_turned, blocks):
    features, rows = x_turned.shape
    size, _, hidden = blocks.shape
    return pl.pallas_call(
        rows_kernel,
        grid=(size,),
        out_shape=jax.ShapeDtypeStruct((features, size * hidden), BF),
        in_specs=[
            pl.BlockSpec((features, rows), lambda n: (0, 0)),
            pl.BlockSpec((1, rows, hidden), lambda n: (n, 0, 0)),
        ],
        out_specs=pl.BlockSpec((features, hidden), lambda n: (0, n)),
        name="row_grads",
        cost_estimate=pl.CostEstimate(
            flops=2 * features * rows * size * hidden,
            bytes_accessed=2 * size * hidden * (rows + features),
            transcendentals=0,
        ),
    )(x_turned, blocks)


def side_by_side(blocks):
    size, rows, width = blocks.shape
    return blocks.transpose(1, 0, 2).reshape(rows, size * width)


def silu_parts(gate_pre):
    sigma = jax.nn.sigmoid(gate_pre)
    return (gate_pre * sigma, sigma * (1.0 + gate_pre * (1.0 - sigma)))


def contract_rows(left, right):
    return lax.dot_general(
        left, right, (((0,), (0,)), ((), ())), preferred_element_type=jnp.float32
    )


def contract_cols(left, right):
    return lax.dot_general(
        left, right, (((1,), (1,)), ((), ())), preferred_element_type=jnp.float32
    )


def general_body(tokens, cotangent, expert_ids, combine_weights, w_gate, w_up, w_down):
    groups = lax.axis_size("ep")
    tok_rows, piece_width = tokens.shape
    chosen = expert_ids.shape[1]
    capacity = tok_rows * chosen * 5 // (3 * groups)
    buffer_rows = groups * capacity
    gate_weight = w_gate[0]
    up_weight = w_up[0]
    down_weight = w_down[0]
    flat_ids = expert_ids.reshape(-1)
    onehot = (flat_ids[:, None] == jnp.arange(groups, dtype=jnp.int32)[None, :]).astype(jnp.int32)
    rank = jnp.sum((jnp.cumsum(onehot, axis=0) - onehot) * onehot, axis=1)
    slot_index = flat_ids * capacity + rank
    places = (jnp.arange(buffer_rows, dtype=jnp.int32)[:, None] == slot_index[None, :]).astype(
        jnp.bfloat16
    )
    placer = jnp.sum(
        places.reshape(buffer_rows, tok_rows, chosen).astype(jnp.float32), axis=2
    ).astype(jnp.bfloat16)
    scaled = (combine_weights[:, :, None] * cotangent[:, None, :].astype(jnp.float32)).astype(
        jnp.bfloat16
    )
    send_grad = jnp.dot(
        places, scaled.reshape(tok_rows * chosen, piece_width), preferred_element_type=jnp.float32
    ).astype(jnp.bfloat16)
    send_rows = jnp.dot(placer, tokens, preferred_element_type=jnp.float32).astype(jnp.bfloat16)
    recv_rows, recv_grad = (
        lax.all_to_all(
            send_rows.reshape(groups, capacity, piece_width),
            "ep",
            split_axis=0,
            concat_axis=0,
            tiled=True,
        ),
        lax.all_to_all(
            send_grad.reshape(groups, capacity, piece_width),
            "ep",
            split_axis=0,
            concat_axis=0,
            tiled=True,
        ),
    )
    recv_rows = recv_rows.reshape(buffer_rows, piece_width)
    recv_grad = recv_grad.reshape(buffer_rows, piece_width)
    x_blocks, dy_blocks = gather([recv_rows, recv_grad], 0)
    piece, dy_full = side_by_side(x_blocks), side_by_side(dy_blocks)
    gate_pre = jnp.dot(piece, gate_weight, preferred_element_type=jnp.float32)
    up_pre = jnp.dot(piece, up_weight, preferred_element_type=jnp.float32)
    active, slope = silu_parts(gate_pre)
    hidden = (active * up_pre).astype(jnp.bfloat16)
    partial_value = jnp.dot(hidden, down_weight, preferred_element_type=jnp.float32)
    grad_hidden = contract_cols(dy_full, down_weight)
    grad_gate_pre = (grad_hidden * up_pre * slope).astype(jnp.bfloat16)
    grad_up_pre = (grad_hidden * active).astype(jnp.bfloat16)
    input_partial = contract_cols(grad_gate_pre, gate_weight) + contract_cols(
        grad_up_pre, up_weight
    )
    out_piece, input_piece = reduce_pieces(
        [partial_value.astype(jnp.bfloat16), input_partial.astype(jnp.bfloat16)], 1
    )
    hidden_in, gate_in, up_in, out_piece, input_piece = lax.optimization_barrier(
        (hidden, grad_gate_pre, grad_up_pre, out_piece, input_piece)
    )
    hidden_blocks, gate_blocks, up_blocks = gather([hidden_in, gate_in, up_in], 2)
    out_back = lax.all_to_all(
        out_piece.reshape(groups, capacity, piece_width),
        "ep",
        split_axis=0,
        concat_axis=0,
        tiled=True,
    ).reshape(buffer_rows, piece_width)
    out_tokens = (
        jnp.take(out_back, slot_index, axis=0)
        .reshape(tok_rows, chosen, piece_width)
        .astype(jnp.float32)
    )
    mixed = jnp.sum(combine_weights[:, :, None] * out_tokens, axis=1).astype(jnp.bfloat16)
    local_products = jnp.sum(cotangent.astype(jnp.float32)[:, None, :] * out_tokens, axis=2)
    grad_combine = lax.psum(local_products, "tp")
    input_back = lax.all_to_all(
        input_piece.reshape(groups, capacity, piece_width),
        "ep",
        split_axis=0,
        concat_axis=0,
        tiled=True,
    ).reshape(buffer_rows, piece_width)
    grad_tokens = jnp.sum(
        jnp.take(input_back, slot_index, axis=0)
        .reshape(tok_rows, chosen, piece_width)
        .astype(jnp.float32),
        axis=1,
    ).astype(jnp.bfloat16)
    down_cols_out = (
        jnp.einsum("nrh,rd->nhd", hidden_blocks, recv_grad, preferred_element_type=jnp.float32)
        .astype(jnp.bfloat16)
        .reshape(-1, piece_width)
    )
    x_turned = recv_rows.T
    gate_rows_out = row_grads(x_turned, gate_blocks)
    up_rows_out = row_grads(x_turned, up_blocks)
    return (
        mixed,
        grad_tokens,
        grad_combine,
        gate_rows_out[None],
        up_rows_out[None],
        down_cols_out[None],
    )


CHUNK = 256
LANES = 128


def fast_form(tokens, expert_ids, w_gate):
    groups, size = lax.axis_size("ep"), lax.axis_size("tp")
    tok_rows, width = tokens.shape
    hidden = w_gate.shape[2]
    capacity = tok_rows * expert_ids.shape[1] * 5 // (3 * groups)
    return (
        size == 8
        and expert_ids.shape[1] == 2
        and groups <= 8
        and width % LANES == 0
        and hidden % CHUNK == 0
        and capacity % 16 == 0
        and groups * capacity % 32 == 0
        and tok_rows <= LANES
        and tok_rows % 8 == 0
    )


def far_copy(src, dst, send, recv, device):
    return pltpu.make_async_remote_copy(
        src_ref=src, dst_ref=dst, send_sem=send, recv_sem=recv, device_id=device, device_id_type=MESH
    )


def layer_kernel(
    chips,
    groups,
    capacity,
    ids,
    ids_t,
    weights,
    tokens,
    cotangent,
    wg_hbm,
    wu_hbm,
    wd_hbm,
    blocks,
    x_own,
    dy_own,
    mixed,
    grad_tokens,
    grad_combine,
    wg,
    wu,
    wd,
    both,
    out_rows,
    own,
    part,
    pre,
    stage,
    got,
    piece,
    back,
    products,
    w_sem,
    z_send,
    z_recv,
    x_send,
    x_recv,
    a_send,
    a_recv,
    keep,
    s_send,
    s_recv,
    r_send,
    r_recv,
    b_send,
    b_recv,
    p_send,
    p_recv,
):
    size = 2 * chips
    tok_rows, width = tokens.shape
    rows = groups * capacity
    model = size * width
    chunks = wg.shape[0]
    wide = 2 * width
    order = ring_order(chips)
    place = [order.index(chip) for chip in range(chips)]
    me = lax.axis_index("tp")
    group = lax.axis_index("ep")
    chip, core = me // 2, me % 2
    spot = pick(place, chip)
    partner = chip * 2 + 1 - core

    def chip_at(offset):
        return pick(order, (spot + offset + chips) % chips)

    def at(offset):
        return chip_at(offset) * 2 + core

    right, left, across = at(1), at(-1), at(2)
    sides = (right, left)

    def other(device):
        return device // 2 * 2 + 1 - core

    def fetches():
        found = []
        for c in range(chunks):
            cut = pl.ds(c * CHUNK, CHUNK)
            found.append(pltpu.make_async_copy(wg_hbm.at[:, cut], wg.at[c], w_sem.at[0, c]))
            found.append(pltpu.make_async_copy(wu_hbm.at[:, cut], wu.at[c], w_sem.at[1, c]))
        for q in range(chips):
            cut = pl.ds(q * wide, wide)
            found.append(pltpu.make_async_copy(wd_hbm.at[:, cut], wd.at[q], w_sem.at[2, q]))
        return found

    barrier = pltpu.get_barrier_semaphore()
    for d in range(1, size):
        pl.semaphore_signal(barrier, inc=1, device_id={"tp": (me + d) % size}, device_id_type=MESH)
    for d in range(1, groups):
        pl.semaphore_signal(
            barrier, inc=1, device_id={"ep": (group + d) % groups}, device_id_type=MESH
        )

    row_id = lax.broadcasted_iota(jnp.int32, (8, tok_rows), 0)
    member_t = jnp.where((ids_t[0:1, :] == row_id) | (ids_t[1:2, :] == row_id), 1.0, 0.0)
    first = lax.broadcasted_iota(jnp.int32, (tok_rows, tok_rows), 0)
    second = lax.broadcasted_iota(jnp.int32, (tok_rows, tok_rows), 1)
    before_t = jnp.dot(
        member_t.astype(BF),
        jnp.where(first < second, 1.0, 0.0).astype(BF),
        preferred_element_type=jnp.float32,
    )
    slot_t = lax.broadcasted_iota(jnp.int32, (capacity, tok_rows), 0).astype(jnp.float32)
    id_0, id_1 = ids[:, 0:1], ids[:, 1:2]
    weight_0, weight_1 = weights[:, 0:1], weights[:, 1:2]
    for p in range(groups):
        placer = (
            jnp.where(slot_t == before_t[p : p + 1, :], 1.0, 0.0) * member_t[p : p + 1, :]
        ).astype(BF)
        weight = jnp.where(id_0 == p, weight_0, 0.0) + jnp.where(id_1 == p, weight_1, 0.0)
        scaled = (weight * cotangent[...].astype(jnp.float32)).astype(BF)
        out_rows[p, 0] = jnp.dot(placer, tokens[...], preferred_element_type=jnp.float32).astype(BF)
        out_rows[p, 1] = jnp.dot(placer, scaled, preferred_element_type=jnp.float32).astype(BF)

    def rows_of(s):
        return pl.ds(pl.multiple_of(s * capacity, 16), capacity)

    def cols_of(device):
        return pl.ds(pl.multiple_of(device * width, LANES), width)

    pl.semaphore_wait(barrier, size + groups - 2)

    def z_out(k):
        p = (group + k) % groups
        return far_copy(
            out_rows.at[p],
            both.at[:, rows_of(group), cols_of(me)],
            z_send.at[k],
            z_recv.at[k],
            {"ep": p},
        )

    for k in range(1, groups):
        z_out(k).start()
    for a in range(2):
        both[a, rows_of(group), cols_of(me)] = out_rows[group, a]
    for copy in fetches():
        copy.start()

    def source(k):
        return (group - k + groups) % groups

    def x_part(k, device, a=None):
        if a is None:
            return both.at[:, rows_of(source(k)), cols_of(device)]
        return both.at[a, rows_of(source(k)), cols_of(device)]

    def x_copy(k, kind, device, target, a=None):
        block = x_part(k, device, a)
        return far_copy(block, block, x_send.at[kind, k], x_recv.at[kind, k], {"tp": target})

    for k in range(groups):
        if k > 0:
            block = x_part(k, me)
            far_copy(block, block, z_send.at[k], z_recv.at[k], {"ep": source(k)}).wait_recv()
        x_copy(k, 0, me, right).start()
        x_copy(k, 1, me, left).start()
        x_copy(k, 4, me, partner).start()
    for k in range(groups):
        for way in range(2):
            origin = sides[1 - way]
            x_copy(k, way, origin, sides[way]).wait_recv()
            x_copy(k, 2 + way, origin, sides[way], way).start()
            x_copy(k, 5 + way, origin, partner).start()
    for k in range(groups):
        for way in range(2):
            x_copy(k, 2 + way, across, sides[way], way).wait_recv()
            x_copy(k, 7 + way, across, partner, way).start()
    for k in range(groups):
        x_copy(k, 4, partner, partner).wait_recv()
        for way in range(2):
            x_copy(k, 5 + way, other(sides[1 - way]), partner).wait_recv()
            x_copy(k, 7 + way, other(across), partner, way).wait_recv()
    for copy in fetches():
        copy.wait()

    half = rows // 2

    def a_part(c, device, way=None):
        if way is None:
            return blocks.at[device, c]
        return blocks.at[device, c, :, pl.ds(way * half, half), :]

    def a_first(c, kind, target):
        return far_copy(
            own.at[c], a_part(c, me), a_send.at[kind, c], a_recv.at[kind, c], {"tp": target}
        )

    def a_copy(c, kind, device, target, way=None):
        block = a_part(c, device, way)
        return far_copy(block, block, a_send.at[kind, c], a_recv.at[kind, c], {"tp": target})

    def a_keep(c):
        return pltpu.make_async_copy(own.at[c], a_part(c, me), keep.at[c])

    def one_chunk(c, _):
        cut = pl.ds(pl.multiple_of(c * CHUNK, CHUNK), CHUNK)
        gate_pre = jnp.dot(both[0], wg[c], preferred_element_type=jnp.float32)
        up_pre = jnp.dot(both[0], wu[c], preferred_element_type=jnp.float32)
        grad_hidden = contract_cols(both[1, :, 0:wide], wd[0, cut, :])
        for q in range(1, chips):
            grad_hidden = grad_hidden + contract_cols(
                both[1, :, q * wide : (q + 1) * wide], wd[q, cut, :]
            )
        active, slope = silu_parts(gate_pre)
        own[c, 0] = (active * up_pre).astype(BF)
        own[c, 1] = (grad_hidden * up_pre * slope).astype(BF)
        own[c, 2] = (grad_hidden * active).astype(BF)
        a_first(c, 0, right).start()
        a_first(c, 1, left).start()
        a_first(c, 4, partner).start()
        a_keep(c).start()
        return 0

    lax.fori_loop(0, chunks, one_chunk, 0)

    turns = [2, 1, chips - 1, 0]

    def swap(a, o):
        return far_copy(
            part.at[a, 1 - core, o], pre.at[a, o], s_send.at[a, o], s_recv.at[a, o], {"tp": partner}
        )

    def ship(a, o):
        return far_copy(
            stage.at[a, o],
            got.at[a, o],
            r_send.at[a, o],
            r_recv.at[a, o],
            {"tp": at(turns[o])},
        )

    def one_chip(o, _):
        q = pick(order, (spot + pick(turns, o)) % chips)
        cut = pl.ds(pl.multiple_of(q * wide, LANES), wide)
        value = jnp.dot(own[0, 0], wd[q, 0:CHUNK, :], preferred_element_type=jnp.float32)
        for c in range(1, chunks):
            value = value + jnp.dot(
                own[c, 0], wd[q, c * CHUNK : (c + 1) * CHUNK, :], preferred_element_type=jnp.float32
            )
        part[0, 0, o] = value[:, :width].astype(BF)
        part[0, 1, o] = value[:, width:].astype(BF)
        swap(0, o).start()
        value = contract_cols(own[0, 1], wg[0, cut, :]) + contract_cols(own[0, 2], wu[0, cut, :])
        for c in range(1, chunks):
            value = value + contract_cols(own[c, 1], wg[c, cut, :])
            value = value + contract_cols(own[c, 2], wu[c, cut, :])
        part[1, 0, o] = value[:, :width].astype(BF)
        part[1, 1, o] = value[:, width:].astype(BF)
        swap(1, o).start()
        return 0

    lax.fori_loop(0, chips, one_chip, 0)

    x_own[...] = both[0, :, cols_of(me)]
    dy_own[...] = both[1, :, cols_of(me)]

    for o in range(chips):
        for a in range(2):
            swap(a, o).wait_recv()

            def add(b, _):
                cut = pl.ds(pl.multiple_of(b * 16, 16), 16)
                stage[a, o, cut, :] = (
                    part[a, core, o, cut, :].astype(jnp.float32)
                    + pre[a, o, cut, :].astype(jnp.float32)
                ).astype(BF)
                return 0

            lax.fori_loop(0, rows // 16, add, 0)
            if o + 1 < chips:
                ship(a, o).start()

    for c in range(chunks):
        for way in range(2):
            origin = sides[1 - way]
            a_copy(c, way, origin, sides[way]).wait_recv()
            a_copy(c, 2 + way, origin, sides[way], way).start()
            a_copy(c, 5 + way, origin, partner).start()

    for a in range(2):
        for o in range(chips - 1):
            ship(a, o).wait_recv()

        def total(b, _):
            cut = pl.ds(pl.multiple_of(b * 16, 16), 16)
            value = stage[a, chips - 1, cut, :].astype(jnp.float32)
            for o in range(chips - 1):
                value = value + got[a, o, cut, :].astype(jnp.float32)
            piece[a, cut, :] = value.astype(BF)
            return 0

        lax.fori_loop(0, rows // 16, total, 0)

    def b_out(k):
        p = (group + k) % groups
        return far_copy(
            piece.at[:, rows_of(p), :], back.at[group], b_send.at[k], b_recv.at[k], {"ep": p}
        )

    for k in range(1, groups):
        b_out(k).start()
    for a in range(2):
        back[group, a] = piece[a, rows_of(group), :]
    for k in range(1, groups):
        block = back.at[source(k)]
        far_copy(block, block, b_send.at[k], b_recv.at[k], {"ep": source(k)}).wait_recv()

    lane = lax.broadcasted_iota(jnp.int32, (tok_rows, LANES), 1)
    member = jnp.where((id_0 == lane) | (id_1 == lane), 1.0, 0.0)
    before = jnp.dot(
        jnp.where(second < first, 1.0, 0.0).astype(BF),
        member.astype(BF),
        preferred_element_type=jnp.float32,
    )
    slot = lax.broadcasted_iota(jnp.int32, (tok_rows, capacity), 1).astype(jnp.float32)
    mix = jnp.zeros((tok_rows, width), jnp.float32)
    grads = jnp.zeros((tok_rows, width), jnp.float32)
    inner = jnp.zeros((tok_rows, LANES), jnp.float32)
    for p in range(groups):
        placer = (jnp.where(slot == before[:, p : p + 1], 1.0, 0.0) * member[:, p : p + 1]).astype(BF)
        out = jnp.dot(placer, back[p, 0], preferred_element_type=jnp.float32)
        weight = jnp.where(id_0 == p, weight_0, 0.0) + jnp.where(id_1 == p, weight_1, 0.0)
        mix = mix + weight * out
        grads = grads + jnp.dot(placer, back[p, 1], preferred_element_type=jnp.float32)
        product = jnp.sum(cotangent[...].astype(jnp.float32) * out, axis=1, keepdims=True)
        inner = inner + jnp.where(((lane == 0) & (id_0 == p)) | ((lane == 1) & (id_1 == p)), product, 0.0)
    mixed[...] = mix.astype(BF)
    grad_tokens[...] = grads.astype(BF)
    if tok_rows < LANES:
        inner = jnp.concatenate([inner, jnp.zeros((LANES - tok_rows, LANES), jnp.float32)], axis=0)
    products[me] = jnp.transpose(inner)[0:8, :]

    def p_copy(d):
        return far_copy(
            products.at[me], products.at[me], p_send.at[d], p_recv.at[d], {"tp": (me + d) % size}
        )

    for d in range(1, size):
        p_copy(d).start()

    for c in range(chunks):
        for way in range(2):
            a_copy(c, 2 + way, across, sides[way], way).wait_recv()
            a_copy(c, 7 + way, across, partner, way).start()

    for d in range(1, size):
        origin = (me - d + size) % size
        block = products.at[origin]
        far_copy(block, block, p_send.at[d], p_recv.at[d], {"tp": origin}).wait_recv()
    summed = products[0]
    for d in range(1, size):
        summed = summed + products[d]
    summed = jnp.concatenate([summed, jnp.zeros((LANES - 8, LANES), jnp.float32)], axis=0)
    grad_combine[...] = jnp.transpose(summed)[0:tok_rows, 0:2]

    for k in range(1, groups):
        z_out(k).wait_send()
        b_out(k).wait_send()
    for k in range(groups):
        for way in range(2):
            x_copy(k, way, me, sides[way]).wait_send()
            x_copy(k, 2 + way, sides[1 - way], sides[way], way).wait_send()
            x_copy(k, 5 + way, sides[1 - way], partner).wait_send()
            x_copy(k, 7 + way, across, partner, way).wait_send()
        x_copy(k, 4, me, partner).wait_send()
    for a in range(2):
        for o in range(chips):
            swap(a, o).wait_send()
        for o in range(chips - 1):
            ship(a, o).wait_send()
    for d in range(1, size):
        p_copy(d).wait_send()
    for c in range(chunks):
        a_keep(c).wait()
        for way in range(2):
            a_first(c, way, sides[way]).wait_send()
            a_copy(c, 2 + way, sides[1 - way], sides[way], way).wait_send()
            a_copy(c, 5 + way, sides[1 - way], partner).wait_send()
            a_copy(c, 7 + way, across, partner, way).wait_send()
        a_first(c, 4, partner).wait_send()
    for c in range(chunks):
        a_copy(c, 4, partner, partner).wait_recv()
        for way in range(2):
            a_copy(c, 5 + way, other(sides[1 - way]), partner).wait_recv()
            a_copy(c, 7 + way, other(across), partner, way).wait_recv()


def layer(ids, ids_t, weights, tokens, cotangent, w_gate, w_up, w_down, capacity):
    size, groups = lax.axis_size("tp"), lax.axis_size("ep")
    chips = size // 2
    tok_rows, width = tokens.shape
    model, hidden = w_gate.shape
    chunks = hidden // CHUNK
    rows = groups * capacity
    whole, any_place = pl.BlockSpec(memory_space=pltpu.VMEM), pl.BlockSpec(memory_space=pl.ANY)
    dma = pltpu.SemaphoreType.DMA
    return pl.pallas_call(
        functools.partial(layer_kernel, chips, groups, capacity),
        out_shape=[
            jax.ShapeDtypeStruct((size, chunks, 3, rows, CHUNK), BF),
            jax.ShapeDtypeStruct((rows, width), BF),
            jax.ShapeDtypeStruct((rows, width), BF),
            jax.ShapeDtypeStruct((tok_rows, width), BF),
            jax.ShapeDtypeStruct((tok_rows, width), BF),
            jax.ShapeDtypeStruct((tok_rows, 2), jnp.float32),
        ],
        in_specs=[whole] * 5 + [any_place] * 3,
        out_specs=[any_place] + [whole] * 5,
        scratch_shapes=[
            pltpu.VMEM((chunks, model, CHUNK), BF),
            pltpu.VMEM((chunks, model, CHUNK), BF),
            pltpu.VMEM((chips, hidden, 2 * width), BF),
            pltpu.VMEM((2, rows, model), BF),
            pltpu.VMEM((groups, 2, capacity, width), BF),
            pltpu.VMEM((chunks, 3, rows, CHUNK), BF),
            pltpu.VMEM((2, 2, chips, rows, width), BF),
            pltpu.VMEM((2, chips, rows, width), BF),
            pltpu.VMEM((2, chips, rows, width), BF),
            pltpu.VMEM((2, chips - 1, rows, width), BF),
            pltpu.VMEM((2, rows, width), BF),
            pltpu.VMEM((groups, 2, capacity, width), BF),
            pltpu.VMEM((size, 8, LANES), jnp.float32),
            dma((3, max(chunks, chips))),
            dma((groups,)),
            dma((groups,)),
            dma((9, groups)),
            dma((9, groups)),
            dma((9, chunks)),
            dma((9, chunks)),
            dma((chunks,)),
            dma((2, chips)),
            dma((2, chips)),
            dma((2, chips - 1)),
            dma((2, chips - 1)),
            dma((groups,)),
            dma((groups,)),
            dma((size,)),
            dma((size,)),
        ],
        compiler_params=pltpu.CompilerParams(
            collective_id=0, has_side_effects=True, vmem_limit_bytes=60 << 20
        ),
        name="layer",
    )(ids, ids_t, weights, tokens, cotangent, w_gate, w_up, w_down)


def grads_kernel(x, dy, mixed_in, tokens_in, combine_in, block, gate, up, down, mixed, grad_tokens, grad_combine):
    @pl.when(pl.program_id(0) == 0)
    def _():
        mixed[...] = mixed_in[...]
        grad_tokens[...] = tokens_in[...]
        grad_combine[...] = combine_in[...]

    for c in range(block.shape[1]):
        cut = pl.ds(c * CHUNK, CHUNK)
        gate[0, :, cut] = contract_rows(x[...], block[0, c, 1]).astype(BF)
        up[0, :, cut] = contract_rows(x[...], block[0, c, 2]).astype(BF)
        down[0, cut, :] = contract_rows(block[0, c, 0], dy[...]).astype(BF)


def weight_grads(x, dy, mixed, grad_tokens, grad_combine, blocks):
    size, chunks, _, rows, _ = blocks.shape
    width = x.shape[1]
    take = 2 if chunks % 2 == 0 else 1
    steps = chunks // take
    hidden = size * chunks * CHUNK

    def whole(a):
        return pl.BlockSpec(a.shape, lambda n: (0, 0))

    return pl.pallas_call(
        grads_kernel,
        grid=(size * steps,),
        out_shape=[
            jax.ShapeDtypeStruct((1, width, hidden), BF),
            jax.ShapeDtypeStruct((1, width, hidden), BF),
            jax.ShapeDtypeStruct((1, hidden, width), BF),
            jax.ShapeDtypeStruct(mixed.shape, BF),
            jax.ShapeDtypeStruct(mixed.shape, BF),
            jax.ShapeDtypeStruct(grad_combine.shape, jnp.float32),
        ],
        in_specs=[whole(x), whole(dy), whole(mixed), whole(mixed), whole(grad_combine)]
        + [pl.BlockSpec((1, take, 3, rows, CHUNK), lambda n: (n // steps, n % steps, 0, 0, 0))],
        out_specs=[
            pl.BlockSpec((1, width, take * CHUNK), lambda n: (0, 0, n)),
            pl.BlockSpec((1, width, take * CHUNK), lambda n: (0, 0, n)),
            pl.BlockSpec((1, take * CHUNK, width), lambda n: (0, n, 0)),
            whole(mixed),
            whole(mixed),
            whole(grad_combine),
        ],
        name="weight_grads",
        cost_estimate=pl.CostEstimate(
            flops=6 * width * rows * hidden,
            bytes_accessed=6 * hidden * (rows + width),
            transcendentals=0,
        ),
    )(x, dy, mixed, grad_tokens, grad_combine, blocks)


def body(tokens, cotangent, expert_ids, combine_weights, w_gate, w_up, w_down):
    if not fast_form(tokens, expert_ids, w_gate):
        return general_body(tokens, cotangent, expert_ids, combine_weights, w_gate, w_up, w_down)
    tok_rows, chosen = expert_ids.shape
    capacity = tok_rows * chosen * 5 // (3 * lax.axis_size("ep"))
    blocks, x, dy, mixed, grad_tokens, grad_combine = layer(
        expert_ids, expert_ids.T, combine_weights, tokens, cotangent, w_gate[0], w_up[0], w_down[0], capacity
    )
    gate, up, down, mixed, grad_tokens, grad_combine = weight_grads(
        x, dy, mixed, grad_tokens, grad_combine, blocks
    )
    return mixed, grad_tokens, grad_combine, gate, up, down


def solution(mesh):
    placed = (
        P("ep", "tp"),
        P("ep", "tp"),
        P("ep", None),
        P("ep", None),
        P("ep", None, "tp"),
        P("ep", None, "tp"),
        P("ep", "tp", None),
    )
    return jax.shard_map(
        body,
        mesh=mesh,
        in_specs=placed,
        out_specs=(
            P("ep", "tp"),
            P("ep", "tp"),
            P("ep", None),
            P("ep", "tp", None),
            P("ep", "tp", None),
            P("ep", None, "tp"),
        ),
        check_vma=False,
    )
```

```python
import functools
import math

import jax
import jax.numpy as jnp
from jax import lax
from jax.experimental import pallas as pl
from jax.experimental.pallas import tpu as pltpu
from jax.sharding import PartitionSpec as P

MESH = pl.DeviceIdType.MESH
BF = jnp.bfloat16


def ring_order(chips):
    side_x = math.isqrt(chips)
    side_x = side_x if side_x * side_x == chips else chips // 2
    side_y = chips // side_x
    order = [x for x in range(side_x)]
    for y in range(1, side_y):
        xs = range(side_x - 1, 0, -1) if y % 2 else range(1, side_x)
        order += [y * side_x + x for x in xs]
    order += [y * side_x for y in range(side_y - 1, 0, -1)]
    return order


def pick(table, index):
    value = jnp.int32(table[0])
    for i in range(1, len(table)):
        value = jnp.where(index == i, jnp.int32(table[i]), value)
    return value


def remote(src, dst, send, recv, device):
    return pltpu.make_async_remote_copy(
        src_ref=src,
        dst_ref=dst,
        send_sem=send,
        recv_sem=recv,
        device_id={"tp": device},
        device_id_type=MESH,
    )


def greet(devices):
    barrier = pltpu.get_barrier_semaphore()
    for device in devices:
        pl.semaphore_signal(barrier, inc=1, device_id={"tp": device}, device_id_type=MESH)
    pl.semaphore_wait(barrier, len(devices))


def gather_kernel(count, chips, *refs):
    own, out = refs[:count], refs[count : 2 * count]
    ring_send, ring_recv, core_send, core_recv, keep = refs[2 * count :]
    order = ring_order(chips)
    place = [order.index(chip) for chip in range(chips)]
    me = lax.axis_index("tp")
    chip, core = me // 2, me % 2
    spot = pick(place, chip)
    partner = chip * 2 + 1 - core
    steps = chips // 2
    rows = own[0].shape[0]
    half = rows // 2

    def at(offset):
        return pick(order, (spot + offset + chips) % chips) * 2 + core

    right, left = at(1), at(-1)
    greet([right, left, partner])

    def part(ref, way, step):
        if step < steps - 1:
            return ref
        return ref.at[pl.ds(way * half, half)]

    def hop(k, way, step):
        index = at(-step if way == 0 else step)
        source = own[k] if step == 0 else out[k].at[index]
        return remote(
            part(source, way, step),
            part(out[k].at[index], way, step),
            ring_send.at[k, way, step],
            ring_recv.at[k, way, step],
            right if way == 0 else left,
        )

    def arrived(k, way, step):
        index = at(-(step + 1) if way == 0 else step + 1)
        block = part(out[k].at[index], way, step)
        return remote(
            block, block, ring_send.at[k, way, step], ring_recv.at[k, way, step], right if way == 0 else left
        ), remote(
            block, block, core_send.at[k, way, step], core_recv.at[k, way, step], partner
        )

    def own_pass(k):
        return remote(
            own[k], out[k].at[me], core_send.at[k, 2, 0], core_recv.at[k, 2, 0], partner
        )

    def own_keep(k):
        return pltpu.make_async_copy(own[k], out[k].at[me], keep.at[k])

    for k in range(count):
        for way in range(2):
            hop(k, way, 0).start()
    for k in range(count):
        own_pass(k).start()
        own_keep(k).start()
    for step in range(steps):
        for k in range(count):
            for way in range(2):
                landed, handed = arrived(k, way, step)
                landed.wait_recv()
                if step + 1 < steps:
                    hop(k, way, step + 1).start()
                handed.start()
    for k in range(count):
        own_keep(k).wait()
        own_pass(k).wait_send()
        other = remote(
            own[k], out[k].at[partner], core_send.at[k, 2, 0], core_recv.at[k, 2, 0], partner
        )
        other.wait_recv()
        for way in range(2):
            for step in range(steps):
                hop(k, way, step).wait_send()
                handed = arrived(k, way, step)[1]
                handed.wait_send()
                index = at(-(step + 1) if way == 0 else step + 1) // 2 * 2 + 1 - core
                block = part(out[k].at[index], way, step)
                remote(
                    block, block, core_send.at[k, way, step], core_recv.at[k, way, step], partner
                ).wait_recv()


def gather(arrays, ident):
    size = lax.axis_size("tp")
    chips, count = size // 2, len(arrays)
    ring = pltpu.SemaphoreType.DMA((count, 2, chips // 2))
    cores = pltpu.SemaphoreType.DMA((count, 3, chips // 2))
    return pl.pallas_call(
        functools.partial(gather_kernel, count, chips),
        out_shape=[jax.ShapeDtypeStruct((size,) + a.shape, a.dtype) for a in arrays],
        in_specs=[pl.BlockSpec(memory_space=pltpu.VMEM)] * count,
        out_specs=[pl.BlockSpec(memory_space=pl.ANY)] * count,
        scratch_shapes=[ring, ring, cores, cores, pltpu.SemaphoreType.DMA((count,))],
        compiler_params=pltpu.CompilerParams(collective_id=ident, has_side_effects=True),
        name=f"gather_{ident}",
    )(*arrays)


def reduce_kernel(count, chips, *refs):
    part, out = refs[:count], refs[count : 2 * count]
    pre, stage, got = refs[2 * count : 5 * count : 3], refs[2 * count + 1 : 5 * count : 3], refs[2 * count + 2 : 5 * count : 3]
    core_send, core_recv, chip_send, chip_recv = refs[5 * count :]
    me = lax.axis_index("tp")
    chip, core = me // 2, me % 2
    partner = chip * 2 + 1 - core
    away = [(chip + o) % chips for o in range(1, chips)]
    greet([partner] + [other * 2 + core for other in away])

    def swap(k):
        return remote(part[k].at[1 - core], pre[k], core_send.at[k], core_recv.at[k], partner)

    def ship(k, o):
        return remote(
            stage[k].at[away[o]], got[k].at[o], chip_send.at[k, o], chip_recv.at[k, o], away[o] * 2 + core
        )

    for k in range(count):
        swap(k).start()
    for k in range(count):
        swap(k).wait()

        def add(q, _):
            stage[k][q] = (
                part[k][core, q].astype(jnp.float32) + pre[k][q].astype(jnp.float32)
            ).astype(BF)
            return 0

        lax.fori_loop(0, chips, add, 0)
        for o in range(chips - 1):
            ship(k, o).start()
    for k in range(count):
        for o in range(chips - 1):
            ship(k, o).wait()
        total = stage[k][chip].astype(jnp.float32)
        for o in range(chips - 1):
            total = total + got[k][o].astype(jnp.float32)
        out[k][...] = total.astype(BF)


def reduce_pieces(partials, ident):
    size = lax.axis_size("tp")
    chips, count = size // 2, len(partials)
    rows, width = partials[0].shape[0], partials[0].shape[1] // size
    cut = [p.reshape(rows, chips, 2, width).transpose(2, 1, 0, 3) for p in partials]
    held = pltpu.VMEM((chips, rows, width), BF)
    got = pltpu.VMEM((chips - 1, rows, width), BF)
    return pl.pallas_call(
        functools.partial(reduce_kernel, count, chips),
        out_shape=[jax.ShapeDtypeStruct((rows, width), BF)] * count,
        in_specs=[pl.BlockSpec(memory_space=pltpu.VMEM)] * count,
        out_specs=[pl.BlockSpec(memory_space=pltpu.VMEM)] * count,
        scratch_shapes=[held, held, got] * count
        + [pltpu.SemaphoreType.DMA((count,))] * 2
        + [pltpu.SemaphoreType.DMA((count, chips - 1))] * 2,
        compiler_params=pltpu.CompilerParams(
            collective_id=ident, has_side_effects=True, vmem_limit_bytes=48 << 20
        ),
        name=f"reduce_{ident}",
    )(*cut)


def rows_kernel(x_ref, g_ref, o_ref):
    o_ref[...] = jnp.dot(x_ref[...], g_ref[0], preferred_element_type=jnp.float32).astype(BF)


def row_grads(x_turned, blocks):
    features, rows = x_turned.shape
    size, _, hidden = blocks.shape
    return pl.pallas_call(
        rows_kernel,
        grid=(size,),
        out_shape=jax.ShapeDtypeStruct((features, size * hidden), BF),
        in_specs=[
            pl.BlockSpec((features, rows), lambda n: (0, 0)),
            pl.BlockSpec((1, rows, hidden), lambda n: (n, 0, 0)),
        ],
        out_specs=pl.BlockSpec((features, hidden), lambda n: (0, n)),
        name="row_grads",
        cost_estimate=pl.CostEstimate(
            flops=2 * features * rows * size * hidden,
            bytes_accessed=2 * size * hidden * (rows + features),
            transcendentals=0,
        ),
    )(x_turned, blocks)


def side_by_side(blocks):
    size, rows, width = blocks.shape
    return blocks.transpose(1, 0, 2).reshape(rows, size * width)


def silu_parts(gate_pre):
    sigma = jax.nn.sigmoid(gate_pre)
    return (gate_pre * sigma, sigma * (1.0 + gate_pre * (1.0 - sigma)))


def contract_rows(left, right):
    return lax.dot_general(
        left, right, (((0,), (0,)), ((), ())), preferred_element_type=jnp.float32
    )


def contract_cols(left, right):
    return lax.dot_general(
        left, right, (((1,), (1,)), ((), ())), preferred_element_type=jnp.float32
    )


def general_body(tokens, cotangent, expert_ids, combine_weights, w_gate, w_up, w_down):
    groups = lax.axis_size("ep")
    tok_rows, piece_width = tokens.shape
    chosen = expert_ids.shape[1]
    capacity = tok_rows * chosen * 5 // (3 * groups)
    buffer_rows = groups * capacity
    gate_weight = w_gate[0]
    up_weight = w_up[0]
    down_weight = w_down[0]
    flat_ids = expert_ids.reshape(-1)
    onehot = (flat_ids[:, None] == jnp.arange(groups, dtype=jnp.int32)[None, :]).astype(jnp.int32)
    rank = jnp.sum((jnp.cumsum(onehot, axis=0) - onehot) * onehot, axis=1)
    slot_index = flat_ids * capacity + rank
    places = (jnp.arange(buffer_rows, dtype=jnp.int32)[:, None] == slot_index[None, :]).astype(
        jnp.bfloat16
    )
    placer = jnp.sum(
        places.reshape(buffer_rows, tok_rows, chosen).astype(jnp.float32), axis=2
    ).astype(jnp.bfloat16)
    scaled = (combine_weights[:, :, None] * cotangent[:, None, :].astype(jnp.float32)).astype(
        jnp.bfloat16
    )
    send_grad = jnp.dot(
        places, scaled.reshape(tok_rows * chosen, piece_width), preferred_element_type=jnp.float32
    ).astype(jnp.bfloat16)
    send_rows = jnp.dot(placer, tokens, preferred_element_type=jnp.float32).astype(jnp.bfloat16)
    recv_rows, recv_grad = (
        lax.all_to_all(
            send_rows.reshape(groups, capacity, piece_width),
            "ep",
            split_axis=0,
            concat_axis=0,
            tiled=True,
        ),
        lax.all_to_all(
            send_grad.reshape(groups, capacity, piece_width),
            "ep",
            split_axis=0,
            concat_axis=0,
            tiled=True,
        ),
    )
    recv_rows = recv_rows.reshape(buffer_rows, piece_width)
    recv_grad = recv_grad.reshape(buffer_rows, piece_width)
    x_blocks, dy_blocks = gather([recv_rows, recv_grad], 0)
    piece, dy_full = side_by_side(x_blocks), side_by_side(dy_blocks)
    gate_pre = jnp.dot(piece, gate_weight, preferred_element_type=jnp.float32)
    up_pre = jnp.dot(piece, up_weight, preferred_element_type=jnp.float32)
    active, slope = silu_parts(gate_pre)
    hidden = (active * up_pre).astype(jnp.bfloat16)
    partial_value = jnp.dot(hidden, down_weight, preferred_element_type=jnp.float32)
    grad_hidden = contract_cols(dy_full, down_weight)
    grad_gate_pre = (grad_hidden * up_pre * slope).astype(jnp.bfloat16)
    grad_up_pre = (grad_hidden * active).astype(jnp.bfloat16)
    input_partial = contract_cols(grad_gate_pre, gate_weight) + contract_cols(
        grad_up_pre, up_weight
    )
    out_piece, input_piece = reduce_pieces(
        [partial_value.astype(jnp.bfloat16), input_partial.astype(jnp.bfloat16)], 1
    )
    hidden_in, gate_in, up_in, out_piece, input_piece = lax.optimization_barrier(
        (hidden, grad_gate_pre, grad_up_pre, out_piece, input_piece)
    )
    hidden_blocks, gate_blocks, up_blocks = gather([hidden_in, gate_in, up_in], 2)
    out_back = lax.all_to_all(
        out_piece.reshape(groups, capacity, piece_width),
        "ep",
        split_axis=0,
        concat_axis=0,
        tiled=True,
    ).reshape(buffer_rows, piece_width)
    out_tokens = (
        jnp.take(out_back, slot_index, axis=0)
        .reshape(tok_rows, chosen, piece_width)
        .astype(jnp.float32)
    )
    mixed = jnp.sum(combine_weights[:, :, None] * out_tokens, axis=1).astype(jnp.bfloat16)
    local_products = jnp.sum(cotangent.astype(jnp.float32)[:, None, :] * out_tokens, axis=2)
    grad_combine = lax.psum(local_products, "tp")
    input_back = lax.all_to_all(
        input_piece.reshape(groups, capacity, piece_width),
        "ep",
        split_axis=0,
        concat_axis=0,
        tiled=True,
    ).reshape(buffer_rows, piece_width)
    grad_tokens = jnp.sum(
        jnp.take(input_back, slot_index, axis=0)
        .reshape(tok_rows, chosen, piece_width)
        .astype(jnp.float32),
        axis=1,
    ).astype(jnp.bfloat16)
    down_cols_out = (
        jnp.einsum("nrh,rd->nhd", hidden_blocks, recv_grad, preferred_element_type=jnp.float32)
        .astype(jnp.bfloat16)
        .reshape(-1, piece_width)
    )
    x_turned = recv_rows.T
    gate_rows_out = row_grads(x_turned, gate_blocks)
    up_rows_out = row_grads(x_turned, up_blocks)
    return (
        mixed,
        grad_tokens,
        grad_combine,
        gate_rows_out[None],
        up_rows_out[None],
        down_cols_out[None],
    )


CHUNK = 256
LANES = 128


def fast_form(tokens, expert_ids, w_gate):
    groups, size = lax.axis_size("ep"), lax.axis_size("tp")
    tok_rows, width = tokens.shape
    hidden = w_gate.shape[2]
    capacity = tok_rows * expert_ids.shape[1] * 5 // (3 * groups)
    return (
        size == 8
        and expert_ids.shape[1] == 2
        and groups <= 8
        and width % LANES == 0
        and hidden % CHUNK == 0
        and capacity % 16 == 0
        and capacity <= LANES
        and groups * capacity % 32 == 0
        and tok_rows <= LANES
        and tok_rows % 16 == 0
    )


def far_copy(src, dst, send, recv, device):
    return pltpu.make_async_remote_copy(
        src_ref=src, dst_ref=dst, send_sem=send, recv_sem=recv, device_id=device, device_id_type=MESH
    )


def layer_kernel(
    chips,
    groups,
    capacity,
    ids_t,
    weights_t,
    tokens,
    cotangent,
    wg_hbm,
    wu_hbm,
    wd_hbm,
    gate_buf,
    up_buf,
    down_buf,
    mixed,
    grad_tokens,
    grad_combine,
    blocks,
    both,
    out_rows,
    part,
    pre,
    stage,
    back,
    ready,
    got,
    turned,
    inner_sum,
    inner_out,
    inner_in,
    products,
    table,
    w_sem,
    z_send,
    z_recv,
    x_send,
    x_recv,
    a_send,
    a_recv,
    s_send,
    s_recv,
    b_send,
    b_recv,
    i_send,
    i_recv,
    r_send,
    r_recv,
    p_send,
    p_recv,
):
    size = 2 * chips
    tok_rows, width = tokens.shape
    rows = groups * capacity
    model = size * width
    hidden = wg_hbm.shape[1]
    chunks = hidden // CHUNK
    wide = 2 * width
    order = ring_order(chips)
    place = [order.index(chip) for chip in range(chips)]
    me = lax.axis_index("tp")
    group = lax.axis_index("ep")
    chip, core = me // 2, me % 2
    spot = pick(place, chip)
    partner = chip * 2 + 1 - core

    def at(offset):
        return pick(order, (spot + offset + chips) % chips) * 2 + core

    right, left, across = at(1), at(-1), at(2)
    sides = (right, left)

    def other(device):
        return device // 2 * 2 + 1 - core

    def fetches():
        found = []
        for c in range(chunks):
            cut = pl.ds(c * CHUNK, CHUNK)
            spread = pl.ds(c * model, model)
            found.append(pltpu.make_async_copy(wg_hbm.at[:, cut], gate_buf.at[spread, :], w_sem.at[0, c]))
            found.append(pltpu.make_async_copy(wu_hbm.at[:, cut], up_buf.at[spread, :], w_sem.at[1, c]))
        for q in range(chips):
            found.append(
                pltpu.make_async_copy(
                    wd_hbm.at[:, pl.ds(q * wide, wide)],
                    down_buf.at[pl.ds(q * hidden, hidden), :],
                    w_sem.at[2, q],
                )
            )
        return found

    barrier = pltpu.get_barrier_semaphore()
    for d in range(1, size):
        pl.semaphore_signal(barrier, inc=1, device_id={"tp": (me + d) % size}, device_id_type=MESH)
    for d in range(1, groups):
        pl.semaphore_signal(
            barrier, inc=1, device_id={"ep": (group + d) % groups}, device_id_type=MESH
        )

    row_id = lax.broadcasted_iota(jnp.int32, (8, tok_rows), 0)
    member_t = jnp.where((ids_t[0:1, :] == row_id) | (ids_t[1:2, :] == row_id), 1.0, 0.0)
    first = lax.broadcasted_iota(jnp.int32, (tok_rows, tok_rows), 0)
    second = lax.broadcasted_iota(jnp.int32, (tok_rows, tok_rows), 1)
    before_t = jnp.dot(
        member_t.astype(BF),
        jnp.where(first < second, 1.0, 0.0).astype(BF),
        preferred_element_type=jnp.float32,
    )
    table[...] = jnp.zeros((LANES, LANES), jnp.float32)
    table[0:2, 0:tok_rows] = ids_t[...].astype(jnp.float32)
    table[2:4, 0:tok_rows] = weights_t[...]
    columns = jnp.transpose(table[...])[0:tok_rows, :]
    choice = (columns[:, 0:1], columns[:, 1:2])
    weight = (columns[:, 2:3], columns[:, 3:4])
    slot_t = lax.broadcasted_iota(jnp.int32, (capacity, tok_rows), 0).astype(jnp.float32)
    for p in range(groups):
        placer = (
            jnp.where(slot_t == before_t[p : p + 1, :], 1.0, 0.0) * member_t[p : p + 1, :]
        ).astype(BF)
        own_weight = jnp.where(choice[0] == p, weight[0], 0.0) + jnp.where(choice[1] == p, weight[1], 0.0)
        scaled = (own_weight * cotangent[...].astype(jnp.float32)).astype(BF)
        out_rows[p, 0] = jnp.dot(placer, tokens[...], preferred_element_type=jnp.float32).astype(BF)
        out_rows[p, 1] = jnp.dot(placer, scaled, preferred_element_type=jnp.float32).astype(BF)

    def rows_of(s):
        return pl.ds(pl.multiple_of(s * capacity, 16), capacity)

    def cols_of(device):
        return pl.ds(pl.multiple_of(device * width, LANES), width)

    def source(k):
        return (group - k + groups) % groups

    pl.semaphore_wait(barrier, size + groups - 2)

    def z_out(k):
        return far_copy(
            out_rows.at[(group + k) % groups],
            both.at[:, rows_of(group), cols_of(me)],
            z_send.at[k],
            z_recv.at[k],
            {"ep": (group + k) % groups},
        )

    for k in range(1, groups):
        z_out(k).start()
    for a in range(2):
        both[a, rows_of(group), cols_of(me)] = out_rows[group, a]
    for copy in fetches():
        copy.start()

    def x_copy(k, kind, device, target, a=None):
        if a is None:
            block = both.at[:, rows_of(source(k)), cols_of(device)]
        else:
            block = both.at[a, rows_of(source(k)), cols_of(device)]
        return far_copy(block, block, x_send.at[kind, k], x_recv.at[kind, k], {"tp": target})

    for k in range(groups):
        if k > 0:
            block = both.at[:, rows_of(source(k)), cols_of(me)]
            far_copy(block, block, z_send.at[k], z_recv.at[k], {"ep": source(k)}).wait_recv()
        x_copy(k, 0, me, right).start()
        x_copy(k, 1, me, left).start()
        x_copy(k, 4, me, partner).start()
    for k in range(groups):
        for way in range(2):
            origin = sides[1 - way]
            x_copy(k, way, origin, sides[way]).wait_recv()
            x_copy(k, 2 + way, origin, sides[way], way).start()
            x_copy(k, 5 + way, origin, partner).start()
    for k in range(groups):
        for way in range(2):
            x_copy(k, 2 + way, across, sides[way], way).wait_recv()
            x_copy(k, 7 + way, across, partner, way).start()
    for k in range(groups):
        x_copy(k, 4, partner, partner).wait_recv()
        for way in range(2):
            x_copy(k, 5 + way, other(sides[1 - way]), partner).wait_recv()
            x_copy(k, 7 + way, other(across), partner, way).wait_recv()
    for copy in fetches():
        copy.wait()

    half = rows // 2

    def a_copy(c, kind, device, target, way=None):
        if way is None:
            block = blocks.at[device, c]
        else:
            block = blocks.at[device, c, :, pl.ds(way * half, half), :]
        return far_copy(block, block, a_send.at[kind, c], a_recv.at[kind, c], {"tp": target})

    inner_sum[...] = jnp.zeros((rows, LANES), jnp.float32)

    def one_chunk(c, _):
        spread = pl.ds(pl.multiple_of(c * model, 16), model)
        gate_pre = jnp.dot(both[0], gate_buf[spread, :], preferred_element_type=jnp.float32)
        up_pre = jnp.dot(both[0], up_buf[spread, :], preferred_element_type=jnp.float32)
        grad_hidden = None
        for q in range(chips):
            cut = pl.ds(pl.multiple_of(q * hidden + c * CHUNK, CHUNK), CHUNK)
            term = contract_cols(both[1, :, q * wide : (q + 1) * wide], down_buf[cut, :])
            grad_hidden = term if q == 0 else grad_hidden + term
        active, slope = silu_parts(gate_pre)
        value = (active * up_pre).astype(BF)
        blocks[me, c, 0] = value
        blocks[me, c, 1] = (grad_hidden * up_pre * slope).astype(BF)
        blocks[me, c, 2] = (grad_hidden * active).astype(BF)
        a_copy(c, 0, me, right).start()
        a_copy(c, 1, me, left).start()
        a_copy(c, 4, me, partner).start()
        product = value.astype(jnp.float32) * grad_hidden
        total = inner_sum[...]
        for n in range(CHUNK // LANES):
            total = total + product[:, n * LANES : (n + 1) * LANES]
        inner_sum[...] = total
        return 0

    lax.fori_loop(0, chunks, one_chunk, 0)

    turns = [2, 1, chips - 1, 0]

    def swap(o):
        return far_copy(part.at[1 - core, o], pre.at[o], s_send.at[o], s_recv.at[o], {"tp": partner})

    def b_out(o, k):
        p = (group + k) % groups
        return far_copy(
            stage.at[o, :, rows_of(p), :],
            back.at[:, rows_of(group), pl.ds(o * width, width)],
            b_send.at[o, k],
            b_recv.at[o, k],
            {"ep": p},
        )

    def one_chip(o, _):
        q = pick(order, (spot + pick(turns, o)) % chips)
        value = None
        for c in range(chunks):
            cut = pl.ds(pl.multiple_of(q * hidden + c * CHUNK, CHUNK), CHUNK)
            term = jnp.dot(blocks[me, c, 0], down_buf[cut, :], preferred_element_type=jnp.float32)
            value = term if c == 0 else value + term
        part[0, o, 0] = value[:, :width].astype(BF)
        part[1, o, 0] = value[:, width:].astype(BF)
        value = None
        for c in range(chunks):
            cut = pl.ds(pl.multiple_of(c * model + q * wide, LANES), wide)
            term = contract_cols(blocks[me, c, 1], gate_buf[cut, :]) + contract_cols(
                blocks[me, c, 2], up_buf[cut, :]
            )
            value = term if c == 0 else value + term
        part[0, o, 1] = value[:, :width].astype(BF)
        part[1, o, 1] = value[:, width:].astype(BF)
        swap(o).start()
        return 0

    lax.fori_loop(0, chips, one_chip, 0)

    for o in range(chips):
        swap(o).wait_recv()

        def add(s, _):
            cut = rows_of(s)
            for a in range(2):
                stage[o, a, cut, :] = (
                    part[core, o, a, cut, :].astype(jnp.float32) + pre[o, a, cut, :].astype(jnp.float32)
                ).astype(BF)
            return 0

        lax.fori_loop(0, groups, add, 0)
        for k in range(1, groups):
            b_out(o, k).start()
        for a in range(2):
            back[a, rows_of(group), o * width : (o + 1) * width] = stage[o, a, rows_of(group), :]

    def i_out(k):
        p = (group + k) % groups
        return far_copy(inner_out.at[p], inner_in.at[group], i_send.at[k], i_recv.at[k], {"ep": p})

    for p in range(groups):
        value = inner_sum[p * capacity : (p + 1) * capacity, :]
        if capacity < LANES:
            value = jnp.concatenate(
                [value, jnp.zeros((LANES - capacity, LANES), jnp.float32)], axis=0
            )
        value = jnp.sum(jnp.transpose(value), axis=0, keepdims=True)
        inner_out[p] = jnp.broadcast_to(value, (8, LANES))
    for k in range(1, groups):
        i_out(k).start()
    inner_in[group] = inner_out[group]

    turned[...] = jnp.transpose(both[0, :, cols_of(me)].astype(jnp.float32)).astype(BF)

    def grads_of(device, c):
        place_of = device * chunks + c
        spread = pl.ds(pl.multiple_of(place_of * width, LANES), width)
        gate_buf[spread, :] = jnp.dot(
            turned[...], blocks[device, c, 1], preferred_element_type=jnp.float32
        ).astype(BF)
        up_buf[spread, :] = jnp.dot(
            turned[...], blocks[device, c, 2], preferred_element_type=jnp.float32
        ).astype(BF)
        down_buf[
            pl.ds(pl.multiple_of(place_of // 2 * CHUNK, CHUNK), CHUNK),
            pl.ds(pl.multiple_of(place_of % 2 * width, LANES), width),
        ] = contract_rows(blocks[device, c, 0], both[1, :, cols_of(me)]).astype(BF)

    def grads_for(found):
        devices, chunk = [d for d, _ in found], [c for _, c in found]

        def step(n, _):
            grads_of(pick(devices, n), pick(chunk, n))
            return 0

        lax.fori_loop(0, len(found), step, 0)

    for c in range(chunks):
        a_copy(c, 4, partner, partner).wait_recv()
    grads_for([(d, c) for c in range(chunks) for d in (me, partner)])

    for c in range(chunks):
        for way in range(2):
            origin = sides[1 - way]
            a_copy(c, way, origin, sides[way]).wait_recv()
            a_copy(c, 2 + way, origin, sides[way], way).start()
            a_copy(c, 5 + way, origin, partner).start()
        found = [(left, c), (right, c)]
        if c > 0:
            for way in range(2):
                a_copy(c - 1, 5 + way, other(sides[1 - way]), partner).wait_recv()
            found += [(other(left), c - 1), (other(right), c - 1)]
        grads_for(found)
    for way in range(2):
        a_copy(chunks - 1, 5 + way, other(sides[1 - way]), partner).wait_recv()
    grads_for([(other(left), chunks - 1), (other(right), chunks - 1)])

    for k in range(1, groups):
        block = inner_in.at[source(k)]
        far_copy(block, block, i_send.at[k], i_recv.at[k], {"ep": source(k)}).wait_recv()
    lane = lax.broadcasted_iota(jnp.int32, (tok_rows, LANES), 1)
    lane_value = lane.astype(jnp.float32)
    columns = jnp.transpose(table[...])[0:tok_rows, :]
    choice = (columns[:, 0:1], columns[:, 1:2])
    weight = (columns[:, 2:3], columns[:, 3:4])
    member = jnp.where((choice[0] == lane_value) | (choice[1] == lane_value), 1.0, 0.0)
    first = lax.broadcasted_iota(jnp.int32, (tok_rows, tok_rows), 0)
    second = lax.broadcasted_iota(jnp.int32, (tok_rows, tok_rows), 1)
    before = jnp.dot(
        jnp.where(second < first, 1.0, 0.0).astype(BF),
        member.astype(BF),
        preferred_element_type=jnp.float32,
    )
    inner = jnp.zeros((tok_rows, LANES), jnp.float32)
    takers = []
    slot = lax.broadcasted_iota(jnp.int32, (tok_rows, rows), 1).astype(jnp.float32)
    for k in range(2):
        rank = jnp.sum(jnp.where(lane_value == choice[k], before, 0.0), axis=1, keepdims=True)
        takers.append(jnp.where(slot == choice[k] * capacity + rank, 1.0, 0.0).astype(BF))
        value = jnp.zeros((tok_rows, LANES), jnp.float32)
        for p in range(groups):
            value = value + jnp.where((lane_value == rank) & (choice[k] == p), inner_in[p][0:1, :], 0.0)
        value = jnp.sum(value, axis=1, keepdims=True) / weight[k]
        inner = inner + jnp.where(lane == k, value, 0.0)
    if tok_rows < LANES:
        inner = jnp.concatenate([inner, jnp.zeros((LANES - tok_rows, LANES), jnp.float32)], axis=0)
    products[me] = jnp.transpose(inner)[0:8, :]

    def p_copy(d):
        return far_copy(
            products.at[me], products.at[me], p_send.at[d], p_recv.at[d], {"tp": (me + d) % size}
        )

    for d in range(1, size):
        p_copy(d).start()

    for c in range(chunks):
        if c == chunks - 1:
            for o in range(chips):
                for k in range(1, groups):
                    block = back.at[:, rows_of(source(k)), pl.ds(o * width, width)]
                    far_copy(
                        block, block, b_send.at[o, k], b_recv.at[o, k], {"ep": source(k)}
                    ).wait_recv()
            for n in range(chips // 2):
                cut = slice(n * wide, (n + 1) * wide)
                mix = weight[0] * jnp.dot(takers[0], back[0, :, cut], preferred_element_type=jnp.float32)
                mix = mix + weight[1] * jnp.dot(
                    takers[1], back[0, :, cut], preferred_element_type=jnp.float32
                )
                grads = jnp.dot(
                    takers[0] + takers[1], back[1, :, cut], preferred_element_type=jnp.float32
                )
                for j in range(2):
                    o = 2 * n + j
                    ready[o, 0] = mix[:, j * width : (j + 1) * width].astype(BF)
                    ready[o, 1] = grads[:, j * width : (j + 1) * width].astype(BF)
                    if o < chips - 1:
                        far_copy(
                            ready.at[o], got.at[o], r_send.at[o], r_recv.at[o], {"tp": at(turns[o])}
                        ).start()
        for way in range(2):
            a_copy(c, 2 + way, across, sides[way], way).wait_recv()
            a_copy(c, 7 + way, across, partner, way).start()
        if c > 0:
            for way in range(2):
                a_copy(c - 1, 7 + way, other(across), partner, way).wait_recv()
            grads_for([(across, c), (other(across), c - 1)])
        else:
            grads_for([(across, c)])
    for way in range(2):
        a_copy(chunks - 1, 7 + way, other(across), partner, way).wait_recv()
    grads_for([(other(across), chunks - 1)])

    for d in range(1, size):
        origin = (me - d + size) % size
        block = products.at[origin]
        far_copy(block, block, p_send.at[d], p_recv.at[d], {"tp": origin}).wait_recv()
    summed = products[0]
    for d in range(1, size):
        summed = summed + products[d]
    grad_combine[...] = summed[0:2, 0:tok_rows]

    def r_copy(o):
        return far_copy(ready.at[o], got.at[o], r_send.at[o], r_recv.at[o], {"tp": at(turns[o])})

    for o in range(chips - 1):
        r_copy(o).wait_recv()
    for a, out in ((0, mixed), (1, grad_tokens)):
        value = ready[chips - 1, a].astype(jnp.float32)
        for o in range(chips - 1):
            value = value + got[o, a].astype(jnp.float32)
        out[...] = value.astype(BF)

    for k in range(1, groups):
        z_out(k).wait_send()
        i_out(k).wait_send()
        for o in range(chips):
            b_out(o, k).wait_send()
    for k in range(groups):
        for way in range(2):
            x_copy(k, way, me, sides[way]).wait_send()
            x_copy(k, 2 + way, sides[1 - way], sides[way], way).wait_send()
            x_copy(k, 5 + way, sides[1 - way], partner).wait_send()
            x_copy(k, 7 + way, across, partner, way).wait_send()
        x_copy(k, 4, me, partner).wait_send()
    for o in range(chips):
        swap(o).wait_send()
    for o in range(chips - 1):
        r_copy(o).wait_send()
    for d in range(1, size):
        p_copy(d).wait_send()
    for c in range(chunks):
        for way in range(2):
            a_copy(c, way, me, sides[way]).wait_send()
            a_copy(c, 2 + way, sides[1 - way], sides[way], way).wait_send()
            a_copy(c, 5 + way, sides[1 - way], partner).wait_send()
            a_copy(c, 7 + way, across, partner, way).wait_send()
        a_copy(c, 4, me, partner).wait_send()


def layer(ids_t, weights_t, tokens, cotangent, w_gate, w_up, w_down, capacity):
    size, groups = lax.axis_size("tp"), lax.axis_size("ep")
    chips = size // 2
    tok_rows, width = tokens.shape
    model, hidden = w_gate.shape
    chunks = hidden // CHUNK
    rows = groups * capacity
    whole, any_place = pl.BlockSpec(memory_space=pltpu.VMEM), pl.BlockSpec(memory_space=pl.ANY)
    dma = pltpu.SemaphoreType.DMA
    return pl.pallas_call(
        functools.partial(layer_kernel, chips, groups, capacity),
        out_shape=[
            pltpu.VMEM((chunks * model, CHUNK), BF),
            pltpu.VMEM((chunks * model, CHUNK), BF),
            pltpu.VMEM((chips * hidden, 2 * width), BF),
            pltpu.VMEM((tok_rows, width), BF),
            pltpu.VMEM((tok_rows, width), BF),
            pltpu.VMEM((2, tok_rows), jnp.float32),
        ],
        in_specs=[whole] * 4 + [any_place] * 3,
        out_specs=[whole] * 6,
        scratch_shapes=[
            pltpu.VMEM((size, chunks, 3, rows, CHUNK), BF),
            pltpu.VMEM((2, rows, model), BF),
            pltpu.VMEM((groups, 2, capacity, width), BF),
            pltpu.VMEM((2, chips, 2, rows, width), BF),
            pltpu.VMEM((chips, 2, rows, width), BF),
            pltpu.VMEM((chips, 2, rows, width), BF),
            pltpu.VMEM((2, rows, chips * width), BF),
            pltpu.VMEM((chips, 2, tok_rows, width), BF),
            pltpu.VMEM((chips - 1, 2, tok_rows, width), BF),
            pltpu.VMEM((width, rows), BF),
            pltpu.VMEM((rows, LANES), jnp.float32),
            pltpu.VMEM((groups, 8, LANES), jnp.float32),
            pltpu.VMEM((groups, 8, LANES), jnp.float32),
            pltpu.VMEM((size, 8, LANES), jnp.float32),
            pltpu.VMEM((LANES, LANES), jnp.float32),
            dma((3, max(chunks, chips))),
            dma((groups,)),
            dma((groups,)),
            dma((9, groups)),
            dma((9, groups)),
            dma((9, chunks)),
            dma((9, chunks)),
            dma((chips,)),
            dma((chips,)),
            dma((chips, groups)),
            dma((chips, groups)),
            dma((groups,)),
            dma((groups,)),
            dma((chips - 1,)),
            dma((chips - 1,)),
            dma((size,)),
            dma((size,)),
        ],
        compiler_params=pltpu.CompilerParams(
            collective_id=0, has_side_effects=True, vmem_limit_bytes=44 << 20
        ),
        name="layer",
    )(ids_t, weights_t, tokens, cotangent, w_gate, w_up, w_down)


def place_kernel(gate_buf, up_buf, down_buf, *refs):
    small, (gate, up, down), outs, sems = refs[:3], refs[3:6], refs[6:9], refs[9]
    width = gate.shape[0]
    count = gate.shape[1] // CHUNK
    copies = []
    for n in range(count):
        cut, spread = pl.ds(n * CHUNK, CHUNK), pl.ds(n * width, width)
        copies.append(pltpu.make_async_copy(gate_buf.at[spread, :], gate.at[:, cut], sems.at[0, n]))
        copies.append(pltpu.make_async_copy(up_buf.at[spread, :], up.at[:, cut], sems.at[1, n]))
        block = down_buf.at[pl.ds(n // 2 * CHUNK, CHUNK), pl.ds(n % 2 * width, width)]
        copies.append(pltpu.make_async_copy(block, down.at[cut, :], sems.at[2, n]))
    for n in range(3):
        copies.append(pltpu.make_async_copy(small[n], outs[n], sems.at[3, n]))
    for copy in copies:
        copy.start()
    for copy in copies:
        copy.wait()


def place_results(gate_buf, up_buf, down_buf, mixed, grad_tokens, grad_combine):
    tok_rows, width = mixed.shape
    hidden = gate_buf.shape[0] // width * CHUNK
    whole, any_place = pl.BlockSpec(memory_space=pltpu.VMEM), pl.BlockSpec(memory_space=pl.ANY)
    return pl.pallas_call(
        place_kernel,
        out_shape=[
            jax.ShapeDtypeStruct((width, hidden), BF),
            jax.ShapeDtypeStruct((width, hidden), BF),
            jax.ShapeDtypeStruct((hidden, width), BF),
            jax.ShapeDtypeStruct((tok_rows, width), BF),
            jax.ShapeDtypeStruct((tok_rows, width), BF),
            jax.ShapeDtypeStruct((2, tok_rows), jnp.float32),
        ],
        in_specs=[whole] * 6,
        out_specs=[any_place] * 6,
        scratch_shapes=[pltpu.SemaphoreType.DMA((4, max(3, hidden // CHUNK)))],
        compiler_params=pltpu.CompilerParams(vmem_limit_bytes=4 << 20),
        name="place_results",
    )(gate_buf, up_buf, down_buf, mixed, grad_tokens, grad_combine)


def body(tokens, cotangent, expert_ids, combine_weights, w_gate, w_up, w_down):
    if not fast_form(tokens, expert_ids, w_gate):
        return general_body(tokens, cotangent, expert_ids, combine_weights, w_gate, w_up, w_down)
    tok_rows, chosen = expert_ids.shape
    capacity = tok_rows * chosen * 5 // (3 * lax.axis_size("ep"))
    held = layer(
        expert_ids.T, combine_weights.T, tokens, cotangent, w_gate[0], w_up[0], w_down[0], capacity
    )
    gate, up, down, mixed, grad_tokens, grad_combine = place_results(*held)
    return mixed, grad_tokens, grad_combine.T, gate[None], up[None], down[None]


def solution(mesh):
    placed = (
        P("ep", "tp"),
        P("ep", "tp"),
        P("ep", None),
        P("ep", None),
        P("ep", None, "tp"),
        P("ep", None, "tp"),
        P("ep", "tp", None),
    )
    return jax.shard_map(
        body,
        mesh=mesh,
        in_specs=placed,
        out_specs=(
            P("ep", "tp"),
            P("ep", "tp"),
            P("ep", None),
            P("ep", "tp", None),
            P("ep", "tp", None),
            P("ep", None, "tp"),
        ),
        check_vma=False,
    )
```

```python
import functools
import math

import jax
import jax.numpy as jnp
from jax import lax
from jax.experimental import pallas as pl
from jax.experimental.pallas import tpu as pltpu
from jax.sharding import PartitionSpec as P

MESH = pl.DeviceIdType.MESH
BF = jnp.bfloat16


def ring_order(chips):
    side_x = math.isqrt(chips)
    side_x = side_x if side_x * side_x == chips else chips // 2
    side_y = chips // side_x
    order = [x for x in range(side_x)]
    for y in range(1, side_y):
        xs = range(side_x - 1, 0, -1) if y % 2 else range(1, side_x)
        order += [y * side_x + x for x in xs]
    order += [y * side_x for y in range(side_y - 1, 0, -1)]
    return order


def pick(table, index):
    value = jnp.int32(table[0])
    for i in range(1, len(table)):
        value = jnp.where(index == i, jnp.int32(table[i]), value)
    return value


def remote(src, dst, send, recv, device):
    return pltpu.make_async_remote_copy(
        src_ref=src,
        dst_ref=dst,
        send_sem=send,
        recv_sem=recv,
        device_id={"tp": device},
        device_id_type=MESH,
    )


def greet(devices):
    barrier = pltpu.get_barrier_semaphore()
    for device in devices:
        pl.semaphore_signal(barrier, inc=1, device_id={"tp": device}, device_id_type=MESH)
    pl.semaphore_wait(barrier, len(devices))


def gather_kernel(count, chips, *refs):
    own, out = refs[:count], refs[count : 2 * count]
    ring_send, ring_recv, core_send, core_recv, keep = refs[2 * count :]
    order = ring_order(chips)
    place = [order.index(chip) for chip in range(chips)]
    me = lax.axis_index("tp")
    chip, core = me // 2, me % 2
    spot = pick(place, chip)
    partner = chip * 2 + 1 - core
    steps = chips // 2
    rows = own[0].shape[0]
    half = rows // 2

    def at(offset):
        return pick(order, (spot + offset + chips) % chips) * 2 + core

    right, left = at(1), at(-1)
    greet([right, left, partner])

    def part(ref, way, step):
        if step < steps - 1:
            return ref
        return ref.at[pl.ds(way * half, half)]

    def hop(k, way, step):
        index = at(-step if way == 0 else step)
        source = own[k] if step == 0 else out[k].at[index]
        return remote(
            part(source, way, step),
            part(out[k].at[index], way, step),
            ring_send.at[k, way, step],
            ring_recv.at[k, way, step],
            right if way == 0 else left,
        )

    def arrived(k, way, step):
        index = at(-(step + 1) if way == 0 else step + 1)
        block = part(out[k].at[index], way, step)
        return remote(
            block, block, ring_send.at[k, way, step], ring_recv.at[k, way, step], right if way == 0 else left
        ), remote(
            block, block, core_send.at[k, way, step], core_recv.at[k, way, step], partner
        )

    def own_pass(k):
        return remote(
            own[k], out[k].at[me], core_send.at[k, 2, 0], core_recv.at[k, 2, 0], partner
        )

    def own_keep(k):
        return pltpu.make_async_copy(own[k], out[k].at[me], keep.at[k])

    for k in range(count):
        for way in range(2):
            hop(k, way, 0).start()
    for k in range(count):
        own_pass(k).start()
        own_keep(k).start()
    for step in range(steps):
        for k in range(count):
            for way in range(2):
                landed, handed = arrived(k, way, step)
                landed.wait_recv()
                if step + 1 < steps:
                    hop(k, way, step + 1).start()
                handed.start()
    for k in range(count):
        own_keep(k).wait()
        own_pass(k).wait_send()
        other = remote(
            own[k], out[k].at[partner], core_send.at[k, 2, 0], core_recv.at[k, 2, 0], partner
        )
        other.wait_recv()
        for way in range(2):
            for step in range(steps):
                hop(k, way, step).wait_send()
                handed = arrived(k, way, step)[1]
                handed.wait_send()
                index = at(-(step + 1) if way == 0 else step + 1) // 2 * 2 + 1 - core
                block = part(out[k].at[index], way, step)
                remote(
                    block, block, core_send.at[k, way, step], core_recv.at[k, way, step], partner
                ).wait_recv()


def gather(arrays, ident):
    size = lax.axis_size("tp")
    chips, count = size // 2, len(arrays)
    ring = pltpu.SemaphoreType.DMA((count, 2, chips // 2))
    cores = pltpu.SemaphoreType.DMA((count, 3, chips // 2))
    return pl.pallas_call(
        functools.partial(gather_kernel, count, chips),
        out_shape=[jax.ShapeDtypeStruct((size,) + a.shape, a.dtype) for a in arrays],
        in_specs=[pl.BlockSpec(memory_space=pltpu.VMEM)] * count,
        out_specs=[pl.BlockSpec(memory_space=pl.ANY)] * count,
        scratch_shapes=[ring, ring, cores, cores, pltpu.SemaphoreType.DMA((count,))],
        compiler_params=pltpu.CompilerParams(collective_id=ident, has_side_effects=True),
        name=f"gather_{ident}",
    )(*arrays)


def reduce_kernel(count, chips, *refs):
    part, out = refs[:count], refs[count : 2 * count]
    pre, stage, got = refs[2 * count : 5 * count : 3], refs[2 * count + 1 : 5 * count : 3], refs[2 * count + 2 : 5 * count : 3]
    core_send, core_recv, chip_send, chip_recv = refs[5 * count :]
    me = lax.axis_index("tp")
    chip, core = me // 2, me % 2
    partner = chip * 2 + 1 - core
    away = [(chip + o) % chips for o in range(1, chips)]
    greet([partner] + [other * 2 + core for other in away])

    def swap(k):
        return remote(part[k].at[1 - core], pre[k], core_send.at[k], core_recv.at[k], partner)

    def ship(k, o):
        return remote(
            stage[k].at[away[o]], got[k].at[o], chip_send.at[k, o], chip_recv.at[k, o], away[o] * 2 + core
        )

    for k in range(count):
        swap(k).start()
    for k in range(count):
        swap(k).wait()

        def add(q, _):
            stage[k][q] = (
                part[k][core, q].astype(jnp.float32) + pre[k][q].astype(jnp.float32)
            ).astype(BF)
            return 0

        lax.fori_loop(0, chips, add, 0)
        for o in range(chips - 1):
            ship(k, o).start()
    for k in range(count):
        for o in range(chips - 1):
            ship(k, o).wait()
        total = stage[k][chip].astype(jnp.float32)
        for o in range(chips - 1):
            total = total + got[k][o].astype(jnp.float32)
        out[k][...] = total.astype(BF)


def reduce_pieces(partials, ident):
    size = lax.axis_size("tp")
    chips, count = size // 2, len(partials)
    rows, width = partials[0].shape[0], partials[0].shape[1] // size
    cut = [p.reshape(rows, chips, 2, width).transpose(2, 1, 0, 3) for p in partials]
    held = pltpu.VMEM((chips, rows, width), BF)
    got = pltpu.VMEM((chips - 1, rows, width), BF)
    return pl.pallas_call(
        functools.partial(reduce_kernel, count, chips),
        out_shape=[jax.ShapeDtypeStruct((rows, width), BF)] * count,
        in_specs=[pl.BlockSpec(memory_space=pltpu.VMEM)] * count,
        out_specs=[pl.BlockSpec(memory_space=pltpu.VMEM)] * count,
        scratch_shapes=[held, held, got] * count
        + [pltpu.SemaphoreType.DMA((count,))] * 2
        + [pltpu.SemaphoreType.DMA((count, chips - 1))] * 2,
        compiler_params=pltpu.CompilerParams(
            collective_id=ident, has_side_effects=True, vmem_limit_bytes=48 << 20
        ),
        name=f"reduce_{ident}",
    )(*cut)


def rows_kernel(x_ref, g_ref, o_ref):
    o_ref[...] = jnp.dot(x_ref[...], g_ref[0], preferred_element_type=jnp.float32).astype(BF)


def row_grads(x_turned, blocks):
    features, rows = x_turned.shape
    size, _, hidden = blocks.shape
    return pl.pallas_call(
        rows_kernel,
        grid=(size,),
        out_shape=jax.ShapeDtypeStruct((features, size * hidden), BF),
        in_specs=[
            pl.BlockSpec((features, rows), lambda n: (0, 0)),
            pl.BlockSpec((1, rows, hidden), lambda n: (n, 0, 0)),
        ],
        out_specs=pl.BlockSpec((features, hidden), lambda n: (0, n)),
        name="row_grads",
        cost_estimate=pl.CostEstimate(
            flops=2 * features * rows * size * hidden,
            bytes_accessed=2 * size * hidden * (rows + features),
            transcendentals=0,
        ),
    )(x_turned, blocks)


def side_by_side(blocks):
    size, rows, width = blocks.shape
    return blocks.transpose(1, 0, 2).reshape(rows, size * width)


def silu_parts(gate_pre):
    sigma = jax.nn.sigmoid(gate_pre)
    return (gate_pre * sigma, sigma * (1.0 + gate_pre * (1.0 - sigma)))


def contract_rows(left, right):
    return lax.dot_general(
        left, right, (((0,), (0,)), ((), ())), preferred_element_type=jnp.float32
    )


def contract_cols(left, right):
    return lax.dot_general(
        left, right, (((1,), (1,)), ((), ())), preferred_element_type=jnp.float32
    )


def general_body(tokens, cotangent, expert_ids, combine_weights, w_gate, w_up, w_down):
    groups = lax.axis_size("ep")
    tok_rows, piece_width = tokens.shape
    chosen = expert_ids.shape[1]
    capacity = tok_rows * chosen * 5 // (3 * groups)
    buffer_rows = groups * capacity
    gate_weight = w_gate[0]
    up_weight = w_up[0]
    down_weight = w_down[0]
    flat_ids = expert_ids.reshape(-1)
    onehot = (flat_ids[:, None] == jnp.arange(groups, dtype=jnp.int32)[None, :]).astype(jnp.int32)
    rank = jnp.sum((jnp.cumsum(onehot, axis=0) - onehot) * onehot, axis=1)
    slot_index = flat_ids * capacity + rank
    places = (jnp.arange(buffer_rows, dtype=jnp.int32)[:, None] == slot_index[None, :]).astype(
        jnp.bfloat16
    )
    placer = jnp.sum(
        places.reshape(buffer_rows, tok_rows, chosen).astype(jnp.float32), axis=2
    ).astype(jnp.bfloat16)
    scaled = (combine_weights[:, :, None] * cotangent[:, None, :].astype(jnp.float32)).astype(
        jnp.bfloat16
    )
    send_grad = jnp.dot(
        places, scaled.reshape(tok_rows * chosen, piece_width), preferred_element_type=jnp.float32
    ).astype(jnp.bfloat16)
    send_rows = jnp.dot(placer, tokens, preferred_element_type=jnp.float32).astype(jnp.bfloat16)
    recv_rows, recv_grad = (
        lax.all_to_all(
            send_rows.reshape(groups, capacity, piece_width),
            "ep",
            split_axis=0,
            concat_axis=0,
            tiled=True,
        ),
        lax.all_to_all(
            send_grad.reshape(groups, capacity, piece_width),
            "ep",
            split_axis=0,
            concat_axis=0,
            tiled=True,
        ),
    )
    recv_rows = recv_rows.reshape(buffer_rows, piece_width)
    recv_grad = recv_grad.reshape(buffer_rows, piece_width)
    x_blocks, dy_blocks = gather([recv_rows, recv_grad], 0)
    piece, dy_full = side_by_side(x_blocks), side_by_side(dy_blocks)
    gate_pre = jnp.dot(piece, gate_weight, preferred_element_type=jnp.float32)
    up_pre = jnp.dot(piece, up_weight, preferred_element_type=jnp.float32)
    active, slope = silu_parts(gate_pre)
    hidden = (active * up_pre).astype(jnp.bfloat16)
    partial_value = jnp.dot(hidden, down_weight, preferred_element_type=jnp.float32)
    grad_hidden = contract_cols(dy_full, down_weight)
    grad_gate_pre = (grad_hidden * up_pre * slope).astype(jnp.bfloat16)
    grad_up_pre = (grad_hidden * active).astype(jnp.bfloat16)
    input_partial = contract_cols(grad_gate_pre, gate_weight) + contract_cols(
        grad_up_pre, up_weight
    )
    out_piece, input_piece = reduce_pieces(
        [partial_value.astype(jnp.bfloat16), input_partial.astype(jnp.bfloat16)], 1
    )
    hidden_in, gate_in, up_in, out_piece, input_piece = lax.optimization_barrier(
        (hidden, grad_gate_pre, grad_up_pre, out_piece, input_piece)
    )
    hidden_blocks, gate_blocks, up_blocks = gather([hidden_in, gate_in, up_in], 2)
    out_back = lax.all_to_all(
        out_piece.reshape(groups, capacity, piece_width),
        "ep",
        split_axis=0,
        concat_axis=0,
        tiled=True,
    ).reshape(buffer_rows, piece_width)
    out_tokens = (
        jnp.take(out_back, slot_index, axis=0)
        .reshape(tok_rows, chosen, piece_width)
        .astype(jnp.float32)
    )
    mixed = jnp.sum(combine_weights[:, :, None] * out_tokens, axis=1).astype(jnp.bfloat16)
    local_products = jnp.sum(cotangent.astype(jnp.float32)[:, None, :] * out_tokens, axis=2)
    grad_combine = lax.psum(local_products, "tp")
    input_back = lax.all_to_all(
        input_piece.reshape(groups, capacity, piece_width),
        "ep",
        split_axis=0,
        concat_axis=0,
        tiled=True,
    ).reshape(buffer_rows, piece_width)
    grad_tokens = jnp.sum(
        jnp.take(input_back, slot_index, axis=0)
        .reshape(tok_rows, chosen, piece_width)
        .astype(jnp.float32),
        axis=1,
    ).astype(jnp.bfloat16)
    down_cols_out = (
        jnp.einsum("nrh,rd->nhd", hidden_blocks, recv_grad, preferred_element_type=jnp.float32)
        .astype(jnp.bfloat16)
        .reshape(-1, piece_width)
    )
    x_turned = recv_rows.T
    gate_rows_out = row_grads(x_turned, gate_blocks)
    up_rows_out = row_grads(x_turned, up_blocks)
    return (
        mixed,
        grad_tokens,
        grad_combine,
        gate_rows_out[None],
        up_rows_out[None],
        down_cols_out[None],
    )


CHUNK = 256
LANES = 128


def fast_form(tokens, expert_ids, w_gate):
    groups, size = lax.axis_size("ep"), lax.axis_size("tp")
    tok_rows, width = tokens.shape
    hidden = w_gate.shape[2]
    capacity = tok_rows * expert_ids.shape[1] * 5 // (3 * groups)
    return (
        size == 8
        and expert_ids.shape[1] == 2
        and 3 <= groups <= 8
        and width % LANES == 0
        and hidden % CHUNK == 0
        and capacity % 16 == 0
        and capacity <= LANES
        and groups * capacity % 32 == 0
        and tok_rows <= LANES
        and tok_rows % 16 == 0
    )


def far_copy(src, dst, send, recv, device):
    return pltpu.make_async_remote_copy(
        src_ref=src, dst_ref=dst, send_sem=send, recv_sem=recv, device_id=device, device_id_type=MESH
    )


def layer_kernel(
    chips,
    groups,
    capacity,
    ids_hbm,
    weights_hbm,
    tokens_hbm,
    cotangent_hbm,
    wg_hbm,
    wu_hbm,
    wd_hbm,
    gate_buf,
    up_buf,
    down_buf,
    mixed,
    grad_tokens,
    grad_combine,
    blocks,
    both,
    out_rows,
    factors,
    part,
    pre,
    stage,
    back,
    ready,
    got,
    turned,
    inner_sum,
    inner_out,
    inner_in,
    products,
    table,
    ids_t,
    weights_t,
    tokens,
    cotangent,
    in_sem,
    w_sem,
    z_recv,
    x_side,
    x_far,
    x_pass,
    a_side,
    a_far,
    a_own,
    a_pass,
    s_recv,
    recv,
    send,
):
    size = 2 * chips
    tok_rows, width = tokens.shape
    rows = groups * capacity
    model = size * width
    hidden = wg_hbm.shape[1]
    chunks = hidden // CHUNK
    wide = 2 * width
    order = ring_order(chips)
    place = [order.index(chip) for chip in range(chips)]
    me = lax.axis_index("tp")
    group = lax.axis_index("ep")
    chip, core = me // 2, me % 2
    spot = pick(place, chip)
    partner = chip * 2 + 1 - core

    def at(offset):
        return pick(order, (spot + offset + chips) % chips) * 2 + core

    right, left, across = at(1), at(-1), at(2)
    sides = (right, left)

    def other(device):
        return device // 2 * 2 + 1 - core

    near = [sorted(range(groups), key=lambda s: (abs(s - g), s)) for g in range(groups)]
    planes = [pick([near[g][k] for g in range(groups)], group) for k in range(groups)]

    def rows_of(s):
        return pl.ds(pl.multiple_of(s * capacity, 16), capacity)

    def cols_of(device):
        return pl.ds(pl.multiple_of(device * width, LANES), width)

    def take(block, sem, device):
        far_copy(block, block, send.at[0], sem, device).wait_recv()

    barrier = pltpu.get_barrier_semaphore()
    for k in range(1, groups):
        pl.semaphore_signal(barrier, inc=1, device_id={"ep": planes[k]}, device_id_type=MESH)
    for d in range(1, size):
        pl.semaphore_signal(barrier, inc=1, device_id={"tp": (me + d) % size}, device_id_type=MESH)

    inputs = (
        (ids_hbm, ids_t),
        (weights_hbm, weights_t),
        (tokens_hbm, tokens),
        (cotangent_hbm, cotangent),
    )
    inputs = [pltpu.make_async_copy(a, b, in_sem.at[n]) for n, (a, b) in enumerate(inputs)]
    for copy in inputs:
        copy.start()
    for copy in inputs:
        copy.wait()
    row_id = lax.broadcasted_iota(jnp.int32, (8, tok_rows), 0)
    member_t = jnp.where((ids_t[0:1, :] == row_id) | (ids_t[1:2, :] == row_id), 1.0, 0.0)
    first = lax.broadcasted_iota(jnp.int32, (tok_rows, tok_rows), 0)
    second = lax.broadcasted_iota(jnp.int32, (tok_rows, tok_rows), 1)
    before_t = jnp.dot(
        member_t.astype(BF),
        jnp.where(first < second, 1.0, 0.0).astype(BF),
        preferred_element_type=jnp.float32,
    )
    table[...] = jnp.zeros((LANES, LANES), jnp.float32)
    table[0:2, 0:tok_rows] = ids_t[...].astype(jnp.float32)
    table[2:4, 0:tok_rows] = weights_t[...]
    columns = jnp.transpose(table[...])[0:tok_rows, :]
    choice = (columns[:, 0:1], columns[:, 1:2])
    weight = (columns[:, 2:3], columns[:, 3:4])
    slot_t = lax.broadcasted_iota(jnp.int32, (capacity, tok_rows), 0).astype(jnp.float32)
    for p in range(groups):
        placer = (
            jnp.where(slot_t == before_t[p : p + 1, :], 1.0, 0.0) * member_t[p : p + 1, :]
        ).astype(BF)
        own_weight = jnp.where(choice[0] == p, weight[0], 0.0) + jnp.where(choice[1] == p, weight[1], 0.0)
        scaled = (own_weight * cotangent[...].astype(jnp.float32)).astype(BF)
        out_rows[p, 0] = jnp.dot(placer, tokens[...], preferred_element_type=jnp.float32).astype(BF)
        out_rows[p, 1] = jnp.dot(placer, scaled, preferred_element_type=jnp.float32).astype(BF)

    pl.semaphore_wait(barrier, size + groups - 2)


    def z_first(a):
        for k in range(groups - 1, 0, -1):
            far_copy(
                out_rows.at[planes[k], a],
                both.at[a, rows_of(group), cols_of(me)],
                send.at[0],
                z_recv.at[a, group],
                {"ep": planes[k]},
            ).start()

    z_first(0)

    def x_block(a, k, device):
        return both.at[a, rows_of(planes[k]), cols_of(device)]

    def x_send(a, k, device, sem, target):
        block = x_block(a, k, device)
        far_copy(block, block, send.at[1], sem, {"tp": target}).start()

    def x_first(a, k):
        if k == 0:
            both[a, rows_of(group), cols_of(me)] = out_rows[group, a]
        else:
            take(x_block(a, k, me), z_recv.at[a, planes[k]], {"ep": planes[k]})
        for way in range(2):
            x_send(a, k, me, x_side.at[a, way, k], sides[way])
        if a == 0 and k > 0:
            x_send(a, k, me, x_far.at[a, k], across)
        x_send(a, k, me, x_pass.at[a], partner)

    def x_relay(a, k):
        for way in range(2):
            origin = sides[1 - way]
            take(x_block(a, k, origin), x_side.at[a, way, k], {"tp": origin})
            if (a + k) % 2 == way and (a == 1 or k == 0):
                x_send(a, k, origin, x_far.at[a, k], sides[way])
            x_send(a, k, origin, x_pass.at[a], partner)

    def x_last(a, k):
        take(x_block(a, k, across), x_far.at[a, k], {"tp": sides[1 - (a + k) % 2]})
        x_send(a, k, across, x_pass.at[a], partner)

    def x_whole(a):
        take(both.at[a, :, pl.ds(0, chips * width)], x_pass.at[a], {"tp": partner})

    def fetch(n):
        source, target = ((wg_hbm, gate_buf), (wu_hbm, up_buf), (wd_hbm, down_buf))[n]
        if n < 2:
            for c in range(chunks):
                pltpu.make_async_copy(
                    source.at[:, pl.ds(c * CHUNK, CHUNK)],
                    target.at[pl.ds(c * model, model), :],
                    w_sem.at[n],
                ).start()
        else:
            for q in range(chips):
                pltpu.make_async_copy(
                    source.at[:, pl.ds(q * wide, wide)],
                    target.at[pl.ds(q * hidden, hidden), :],
                    w_sem.at[n],
                ).start()

    def fetched(n):
        target = (gate_buf, up_buf, down_buf)[n]
        pltpu.make_async_copy(target, target, w_sem.at[n]).wait()

    x_first(0, 0)
    x_first(1, 0)
    for n in range(3):
        fetch(n)
    x_relay(0, 0)
    for k in range(1, groups):
        x_first(0, k)
        if k == 2:
            z_first(1)
        if k == 1:
            x_relay(1, 0)
            x_last(0, 0)
        else:
            x_relay(0, k - 1)
        if k == groups - 1:
            x_last(1, 0)
    x_first(1, 1)
    x_relay(0, groups - 1)
    x_last(0, 1)
    x_first(1, 2)
    x_relay(1, 1)
    for k in range(3, groups):
        x_last(0, k - 1)
        x_first(1, k)
    x_last(0, groups - 1)
    x_whole(0)
    fetched(0)
    fetched(1)

    half = rows // 2
    kinds = ((0, 1), (1, 2))

    def a_block(b, c, device, way=None):
        start, count = kinds[b]
        if way is None:
            return blocks.at[device, c, pl.ds(start, count)]
        return blocks.at[device, c, pl.ds(start, count), pl.ds(way * half, half), :]

    def a_send(b, c, device, sem, target, way=None):
        block = a_block(b, c, device, way)
        far_copy(block, block, send.at[2], sem, {"tp": target}).start()

    def a_first(b, c):
        for way in range(2):
            a_send(b, c, me, a_side.at[b, way, c], sides[way])
        a_send(b, c, me, a_own.at[b], partner)

    def a_relay(b, c):
        for way in range(2):
            origin = sides[1 - way]
            take(a_block(b, c, origin), a_side.at[b, way, c], {"tp": origin})
            a_send(b, c, origin, a_far.at[b, c], sides[way], way)
            a_send(b, c, origin, a_pass.at[b, 0, c], partner)

    def a_relayed(b, c):
        start, count = kinds[b]
        take(blocks.at[pl.ds(0, 2), c, pl.ds(start, count)], a_pass.at[b, 0, c], {"tp": partner})

    def a_last(b, c):
        take(a_block(b, c, across), a_far.at[b, c], {"tp": left})
        a_send(b, c, across, a_pass.at[b, 1, c], partner)

    def a_lasted(b, c):
        take(a_block(b, c, other(across)), a_pass.at[b, 1, c], {"tp": partner})

    def hidden_chunk(c):
        spread = pl.ds(c * model, model)
        gate_pre = jnp.dot(both[0], gate_buf[spread, :], preferred_element_type=jnp.float32)
        up_pre = jnp.dot(both[0], up_buf[spread, :], preferred_element_type=jnp.float32)
        active, slope = silu_parts(gate_pre)
        blocks[me, c, 0] = (active * up_pre).astype(BF)
        factors[0, c] = up_pre * slope
        factors[1, c] = active

    later = [(x_last, k) for k in range(1, groups)]
    split = [len(later) * c // max(1, chunks - 1) for c in range(chunks)]
    done = 0
    for c in range(chunks):
        hidden_chunk(c)
        if c == 0:
            for k in range(2, groups):
                x_relay(1, k)
        a_first(0, c)
        for step, k in later[done : split[c]]:
            step(1, k)
        done = split[c]
    x_whole(1)
    fetched(2)
    inner_sum[...] = jnp.zeros((rows, LANES), jnp.float32)

    def grad_chunk(c, _):
        grad_hidden = None
        for q in range(chips):
            cut = pl.ds(pl.multiple_of(q * hidden + c * CHUNK, CHUNK), CHUNK)
            term = contract_cols(both[1, :, q * wide : (q + 1) * wide], down_buf[cut, :])
            grad_hidden = term if q == 0 else grad_hidden + term
        blocks[me, c, 1] = (grad_hidden * factors[0, c]).astype(BF)
        blocks[me, c, 2] = (grad_hidden * factors[1, c]).astype(BF)
        a_first(1, c)
        product = blocks[me, c, 0].astype(jnp.float32) * grad_hidden
        total = inner_sum[...]
        for n in range(CHUNK // LANES):
            total = total + product[:, n * LANES : (n + 1) * LANES]
        inner_sum[...] = total
        return 0

    lax.fori_loop(0, chunks, grad_chunk, 0)

    turns = [2, 1, chips - 1, 0]

    def swap(a, o, value):
        part[a, 0, o] = value[:, :width].astype(BF)
        part[a, 1, o] = value[:, width:].astype(BF)
        far_copy(
            part.at[a, 1 - core, o], pre.at[a, o], send.at[3], s_recv.at[a, o], {"tp": partner}
        ).start()

    def out_part(o, _):
        q = pick(order, (spot + pick(turns, o)) % chips)
        value = None
        for c in range(chunks):
            cut = pl.ds(pl.multiple_of(q * hidden + c * CHUNK, CHUNK), CHUNK)
            term = jnp.dot(blocks[me, c, 0], down_buf[cut, :], preferred_element_type=jnp.float32)
            value = term if c == 0 else value + term
        swap(0, o, value)
        return 0

    def in_part(o, _):
        q = pick(order, (spot + pick(turns, o)) % chips)
        value = None
        for c in range(chunks):
            cut = pl.ds(pl.multiple_of(c * model + q * wide, LANES), wide)
            term = contract_cols(blocks[me, c, 1], gate_buf[cut, :]) + contract_cols(
                blocks[me, c, 2], up_buf[cut, :]
            )
            value = term if c == 0 else value + term
        swap(1, o, value)
        return 0

    def spread_parts(a):
        for o in range(chips):
            take(pre.at[a, o], s_recv.at[a, o], {"tp": partner})

            def add(s, _):
                cut = rows_of(s)
                stage[a, o, cut, :] = (
                    part[a, core, o, cut, :].astype(jnp.float32) + pre[a, o, cut, :].astype(jnp.float32)
                ).astype(BF)
                return 0

            lax.fori_loop(0, groups, add, 0)
            for k in range(groups - 1, 0, -1):
                far_copy(
                    stage.at[a, o, rows_of(planes[k]), :],
                    back.at[a, rows_of(group), pl.ds(o * width, width)],
                    send.at[4],
                    recv.at[0],
                    {"ep": planes[k]},
                ).start()
            back[a, rows_of(group), o * width : (o + 1) * width] = stage[a, o, rows_of(group), :]

    lax.fori_loop(0, chips, out_part, 0)
    spread_parts(0)
    lax.fori_loop(0, chips, in_part, 0)
    spread_parts(1)

    for p in range(groups):
        value = inner_sum[p * capacity : (p + 1) * capacity, :]
        if capacity < LANES:
            value = jnp.concatenate(
                [value, jnp.zeros((LANES - capacity, LANES), jnp.float32)], axis=0
            )
        value = jnp.sum(jnp.transpose(value), axis=0, keepdims=True)
        inner_out[p] = jnp.broadcast_to(value, (8, LANES))
    for k in range(1, groups):
        far_copy(
            inner_out.at[planes[k]], inner_in.at[group], send.at[5], recv.at[1], {"ep": planes[k]}
        ).start()
    inner_in[group] = inner_out[group]

    turned[...] = jnp.transpose(both[0, :, cols_of(me)].astype(jnp.float32)).astype(BF)

    def down_grads(device, c):
        place_of = device * chunks + c
        down_buf[
            pl.ds(pl.multiple_of(place_of // 2 * CHUNK, CHUNK), CHUNK),
            pl.ds(pl.multiple_of(place_of % 2 * width, LANES), width),
        ] = contract_rows(blocks[device, c, 0], both[1, :, cols_of(me)]).astype(BF)

    def side_grads(device, c):
        spread = pl.ds(pl.multiple_of((device * chunks + c) * width, LANES), width)
        gate_buf[spread, :] = jnp.dot(
            turned[...], blocks[device, c, 1], preferred_element_type=jnp.float32
        ).astype(BF)
        up_buf[spread, :] = jnp.dot(
            turned[...], blocks[device, c, 2], preferred_element_type=jnp.float32
        ).astype(BF)

    def grads_for(b, found):
        devices, chunk = [d for d, _ in found], [c for _, c in found]

        def step(n, _):
            (down_grads, side_grads)[b](pick(devices, n), pick(chunk, n))
            return 0

        lax.fori_loop(0, len(found), step, 0)

    def relays(b):
        for c in range(chunks):
            a_relay(b, c)
            found = [(left, c), (right, c)]
            if c > 0:
                a_relayed(b, c - 1)
                found += [(other(left), c - 1), (other(right), c - 1)]
            grads_for(b, found)
        a_relayed(b, chunks - 1)
        grads_for(b, [(other(left), chunks - 1), (other(right), chunks - 1)])

    for c in range(chunks):
        a_relay(0, c)
    take(blocks.at[partner, :, pl.ds(0, 1)], a_own.at[0], {"tp": partner})
    take(blocks.at[partner, :, pl.ds(1, 2)], a_own.at[1], {"tp": partner})
    for b in range(2):
        grads_for(b, [(d, c) for c in range(chunks) for d in (me, partner)])
    for c in range(chunks):
        a_relayed(0, c)
    grads_for(0, [(d, c) for c in range(chunks) for d in (left, right, other(left), other(right))])
    relays(1)

    take(inner_in.at[pl.ds(0, groups - 1)], recv.at[1], {"ep": planes[1]})
    lane = lax.broadcasted_iota(jnp.int32, (tok_rows, LANES), 1)
    lane_value = lane.astype(jnp.float32)
    columns = jnp.transpose(table[...])[0:tok_rows, :]
    choice = (columns[:, 0:1], columns[:, 1:2])
    weight = (columns[:, 2:3], columns[:, 3:4])
    member = jnp.where((choice[0] == lane_value) | (choice[1] == lane_value), 1.0, 0.0)
    first = lax.broadcasted_iota(jnp.int32, (tok_rows, tok_rows), 0)
    second = lax.broadcasted_iota(jnp.int32, (tok_rows, tok_rows), 1)
    before = jnp.dot(
        jnp.where(second < first, 1.0, 0.0).astype(BF),
        member.astype(BF),
        preferred_element_type=jnp.float32,
    )
    inner = jnp.zeros((tok_rows, LANES), jnp.float32)
    takers = []
    slot = lax.broadcasted_iota(jnp.int32, (tok_rows, rows), 1).astype(jnp.float32)
    for k in range(2):
        rank = jnp.sum(jnp.where(lane_value == choice[k], before, 0.0), axis=1, keepdims=True)
        takers.append(jnp.where(slot == choice[k] * capacity + rank, 1.0, 0.0).astype(BF))
        value = jnp.zeros((tok_rows, LANES), jnp.float32)
        for p in range(groups):
            value = value + jnp.where((lane_value == rank) & (choice[k] == p), inner_in[p][0:1, :], 0.0)
        value = jnp.sum(value, axis=1, keepdims=True) / weight[k]
        inner = inner + jnp.where(lane == k, value, 0.0)
    if tok_rows < LANES:
        inner = jnp.concatenate([inner, jnp.zeros((LANES - tok_rows, LANES), jnp.float32)], axis=0)
    products[me] = jnp.transpose(inner)[0:8, :]
    for d in range(1, size):
        far_copy(
            products.at[me], products.at[me], send.at[6], recv.at[2], {"tp": (me + d) % size}
        ).start()

    take(back.at[:, pl.ds(0, rows - capacity), :], recv.at[0], {"ep": planes[1]})
    for n in range(chips // 2):
        cut = slice(n * wide, (n + 1) * wide)
        mix = weight[0] * jnp.dot(takers[0], back[0, :, cut], preferred_element_type=jnp.float32)
        mix = mix + weight[1] * jnp.dot(
            takers[1], back[0, :, cut], preferred_element_type=jnp.float32
        )
        grads = jnp.dot(takers[0] + takers[1], back[1, :, cut], preferred_element_type=jnp.float32)
        for j in range(2):
            o = 2 * n + j
            ready[o, 0] = mix[:, j * width : (j + 1) * width].astype(BF)
            ready[o, 1] = grads[:, j * width : (j + 1) * width].astype(BF)
            if o < chips - 1:
                far_copy(
                    ready.at[o], got.at[o], send.at[7], recv.at[3], {"tp": at(turns[o])}
                ).start()

    for b in range(2):
        for c in range(chunks):
            a_last(b, c)
            if c > 0:
                a_lasted(b, c - 1)
                grads_for(b, [(across, c), (other(across), c - 1)])
            else:
                grads_for(b, [(across, c)])
        a_lasted(b, chunks - 1)
        grads_for(b, [(other(across), chunks - 1)])

    take(products.at[pl.ds(0, size - 1)], recv.at[2], {"tp": partner})
    summed = products[0]
    for d in range(1, size):
        summed = summed + products[d]
    grad_combine[...] = summed[0:2, 0:tok_rows]

    take(got, recv.at[3], {"tp": right})
    for a, out in ((0, mixed), (1, grad_tokens)):
        value = ready[chips - 1, a].astype(jnp.float32)
        for o in range(chips - 1):
            value = value + got[o, a].astype(jnp.float32)
        out[...] = value.astype(BF)

    def sent(block, n):
        far_copy(block, block, send.at[n], recv.at[0], {"tp": partner}).wait_send()

    sent(out_rows.at[pl.ds(0, groups - 1)], 0)
    sent(both.at[:, :, pl.ds(0, (chips + 3) * width)], 1)
    sent(blocks.at[pl.ds(0, chips + 3)], 2)
    sent(part.at[:, 0], 3)
    sent(back.at[:, pl.ds(0, rows - capacity), :], 4)
    sent(inner_out.at[pl.ds(0, groups - 1)], 5)
    sent(products.at[pl.ds(0, size - 1)], 6)
    sent(ready.at[pl.ds(0, chips - 1)], 7)


def layer(ids_t, weights_t, tokens, cotangent, w_gate, w_up, w_down, capacity):
    size, groups = lax.axis_size("tp"), lax.axis_size("ep")
    chips = size // 2
    tok_rows, width = tokens.shape
    model, hidden = w_gate.shape
    chunks = hidden // CHUNK
    rows = groups * capacity
    whole, any_place = pl.BlockSpec(memory_space=pltpu.VMEM), pl.BlockSpec(memory_space=pl.ANY)
    dma = pltpu.SemaphoreType.DMA
    return pl.pallas_call(
        functools.partial(layer_kernel, chips, groups, capacity),
        out_shape=[
            pltpu.VMEM((chunks * model, CHUNK), BF),
            pltpu.VMEM((chunks * model, CHUNK), BF),
            pltpu.VMEM((chips * hidden, 2 * width), BF),
            pltpu.VMEM((tok_rows, width), BF),
            pltpu.VMEM((tok_rows, width), BF),
            pltpu.VMEM((2, tok_rows), jnp.float32),
        ],
        in_specs=[any_place] * 7,
        out_specs=[whole] * 6,
        scratch_shapes=[
            pltpu.VMEM((size, chunks, 3, rows, CHUNK), BF),
            pltpu.VMEM((2, rows, model), BF),
            pltpu.VMEM((groups, 2, capacity, width), BF),
            pltpu.VMEM((2, chunks, rows, CHUNK), jnp.float32),
            pltpu.VMEM((2, 2, chips, rows, width), BF),
            pltpu.VMEM((2, chips, rows, width), BF),
            pltpu.VMEM((2, chips, rows, width), BF),
            pltpu.VMEM((2, rows, chips * width), BF),
            pltpu.VMEM((chips, 2, tok_rows, width), BF),
            pltpu.VMEM((chips - 1, 2, tok_rows, width), BF),
            pltpu.VMEM((width, rows), BF),
            pltpu.VMEM((rows, LANES), jnp.float32),
            pltpu.VMEM((groups, 8, LANES), jnp.float32),
            pltpu.VMEM((groups, 8, LANES), jnp.float32),
            pltpu.VMEM((size, 8, LANES), jnp.float32),
            pltpu.VMEM((LANES, LANES), jnp.float32),
            pltpu.VMEM((2, tok_rows), jnp.int32),
            pltpu.VMEM((2, tok_rows), jnp.float32),
            pltpu.VMEM((tok_rows, width), BF),
            pltpu.VMEM((tok_rows, width), BF),
            dma((4,)),
            dma((3,)),
            dma((2, groups)),
            dma((2, 2, groups)),
            dma((2, groups)),
            dma((2,)),
            dma((2, 2, chunks)),
            dma((2, chunks)),
            dma((2,)),
            dma((2, 2, chunks)),
            dma((2, chips)),
            dma((4,)),
            dma((8,)),
        ],
        compiler_params=pltpu.CompilerParams(
            collective_id=0, has_side_effects=True, vmem_limit_bytes=44 << 20
        ),
        name="layer",
    )(ids_t, weights_t, tokens, cotangent, w_gate, w_up, w_down)


def place_kernel(gate_buf, up_buf, down_buf, *refs):
    small, (gate, up, down), outs, sems = refs[:3], refs[3:6], refs[6:9], refs[9]
    width = gate.shape[0]
    count = gate.shape[1] // CHUNK
    for n in range(count):
        cut, spread = pl.ds(n * CHUNK, CHUNK), pl.ds(n * width, width)
        pltpu.make_async_copy(gate_buf.at[spread, :], gate.at[:, cut], sems.at[0]).start()
        pltpu.make_async_copy(up_buf.at[spread, :], up.at[:, cut], sems.at[1]).start()
        block = down_buf.at[pl.ds(n // 2 * CHUNK, CHUNK), pl.ds(n % 2 * width, width)]
        pltpu.make_async_copy(block, down.at[cut, :], sems.at[2]).start()
    for n in range(3):
        pltpu.make_async_copy(small[n], outs[n], sems.at[3 + n]).start()
    for n in range(3):
        pltpu.make_async_copy(small[n], outs[n], sems.at[3 + n]).wait()
    for n, result in enumerate((gate, up, down)):
        pltpu.make_async_copy(result, result, sems.at[n]).wait()


def place_results(gate_buf, up_buf, down_buf, mixed, grad_tokens, grad_combine):
    tok_rows, width = mixed.shape
    hidden = gate_buf.shape[0] // width * CHUNK
    whole, any_place = pl.BlockSpec(memory_space=pltpu.VMEM), pl.BlockSpec(memory_space=pl.ANY)
    return pl.pallas_call(
        place_kernel,
        out_shape=[
            jax.ShapeDtypeStruct((width, hidden), BF),
            jax.ShapeDtypeStruct((width, hidden), BF),
            jax.ShapeDtypeStruct((hidden, width), BF),
            jax.ShapeDtypeStruct((tok_rows, width), BF),
            jax.ShapeDtypeStruct((tok_rows, width), BF),
            jax.ShapeDtypeStruct((2, tok_rows), jnp.float32),
        ],
        in_specs=[whole] * 6,
        out_specs=[any_place] * 6,
        scratch_shapes=[pltpu.SemaphoreType.DMA((6,))],
        compiler_params=pltpu.CompilerParams(vmem_limit_bytes=4 << 20),
        name="place_results",
    )(gate_buf, up_buf, down_buf, mixed, grad_tokens, grad_combine)


def body(tokens, cotangent, expert_ids, combine_weights, w_gate, w_up, w_down):
    if not fast_form(tokens, expert_ids, w_gate):
        return general_body(tokens, cotangent, expert_ids, combine_weights, w_gate, w_up, w_down)
    tok_rows, chosen = expert_ids.shape
    capacity = tok_rows * chosen * 5 // (3 * lax.axis_size("ep"))
    held = layer(
        expert_ids.T, combine_weights.T, tokens, cotangent, w_gate[0], w_up[0], w_down[0], capacity
    )
    gate, up, down, mixed, grad_tokens, grad_combine = place_results(*held)
    return mixed, grad_tokens, grad_combine.T, gate[None], up[None], down[None]


def solution(mesh):
    placed = (
        P("ep", "tp"),
        P("ep", "tp"),
        P("ep", None),
        P("ep", None),
        P("ep", None, "tp"),
        P("ep", None, "tp"),
        P("ep", "tp", None),
    )
    return jax.shard_map(
        body,
        mesh=mesh,
        in_specs=placed,
        out_specs=(
            P("ep", "tp"),
            P("ep", "tp"),
            P("ep", None),
            P("ep", "tp", None),
            P("ep", "tp", None),
            P("ep", None, "tp"),
        ),
        check_vma=False,
    )
```

```python
import functools
import math

import jax
import jax.numpy as jnp
from jax import lax
from jax.experimental import pallas as pl
from jax.experimental.pallas import tpu as pltpu
from jax.sharding import PartitionSpec as P

MESH = pl.DeviceIdType.MESH
BF = jnp.bfloat16


def ring_order(chips):
    side_x = math.isqrt(chips)
    side_x = side_x if side_x * side_x == chips else chips // 2
    side_y = chips // side_x
    order = [x for x in range(side_x)]
    for y in range(1, side_y):
        xs = range(side_x - 1, 0, -1) if y % 2 else range(1, side_x)
        order += [y * side_x + x for x in xs]
    order += [y * side_x for y in range(side_y - 1, 0, -1)]
    return order


def pick(table, index):
    value = jnp.int32(table[0])
    for i in range(1, len(table)):
        value = jnp.where(index == i, jnp.int32(table[i]), value)
    return value


def remote(src, dst, send, recv, device):
    return pltpu.make_async_remote_copy(
        src_ref=src,
        dst_ref=dst,
        send_sem=send,
        recv_sem=recv,
        device_id={"tp": device},
        device_id_type=MESH,
    )


def greet(devices):
    barrier = pltpu.get_barrier_semaphore()
    for device in devices:
        pl.semaphore_signal(barrier, inc=1, device_id={"tp": device}, device_id_type=MESH)
    pl.semaphore_wait(barrier, len(devices))


def gather_kernel(count, chips, *refs):
    own, out = refs[:count], refs[count : 2 * count]
    ring_send, ring_recv, core_send, core_recv, keep = refs[2 * count :]
    order = ring_order(chips)
    place = [order.index(chip) for chip in range(chips)]
    me = lax.axis_index("tp")
    chip, core = me // 2, me % 2
    spot = pick(place, chip)
    partner = chip * 2 + 1 - core
    steps = chips // 2
    rows = own[0].shape[0]
    half = rows // 2

    def at(offset):
        return pick(order, (spot + offset + chips) % chips) * 2 + core

    right, left = at(1), at(-1)
    greet([right, left, partner])

    def part(ref, way, step):
        if step < steps - 1:
            return ref
        return ref.at[pl.ds(way * half, half)]

    def hop(k, way, step):
        index = at(-step if way == 0 else step)
        source = own[k] if step == 0 else out[k].at[index]
        return remote(
            part(source, way, step),
            part(out[k].at[index], way, step),
            ring_send.at[k, way, step],
            ring_recv.at[k, way, step],
            right if way == 0 else left,
        )

    def arrived(k, way, step):
        index = at(-(step + 1) if way == 0 else step + 1)
        block = part(out[k].at[index], way, step)
        return remote(
            block, block, ring_send.at[k, way, step], ring_recv.at[k, way, step], right if way == 0 else left
        ), remote(
            block, block, core_send.at[k, way, step], core_recv.at[k, way, step], partner
        )

    def own_pass(k):
        return remote(
            own[k], out[k].at[me], core_send.at[k, 2, 0], core_recv.at[k, 2, 0], partner
        )

    def own_keep(k):
        return pltpu.make_async_copy(own[k], out[k].at[me], keep.at[k])

    for k in range(count):
        for way in range(2):
            hop(k, way, 0).start()
    for k in range(count):
        own_pass(k).start()
        own_keep(k).start()
    for step in range(steps):
        for k in range(count):
            for way in range(2):
                landed, handed = arrived(k, way, step)
                landed.wait_recv()
                if step + 1 < steps:
                    hop(k, way, step + 1).start()
                handed.start()
    for k in range(count):
        own_keep(k).wait()
        own_pass(k).wait_send()
        other = remote(
            own[k], out[k].at[partner], core_send.at[k, 2, 0], core_recv.at[k, 2, 0], partner
        )
        other.wait_recv()
        for way in range(2):
            for step in range(steps):
                hop(k, way, step).wait_send()
                handed = arrived(k, way, step)[1]
                handed.wait_send()
                index = at(-(step + 1) if way == 0 else step + 1) // 2 * 2 + 1 - core
                block = part(out[k].at[index], way, step)
                remote(
                    block, block, core_send.at[k, way, step], core_recv.at[k, way, step], partner
                ).wait_recv()


def gather(arrays, ident):
    size = lax.axis_size("tp")
    chips, count = size // 2, len(arrays)
    ring = pltpu.SemaphoreType.DMA((count, 2, chips // 2))
    cores = pltpu.SemaphoreType.DMA((count, 3, chips // 2))
    return pl.pallas_call(
        functools.partial(gather_kernel, count, chips),
        out_shape=[jax.ShapeDtypeStruct((size,) + a.shape, a.dtype) for a in arrays],
        in_specs=[pl.BlockSpec(memory_space=pltpu.VMEM)] * count,
        out_specs=[pl.BlockSpec(memory_space=pl.ANY)] * count,
        scratch_shapes=[ring, ring, cores, cores, pltpu.SemaphoreType.DMA((count,))],
        compiler_params=pltpu.CompilerParams(collective_id=ident, has_side_effects=True),
        name=f"gather_{ident}",
    )(*arrays)


def reduce_kernel(count, chips, *refs):
    part, out = refs[:count], refs[count : 2 * count]
    pre, stage, got = refs[2 * count : 5 * count : 3], refs[2 * count + 1 : 5 * count : 3], refs[2 * count + 2 : 5 * count : 3]
    core_send, core_recv, chip_send, chip_recv = refs[5 * count :]
    me = lax.axis_index("tp")
    chip, core = me // 2, me % 2
    partner = chip * 2 + 1 - core
    away = [(chip + o) % chips for o in range(1, chips)]
    greet([partner] + [other * 2 + core for other in away])

    def swap(k):
        return remote(part[k].at[1 - core], pre[k], core_send.at[k], core_recv.at[k], partner)

    def ship(k, o):
        return remote(
            stage[k].at[away[o]], got[k].at[o], chip_send.at[k, o], chip_recv.at[k, o], away[o] * 2 + core
        )

    for k in range(count):
        swap(k).start()
    for k in range(count):
        swap(k).wait()

        def add(q, _):
            stage[k][q] = (
                part[k][core, q].astype(jnp.float32) + pre[k][q].astype(jnp.float32)
            ).astype(BF)
            return 0

        lax.fori_loop(0, chips, add, 0)
        for o in range(chips - 1):
            ship(k, o).start()
    for k in range(count):
        for o in range(chips - 1):
            ship(k, o).wait()
        total = stage[k][chip].astype(jnp.float32)
        for o in range(chips - 1):
            total = total + got[k][o].astype(jnp.float32)
        out[k][...] = total.astype(BF)


def reduce_pieces(partials, ident):
    size = lax.axis_size("tp")
    chips, count = size // 2, len(partials)
    rows, width = partials[0].shape[0], partials[0].shape[1] // size
    cut = [p.reshape(rows, chips, 2, width).transpose(2, 1, 0, 3) for p in partials]
    held = pltpu.VMEM((chips, rows, width), BF)
    got = pltpu.VMEM((chips - 1, rows, width), BF)
    return pl.pallas_call(
        functools.partial(reduce_kernel, count, chips),
        out_shape=[jax.ShapeDtypeStruct((rows, width), BF)] * count,
        in_specs=[pl.BlockSpec(memory_space=pltpu.VMEM)] * count,
        out_specs=[pl.BlockSpec(memory_space=pltpu.VMEM)] * count,
        scratch_shapes=[held, held, got] * count
        + [pltpu.SemaphoreType.DMA((count,))] * 2
        + [pltpu.SemaphoreType.DMA((count, chips - 1))] * 2,
        compiler_params=pltpu.CompilerParams(
            collective_id=ident, has_side_effects=True, vmem_limit_bytes=48 << 20
        ),
        name=f"reduce_{ident}",
    )(*cut)


def rows_kernel(x_ref, g_ref, o_ref):
    o_ref[...] = jnp.dot(x_ref[...], g_ref[0], preferred_element_type=jnp.float32).astype(BF)


def row_grads(x_turned, blocks):
    features, rows = x_turned.shape
    size, _, hidden = blocks.shape
    return pl.pallas_call(
        rows_kernel,
        grid=(size,),
        out_shape=jax.ShapeDtypeStruct((features, size * hidden), BF),
        in_specs=[
            pl.BlockSpec((features, rows), lambda n: (0, 0)),
            pl.BlockSpec((1, rows, hidden), lambda n: (n, 0, 0)),
        ],
        out_specs=pl.BlockSpec((features, hidden), lambda n: (0, n)),
        name="row_grads",
        cost_estimate=pl.CostEstimate(
            flops=2 * features * rows * size * hidden,
            bytes_accessed=2 * size * hidden * (rows + features),
            transcendentals=0,
        ),
    )(x_turned, blocks)


def side_by_side(blocks):
    size, rows, width = blocks.shape
    return blocks.transpose(1, 0, 2).reshape(rows, size * width)


def silu_parts(gate_pre):
    sigma = jax.nn.sigmoid(gate_pre)
    return (gate_pre * sigma, sigma * (1.0 + gate_pre * (1.0 - sigma)))


def contract_rows(left, right):
    return lax.dot_general(
        left, right, (((0,), (0,)), ((), ())), preferred_element_type=jnp.float32
    )


def contract_cols(left, right):
    return lax.dot_general(
        left, right, (((1,), (1,)), ((), ())), preferred_element_type=jnp.float32
    )


def general_body(tokens, cotangent, expert_ids, combine_weights, w_gate, w_up, w_down):
    groups = lax.axis_size("ep")
    tok_rows, piece_width = tokens.shape
    chosen = expert_ids.shape[1]
    capacity = tok_rows * chosen * 5 // (3 * groups)
    buffer_rows = groups * capacity
    gate_weight = w_gate[0]
    up_weight = w_up[0]
    down_weight = w_down[0]
    flat_ids = expert_ids.reshape(-1)
    onehot = (flat_ids[:, None] == jnp.arange(groups, dtype=jnp.int32)[None, :]).astype(jnp.int32)
    rank = jnp.sum((jnp.cumsum(onehot, axis=0) - onehot) * onehot, axis=1)
    slot_index = flat_ids * capacity + rank
    places = (jnp.arange(buffer_rows, dtype=jnp.int32)[:, None] == slot_index[None, :]).astype(
        jnp.bfloat16
    )
    placer = jnp.sum(
        places.reshape(buffer_rows, tok_rows, chosen).astype(jnp.float32), axis=2
    ).astype(jnp.bfloat16)
    scaled = (combine_weights[:, :, None] * cotangent[:, None, :].astype(jnp.float32)).astype(
        jnp.bfloat16
    )
    send_grad = jnp.dot(
        places, scaled.reshape(tok_rows * chosen, piece_width), preferred_element_type=jnp.float32
    ).astype(jnp.bfloat16)
    send_rows = jnp.dot(placer, tokens, preferred_element_type=jnp.float32).astype(jnp.bfloat16)
    recv_rows, recv_grad = (
        lax.all_to_all(
            send_rows.reshape(groups, capacity, piece_width),
            "ep",
            split_axis=0,
            concat_axis=0,
            tiled=True,
        ),
        lax.all_to_all(
            send_grad.reshape(groups, capacity, piece_width),
            "ep",
            split_axis=0,
            concat_axis=0,
            tiled=True,
        ),
    )
    recv_rows = recv_rows.reshape(buffer_rows, piece_width)
    recv_grad = recv_grad.reshape(buffer_rows, piece_width)
    x_blocks, dy_blocks = gather([recv_rows, recv_grad], 0)
    piece, dy_full = side_by_side(x_blocks), side_by_side(dy_blocks)
    gate_pre = jnp.dot(piece, gate_weight, preferred_element_type=jnp.float32)
    up_pre = jnp.dot(piece, up_weight, preferred_element_type=jnp.float32)
    active, slope = silu_parts(gate_pre)
    hidden = (active * up_pre).astype(jnp.bfloat16)
    partial_value = jnp.dot(hidden, down_weight, preferred_element_type=jnp.float32)
    grad_hidden = contract_cols(dy_full, down_weight)
    grad_gate_pre = (grad_hidden * up_pre * slope).astype(jnp.bfloat16)
    grad_up_pre = (grad_hidden * active).astype(jnp.bfloat16)
    input_partial = contract_cols(grad_gate_pre, gate_weight) + contract_cols(
        grad_up_pre, up_weight
    )
    out_piece, input_piece = reduce_pieces(
        [partial_value.astype(jnp.bfloat16), input_partial.astype(jnp.bfloat16)], 1
    )
    hidden_in, gate_in, up_in, out_piece, input_piece = lax.optimization_barrier(
        (hidden, grad_gate_pre, grad_up_pre, out_piece, input_piece)
    )
    hidden_blocks, gate_blocks, up_blocks = gather([hidden_in, gate_in, up_in], 2)
    out_back = lax.all_to_all(
        out_piece.reshape(groups, capacity, piece_width),
        "ep",
        split_axis=0,
        concat_axis=0,
        tiled=True,
    ).reshape(buffer_rows, piece_width)
    out_tokens = (
        jnp.take(out_back, slot_index, axis=0)
        .reshape(tok_rows, chosen, piece_width)
        .astype(jnp.float32)
    )
    mixed = jnp.sum(combine_weights[:, :, None] * out_tokens, axis=1).astype(jnp.bfloat16)
    local_products = jnp.sum(cotangent.astype(jnp.float32)[:, None, :] * out_tokens, axis=2)
    grad_combine = lax.psum(local_products, "tp")
    input_back = lax.all_to_all(
        input_piece.reshape(groups, capacity, piece_width),
        "ep",
        split_axis=0,
        concat_axis=0,
        tiled=True,
    ).reshape(buffer_rows, piece_width)
    grad_tokens = jnp.sum(
        jnp.take(input_back, slot_index, axis=0)
        .reshape(tok_rows, chosen, piece_width)
        .astype(jnp.float32),
        axis=1,
    ).astype(jnp.bfloat16)
    down_cols_out = (
        jnp.einsum("nrh,rd->nhd", hidden_blocks, recv_grad, preferred_element_type=jnp.float32)
        .astype(jnp.bfloat16)
        .reshape(-1, piece_width)
    )
    x_turned = recv_rows.T
    gate_rows_out = row_grads(x_turned, gate_blocks)
    up_rows_out = row_grads(x_turned, up_blocks)
    return (
        mixed,
        grad_tokens,
        grad_combine,
        gate_rows_out[None],
        up_rows_out[None],
        down_cols_out[None],
    )


CHUNK = 256
LANES = 128


def fast_form(tokens, expert_ids, w_gate):
    groups, size = lax.axis_size("ep"), lax.axis_size("tp")
    tok_rows, width = tokens.shape
    hidden = w_gate.shape[2]
    capacity = tok_rows * expert_ids.shape[1] * 5 // (3 * groups)
    return (
        size == 8
        and expert_ids.shape[1] == 2
        and 3 <= groups <= 8
        and width % LANES == 0
        and hidden % CHUNK == 0
        and capacity % 16 == 0
        and capacity <= LANES
        and groups * capacity % 32 == 0
        and tok_rows <= LANES
        and tok_rows % 16 == 0
    )


def far_copy(src, dst, send, recv, device):
    return pltpu.make_async_remote_copy(
        src_ref=src, dst_ref=dst, send_sem=send, recv_sem=recv, device_id=device, device_id_type=MESH
    )


def layer_kernel(
    chips,
    groups,
    capacity,
    ids_hbm,
    weights_hbm,
    tokens_hbm,
    cotangent_hbm,
    wg_hbm,
    wu_hbm,
    wd_hbm,
    gate_buf,
    up_buf,
    down_buf,
    mixed,
    grad_tokens,
    grad_combine,
    blocks,
    both,
    out_rows,
    dy_rows,
    cots,
    factors,
    part,
    pre,
    stage,
    back,
    ready,
    got,
    turned,
    inner_sum,
    inner_out,
    inner_in,
    products,
    table,
    ids_t,
    weights_t,
    tokens,
    cotangent,
    in_sem,
    w_sem,
    z_recv,
    x_side,
    x_far,
    x_pass,
    a_side,
    a_far,
    a_own,
    a_pass,
    s_recv,
    recv,
    send,
):
    size = 2 * chips
    tok_rows, width = tokens.shape
    rows = groups * capacity
    model = size * width
    hidden = wg_hbm.shape[1]
    chunks = hidden // CHUNK
    wide = 2 * width
    order = ring_order(chips)
    place = [order.index(chip) for chip in range(chips)]
    me = lax.axis_index("tp")
    group = lax.axis_index("ep")
    chip, core = me // 2, me % 2
    spot = pick(place, chip)
    partner = chip * 2 + 1 - core

    def at(offset):
        return pick(order, (spot + offset + chips) % chips) * 2 + core

    right, left, across = at(1), at(-1), at(2)
    sides = (right, left)

    def other(device):
        return device // 2 * 2 + 1 - core

    near = [sorted(range(groups), key=lambda s: (abs(s - g), s)) for g in range(groups)]
    planes = [pick([near[g][k] for g in range(groups)], group) for k in range(groups)]

    def rows_of(s):
        return pl.ds(pl.multiple_of(s * capacity, 16), capacity)

    def cols_of(device):
        return pl.ds(pl.multiple_of(device * width, LANES), width)

    def take(block, sem, device):
        far_copy(block, block, send.at[0], sem, device).wait_recv()

    barrier = pltpu.get_barrier_semaphore()
    for k in range(1, groups):
        pl.semaphore_signal(barrier, inc=1, device_id={"ep": planes[k]}, device_id_type=MESH)
    for d in range(1, size):
        pl.semaphore_signal(barrier, inc=1, device_id={"tp": (me + d) % size}, device_id_type=MESH)

    inputs = (
        (ids_hbm, ids_t),
        (weights_hbm, weights_t),
        (tokens_hbm, tokens),
        (cotangent_hbm, cotangent),
    )
    inputs = [pltpu.make_async_copy(a, b, in_sem.at[n]) for n, (a, b) in enumerate(inputs)]
    for copy in inputs:
        copy.start()
    for copy in inputs:
        copy.wait()
    row_id = lax.broadcasted_iota(jnp.int32, (8, tok_rows), 0)
    member_t = jnp.where((ids_t[0:1, :] == row_id) | (ids_t[1:2, :] == row_id), 1.0, 0.0)
    first = lax.broadcasted_iota(jnp.int32, (tok_rows, tok_rows), 0)
    second = lax.broadcasted_iota(jnp.int32, (tok_rows, tok_rows), 1)
    before_t = jnp.dot(
        member_t.astype(BF),
        jnp.where(first < second, 1.0, 0.0).astype(BF),
        preferred_element_type=jnp.float32,
    )
    table[...] = jnp.zeros((LANES, LANES), jnp.float32)
    table[0:2, 0:tok_rows] = ids_t[...].astype(jnp.float32)
    table[2:4, 0:tok_rows] = weights_t[...]
    columns = jnp.transpose(table[...])[0:tok_rows, :]
    choice = (columns[:, 0:1], columns[:, 1:2])
    weight = (columns[:, 2:3], columns[:, 3:4])
    slot_t = lax.broadcasted_iota(jnp.int32, (capacity, tok_rows), 0).astype(jnp.float32)
    for p in range(groups):
        placer = (
            jnp.where(slot_t == before_t[p : p + 1, :], 1.0, 0.0) * member_t[p : p + 1, :]
        ).astype(BF)
        out_rows[p] = jnp.dot(placer, tokens[...], preferred_element_type=jnp.float32).astype(BF)

    pl.semaphore_wait(barrier, size + groups - 2)


    for k in range(groups - 1, 0, -1):
        far_copy(
            out_rows.at[planes[k]],
            both.at[0, rows_of(group), cols_of(me)],
            send.at[0],
            z_recv.at[0, group],
            {"ep": planes[k]},
        ).start()
    for target in (across, right, left):
        far_copy(cotangent, cots.at[chip], send.at[8], recv.at[4], {"tp": target}).start()
    cots[chip] = cotangent[...]

    def x_block(a, k, device):
        return both.at[a, rows_of(planes[k]), cols_of(device)]

    def x_send(a, k, device, sem, target):
        block = x_block(a, k, device)
        far_copy(block, block, send.at[1], sem, {"tp": target}).start()

    def side_of(k):
        return 0 if k < 2 else 2

    def x_first(k):
        if k == 0:
            both[0, rows_of(group), cols_of(me)] = out_rows[group]
        else:
            take(x_block(0, k, me), z_recv.at[0, planes[k]], {"ep": planes[k]})
        for way in range(2):
            x_send(0, k, me, x_side.at[way, k], sides[way])
        if k > 0:
            x_send(0, k, me, x_far.at[k], across)
        x_send(0, k, me, x_pass.at[side_of(k)], partner)

    def x_relay(k):
        for way in range(2):
            origin = sides[1 - way]
            take(x_block(0, k, origin), x_side.at[way, k], {"tp": origin})
            if k == 0 and way == 0:
                x_send(0, k, origin, x_far.at[k], sides[way])
            x_send(0, k, origin, x_pass.at[side_of(k)], partner)

    def x_last(k):
        take(x_block(0, k, across), x_far.at[k], {"tp": across})
        x_send(0, k, across, x_pass.at[side_of(k)], partner)

    def dy_pass(k):
        for q in range(chips):
            x_send(1, k, q * 2 + core, x_pass.at[1], partner)

    def dy_first():
        take(cots.at[pl.ds(0, chips - 1)], recv.at[4], {"tp": across})
        for p in range(groups):
            placer = (
                jnp.where(slot_t == before_t[p : p + 1, :], 1.0, 0.0) * member_t[p : p + 1, :]
            ).astype(BF)
            own_weight = jnp.where(choice[0] == p, weight[0], 0.0) + jnp.where(
                choice[1] == p, weight[1], 0.0
            )
            for q in range(chips):
                scaled = (own_weight * cots[q].astype(jnp.float32)).astype(BF)
                dy_rows[p, q] = jnp.dot(placer, scaled, preferred_element_type=jnp.float32).astype(BF)
        for k in range(1, groups):
            for q in range(chips):
                far_copy(
                    dy_rows.at[planes[k], q],
                    both.at[1, rows_of(group), cols_of(q * 2 + core)],
                    send.at[9],
                    z_recv.at[1, group],
                    {"ep": planes[k]},
                ).start()
        for q in range(chips):
            both[1, rows_of(group), cols_of(q * 2 + core)] = dy_rows[group, q]
        dy_pass(0)

    def dy_next(k):
        take(
            both.at[1, rows_of(planes[k]), pl.ds(0, chips * width)],
            z_recv.at[1, planes[k]],
            {"ep": planes[k]},
        )
        dy_pass(k)

    def x_whole(a, n, count):
        block = both.at[a, pl.ds(0, count * capacity), pl.ds(0, chips * width)]
        take(block, x_pass.at[n], {"tp": partner})

    def fetch(n):
        source, target = ((wg_hbm, gate_buf), (wu_hbm, up_buf), (wd_hbm, down_buf))[n]
        if n < 2:
            for c in range(chunks):
                pltpu.make_async_copy(
                    source.at[:, pl.ds(c * CHUNK, CHUNK)],
                    target.at[pl.ds(c * model, model), :],
                    w_sem.at[n],
                ).start()
        else:
            for q in range(chips):
                pltpu.make_async_copy(
                    source.at[:, pl.ds(q * wide, wide)],
                    target.at[pl.ds(q * hidden, hidden), :],
                    w_sem.at[n],
                ).start()

    def fetched(n):
        target = (gate_buf, up_buf, down_buf)[n]
        pltpu.make_async_copy(target, target, w_sem.at[n]).wait()

    x_first(0)
    for n in range(3):
        fetch(n)
    x_relay(0)
    x_first(1)
    x_last(0)
    x_first(2)
    dy_first()
    x_relay(1)
    x_last(1)
    for k in range(3, groups):
        x_first(k)
    x_whole(0, 0, 2)
    for n in range(3):
        fetched(n)

    half = rows // 2
    kinds = ((0, 1), (1, 2))

    def a_block(b, c, device, way=None):
        start, count = kinds[b]
        if way is None:
            return blocks.at[device, c, pl.ds(start, count)]
        return blocks.at[device, c, pl.ds(start, count), pl.ds(way * half, half), :]

    def a_send(b, c, device, sem, target, way=None):
        block = a_block(b, c, device, way)
        far_copy(block, block, send.at[2], sem, {"tp": target}).start()

    def a_first(b, c):
        for way in range(2):
            a_send(b, c, me, a_side.at[b, way, c], sides[way])
        a_send(b, c, me, a_own.at[b], partner)

    def a_relay(b, c):
        for way in range(2):
            origin = sides[1 - way]
            take(a_block(b, c, origin), a_side.at[b, way, c], {"tp": origin})
            a_send(b, c, origin, a_far.at[b, c], sides[way], way)
            a_send(b, c, origin, a_pass.at[b, 0, c], partner)

    def a_relayed(b, c):
        start, count = kinds[b]
        take(blocks.at[pl.ds(0, 2), c, pl.ds(start, count)], a_pass.at[b, 0, c], {"tp": partner})

    def a_last(b, c):
        take(a_block(b, c, across), a_far.at[b, c], {"tp": left})
        a_send(b, c, across, a_pass.at[b, 1, c], partner)

    def a_lasted(b, c):
        take(a_block(b, c, other(across)), a_pass.at[b, 1, c], {"tp": partner})

    def hidden_rows(c, k):
        spread = pl.ds(c * model, model)
        cut = rows_of(planes[k])
        held = both[0, cut, :]
        gate_pre = jnp.dot(held, gate_buf[spread, :], preferred_element_type=jnp.float32)
        up_pre = jnp.dot(held, up_buf[spread, :], preferred_element_type=jnp.float32)
        active, slope = silu_parts(gate_pre)
        blocks[me, c, 0, cut, :] = (active * up_pre).astype(BF)
        block = blocks.at[me, c, pl.ds(0, 1), cut, :]
        for way in range(2):
            far_copy(block, block, send.at[2], a_side.at[0, way, c], {"tp": sides[way]}).start()
        far_copy(block, block, send.at[2], a_own.at[0], {"tp": partner}).start()
        factors[0, c, cut, :] = up_pre * slope
        factors[1, c, cut, :] = active

    turns = [2, 1, chips - 1, 0]

    def swap(a, o, value):
        part[a, 0, o] = value[:, :width].astype(BF)
        part[a, 1, o] = value[:, width:].astype(BF)
        far_copy(
            part.at[a, 1 - core, o], pre.at[a, o], send.at[3], s_recv.at[a, o], {"tp": partner}
        ).start()

    def out_part(o, _):
        q = pick(order, (spot + pick(turns, o)) % chips)
        value = None
        for c in range(chunks):
            cut = pl.ds(pl.multiple_of(q * hidden + c * CHUNK, CHUNK), CHUNK)
            term = jnp.dot(blocks[me, c, 0], down_buf[cut, :], preferred_element_type=jnp.float32)
            value = term if c == 0 else value + term
        swap(0, o, value)
        return 0

    def in_part(o, _):
        q = pick(order, (spot + pick(turns, o)) % chips)
        value = None
        for c in range(chunks):
            cut = pl.ds(pl.multiple_of(c * model + q * wide, LANES), wide)
            term = contract_cols(blocks[me, c, 1], gate_buf[cut, :]) + contract_cols(
                blocks[me, c, 2], up_buf[cut, :]
            )
            value = term if c == 0 else value + term
        swap(1, o, value)
        return 0

    def spread_parts(a):
        for o in range(chips):
            take(pre.at[a, o], s_recv.at[a, o], {"tp": partner})

            def add(s, _):
                cut = rows_of(s)
                stage[a, o, cut, :] = (
                    part[a, core, o, cut, :].astype(jnp.float32) + pre[a, o, cut, :].astype(jnp.float32)
                ).astype(BF)
                return 0

            lax.fori_loop(0, groups, add, 0)
            for k in range(groups - 1, 0, -1):
                far_copy(
                    stage.at[a, o, rows_of(planes[k]), :],
                    back.at[a, rows_of(group), pl.ds(o * width, width)],
                    send.at[4],
                    recv.at[0],
                    {"ep": planes[k]},
                ).start()
            back[a, rows_of(group), o * width : (o + 1) * width] = stage[a, o, rows_of(group), :]

    rest = [(x_relay, k) for k in range(2, groups)] + [(x_last, k) for k in range(2, groups)]
    done = 0
    for c in range(chunks):
        for k in range(2):
            hidden_rows(c, k)
        upto = len(rest) * (c + 1) // chunks
        for step, k in rest[done:upto]:
            step(k)
        done = upto
    x_whole(0, 2, groups - 2)
    for c in range(chunks):
        for k in range(2, groups):
            hidden_rows(c, k)
    lax.fori_loop(0, chips, out_part, 0)
    a_relay(0, 0)
    for k in range(1, groups):
        if k < chunks - 1:
            a_relay(0, k)
        dy_next(k)
    x_whole(1, 1, groups)
    spread_parts(0)
    inner_sum[...] = jnp.zeros((rows, LANES), jnp.float32)

    def grad_chunk(c, _):
        grad_hidden = None
        for q in range(chips):
            cut = pl.ds(pl.multiple_of(q * hidden + c * CHUNK, CHUNK), CHUNK)
            term = contract_cols(both[1, :, q * wide : (q + 1) * wide], down_buf[cut, :])
            grad_hidden = term if q == 0 else grad_hidden + term
        blocks[me, c, 1] = (grad_hidden * factors[0, c]).astype(BF)
        blocks[me, c, 2] = (grad_hidden * factors[1, c]).astype(BF)
        a_first(1, c)
        product = blocks[me, c, 0].astype(jnp.float32) * grad_hidden
        total = inner_sum[...]
        for n in range(CHUNK // LANES):
            total = total + product[:, n * LANES : (n + 1) * LANES]
        inner_sum[...] = total
        return 0

    lax.fori_loop(0, chunks, grad_chunk, 0)
    for c in range(max(1, min(groups, chunks - 1)), chunks):
        a_relay(0, c)

    lax.fori_loop(0, chips, in_part, 0)
    spread_parts(1)

    for p in range(groups):
        value = inner_sum[p * capacity : (p + 1) * capacity, :]
        if capacity < LANES:
            value = jnp.concatenate(
                [value, jnp.zeros((LANES - capacity, LANES), jnp.float32)], axis=0
            )
        value = jnp.sum(jnp.transpose(value), axis=0, keepdims=True)
        inner_out[p] = jnp.broadcast_to(value, (8, LANES))
    for k in range(1, groups):
        far_copy(
            inner_out.at[planes[k]], inner_in.at[group], send.at[5], recv.at[1], {"ep": planes[k]}
        ).start()
    inner_in[group] = inner_out[group]

    turned[...] = jnp.transpose(both[0, :, cols_of(me)].astype(jnp.float32)).astype(BF)

    def down_grads(device, c):
        place_of = device * chunks + c
        down_buf[
            pl.ds(pl.multiple_of(place_of // 2 * CHUNK, CHUNK), CHUNK),
            pl.ds(pl.multiple_of(place_of % 2 * width, LANES), width),
        ] = contract_rows(blocks[device, c, 0], both[1, :, cols_of(me)]).astype(BF)

    def side_grads(device, c):
        spread = pl.ds(pl.multiple_of((device * chunks + c) * width, LANES), width)
        gate_buf[spread, :] = jnp.dot(
            turned[...], blocks[device, c, 1], preferred_element_type=jnp.float32
        ).astype(BF)
        up_buf[spread, :] = jnp.dot(
            turned[...], blocks[device, c, 2], preferred_element_type=jnp.float32
        ).astype(BF)

    def grads_for(b, found):
        devices, chunk = [d for d, _ in found], [c for _, c in found]

        def step(n, _):
            (down_grads, side_grads)[b](pick(devices, n), pick(chunk, n))
            return 0

        lax.fori_loop(0, len(found), step, 0)

    def relays(b):
        for c in range(chunks):
            a_relay(b, c)
            found = [(left, c), (right, c)]
            if c > 0:
                a_relayed(b, c - 1)
                found += [(other(left), c - 1), (other(right), c - 1)]
            grads_for(b, found)
        a_relayed(b, chunks - 1)
        grads_for(b, [(other(left), chunks - 1), (other(right), chunks - 1)])

    take(blocks.at[partner, :, pl.ds(0, 1)], a_own.at[0], {"tp": partner})
    take(blocks.at[partner, :, pl.ds(1, 2)], a_own.at[1], {"tp": partner})
    for b in range(2):
        grads_for(b, [(d, c) for c in range(chunks) for d in (me, partner)])
    for c in range(chunks):
        a_relayed(0, c)
    grads_for(0, [(d, c) for c in range(chunks) for d in (left, right, other(left), other(right))])
    relays(1)

    take(inner_in.at[pl.ds(0, groups - 1)], recv.at[1], {"ep": planes[1]})
    lane = lax.broadcasted_iota(jnp.int32, (tok_rows, LANES), 1)
    lane_value = lane.astype(jnp.float32)
    columns = jnp.transpose(table[...])[0:tok_rows, :]
    choice = (columns[:, 0:1], columns[:, 1:2])
    weight = (columns[:, 2:3], columns[:, 3:4])
    member = jnp.where((choice[0] == lane_value) | (choice[1] == lane_value), 1.0, 0.0)
    first = lax.broadcasted_iota(jnp.int32, (tok_rows, tok_rows), 0)
    second = lax.broadcasted_iota(jnp.int32, (tok_rows, tok_rows), 1)
    before = jnp.dot(
        jnp.where(second < first, 1.0, 0.0).astype(BF),
        member.astype(BF),
        preferred_element_type=jnp.float32,
    )
    inner = jnp.zeros((tok_rows, LANES), jnp.float32)
    takers = []
    slot = lax.broadcasted_iota(jnp.int32, (tok_rows, rows), 1).astype(jnp.float32)
    for k in range(2):
        rank = jnp.sum(jnp.where(lane_value == choice[k], before, 0.0), axis=1, keepdims=True)
        takers.append(jnp.where(slot == choice[k] * capacity + rank, 1.0, 0.0).astype(BF))
        value = jnp.zeros((tok_rows, LANES), jnp.float32)
        for p in range(groups):
            value = value + jnp.where((lane_value == rank) & (choice[k] == p), inner_in[p][0:1, :], 0.0)
        value = jnp.sum(value, axis=1, keepdims=True) / weight[k]
        inner = inner + jnp.where(lane == k, value, 0.0)
    if tok_rows < LANES:
        inner = jnp.concatenate([inner, jnp.zeros((LANES - tok_rows, LANES), jnp.float32)], axis=0)
    products[me] = jnp.transpose(inner)[0:8, :]
    for d in range(1, size):
        far_copy(
            products.at[me], products.at[me], send.at[6], recv.at[2], {"tp": (me + d) % size}
        ).start()

    take(back.at[:, pl.ds(0, rows - capacity), :], recv.at[0], {"ep": planes[1]})
    for n in range(chips // 2):
        cut = slice(n * wide, (n + 1) * wide)
        mix = weight[0] * jnp.dot(takers[0], back[0, :, cut], preferred_element_type=jnp.float32)
        mix = mix + weight[1] * jnp.dot(
            takers[1], back[0, :, cut], preferred_element_type=jnp.float32
        )
        grads = jnp.dot(takers[0] + takers[1], back[1, :, cut], preferred_element_type=jnp.float32)
        for j in range(2):
            o = 2 * n + j
            ready[o, 0] = mix[:, j * width : (j + 1) * width].astype(BF)
            ready[o, 1] = grads[:, j * width : (j + 1) * width].astype(BF)
            if o < chips - 1:
                far_copy(
                    ready.at[o], got.at[o], send.at[7], recv.at[3], {"tp": at(turns[o])}
                ).start()

    for b in range(2):
        for c in range(chunks):
            a_last(b, c)
            if c > 0:
                a_lasted(b, c - 1)
                grads_for(b, [(across, c), (other(across), c - 1)])
            else:
                grads_for(b, [(across, c)])
        a_lasted(b, chunks - 1)
        grads_for(b, [(other(across), chunks - 1)])

    take(products.at[pl.ds(0, size - 1)], recv.at[2], {"tp": partner})
    summed = products[0]
    for d in range(1, size):
        summed = summed + products[d]
    grad_combine[...] = summed[0:2, 0:tok_rows]

    take(got, recv.at[3], {"tp": right})
    for a, out in ((0, mixed), (1, grad_tokens)):
        value = ready[chips - 1, a].astype(jnp.float32)
        for o in range(chips - 1):
            value = value + got[o, a].astype(jnp.float32)
        out[...] = value.astype(BF)

    def sent(block, n):
        far_copy(block, block, send.at[n], recv.at[0], {"tp": partner}).wait_send()

    sent(out_rows.at[pl.ds(0, groups - 1)], 0)
    sent(both.at[0, :, pl.ds(0, (chips + 3) * width)], 1)
    sent(both.at[1, :, pl.ds(0, chips * width)], 1)
    sent(cots.at[pl.ds(0, chips - 1)], 8)
    sent(dy_rows.at[pl.ds(0, groups - 1)], 9)
    sent(blocks.at[pl.ds(0, chips + 3)], 2)
    sent(part.at[:, 0], 3)
    sent(back.at[:, pl.ds(0, rows - capacity), :], 4)
    sent(inner_out.at[pl.ds(0, groups - 1)], 5)
    sent(products.at[pl.ds(0, size - 1)], 6)
    sent(ready.at[pl.ds(0, chips - 1)], 7)


def layer(ids_t, weights_t, tokens, cotangent, w_gate, w_up, w_down, capacity):
    size, groups = lax.axis_size("tp"), lax.axis_size("ep")
    chips = size // 2
    tok_rows, width = tokens.shape
    model, hidden = w_gate.shape
    chunks = hidden // CHUNK
    rows = groups * capacity
    whole, any_place = pl.BlockSpec(memory_space=pltpu.VMEM), pl.BlockSpec(memory_space=pl.ANY)
    dma = pltpu.SemaphoreType.DMA
    return pl.pallas_call(
        functools.partial(layer_kernel, chips, groups, capacity),
        out_shape=[
            pltpu.VMEM((chunks * model, CHUNK), BF),
            pltpu.VMEM((chunks * model, CHUNK), BF),
            pltpu.VMEM((chips * hidden, 2 * width), BF),
            pltpu.VMEM((tok_rows, width), BF),
            pltpu.VMEM((tok_rows, width), BF),
            pltpu.VMEM((2, tok_rows), jnp.float32),
        ],
        in_specs=[any_place] * 7,
        out_specs=[whole] * 6,
        scratch_shapes=[
            pltpu.VMEM((size, chunks, 3, rows, CHUNK), BF),
            pltpu.VMEM((2, rows, model), BF),
            pltpu.VMEM((groups, capacity, width), BF),
            pltpu.VMEM((groups, chips, capacity, width), BF),
            pltpu.VMEM((chips, tok_rows, width), BF),
            pltpu.VMEM((2, chunks, rows, CHUNK), jnp.float32),
            pltpu.VMEM((2, 2, chips, rows, width), BF),
            pltpu.VMEM((2, chips, rows, width), BF),
            pltpu.VMEM((2, chips, rows, width), BF),
            pltpu.VMEM((2, rows, chips * width), BF),
            pltpu.VMEM((chips, 2, tok_rows, width), BF),
            pltpu.VMEM((chips - 1, 2, tok_rows, width), BF),
            pltpu.VMEM((width, rows), BF),
            pltpu.VMEM((rows, LANES), jnp.float32),
            pltpu.VMEM((groups, 8, LANES), jnp.float32),
            pltpu.VMEM((groups, 8, LANES), jnp.float32),
            pltpu.VMEM((size, 8, LANES), jnp.float32),
            pltpu.VMEM((LANES, LANES), jnp.float32),
            pltpu.VMEM((2, tok_rows), jnp.int32),
            pltpu.VMEM((2, tok_rows), jnp.float32),
            pltpu.VMEM((tok_rows, width), BF),
            pltpu.VMEM((tok_rows, width), BF),
            dma((4,)),
            dma((3,)),
            dma((2, groups)),
            dma((2, groups)),
            dma((groups,)),
            dma((3,)),
            dma((2, 2, chunks)),
            dma((2, chunks)),
            dma((2,)),
            dma((2, 2, chunks)),
            dma((2, chips)),
            dma((5,)),
            dma((10,)),
        ],
        compiler_params=pltpu.CompilerParams(
            collective_id=0, has_side_effects=True, vmem_limit_bytes=44 << 20
        ),
        name="layer",
    )(ids_t, weights_t, tokens, cotangent, w_gate, w_up, w_down)


def place_kernel(gate_buf, up_buf, down_buf, *refs):
    small, (gate, up, down), outs, sems = refs[:3], refs[3:6], refs[6:9], refs[9]
    width = gate.shape[0]
    count = gate.shape[1] // CHUNK
    for n in range(count):
        cut, spread = pl.ds(n * CHUNK, CHUNK), pl.ds(n * width, width)
        pltpu.make_async_copy(gate_buf.at[spread, :], gate.at[:, cut], sems.at[0]).start()
        pltpu.make_async_copy(up_buf.at[spread, :], up.at[:, cut], sems.at[1]).start()
        block = down_buf.at[pl.ds(n // 2 * CHUNK, CHUNK), pl.ds(n % 2 * width, width)]
        pltpu.make_async_copy(block, down.at[cut, :], sems.at[2]).start()
    for n in range(3):
        pltpu.make_async_copy(small[n], outs[n], sems.at[3 + n]).start()
    for n in range(3):
        pltpu.make_async_copy(small[n], outs[n], sems.at[3 + n]).wait()
    for n, result in enumerate((gate, up, down)):
        pltpu.make_async_copy(result, result, sems.at[n]).wait()


def place_results(gate_buf, up_buf, down_buf, mixed, grad_tokens, grad_combine):
    tok_rows, width = mixed.shape
    hidden = gate_buf.shape[0] // width * CHUNK
    whole, any_place = pl.BlockSpec(memory_space=pltpu.VMEM), pl.BlockSpec(memory_space=pl.ANY)
    return pl.pallas_call(
        place_kernel,
        out_shape=[
            jax.ShapeDtypeStruct((width, hidden), BF),
            jax.ShapeDtypeStruct((width, hidden), BF),
            jax.ShapeDtypeStruct((hidden, width), BF),
            jax.ShapeDtypeStruct((tok_rows, width), BF),
            jax.ShapeDtypeStruct((tok_rows, width), BF),
            jax.ShapeDtypeStruct((2, tok_rows), jnp.float32),
        ],
        in_specs=[whole] * 6,
        out_specs=[any_place] * 6,
        scratch_shapes=[pltpu.SemaphoreType.DMA((6,))],
        compiler_params=pltpu.CompilerParams(vmem_limit_bytes=4 << 20),
        name="place_results",
    )(gate_buf, up_buf, down_buf, mixed, grad_tokens, grad_combine)


def body(tokens, cotangent, expert_ids, combine_weights, w_gate, w_up, w_down):
    if not fast_form(tokens, expert_ids, w_gate):
        return general_body(tokens, cotangent, expert_ids, combine_weights, w_gate, w_up, w_down)
    tok_rows, chosen = expert_ids.shape
    capacity = tok_rows * chosen * 5 // (3 * lax.axis_size("ep"))
    held = layer(
        expert_ids.T, combine_weights.T, tokens, cotangent, w_gate[0], w_up[0], w_down[0], capacity
    )
    gate, up, down, mixed, grad_tokens, grad_combine = place_results(*held)
    return mixed, grad_tokens, grad_combine.T, gate[None], up[None], down[None]


def solution(mesh):
    placed = (
        P("ep", "tp"),
        P("ep", "tp"),
        P("ep", None),
        P("ep", None),
        P("ep", None, "tp"),
        P("ep", None, "tp"),
        P("ep", "tp", None),
    )
    return jax.shard_map(
        body,
        mesh=mesh,
        in_specs=placed,
        out_specs=(
            P("ep", "tp"),
            P("ep", "tp"),
            P("ep", None),
            P("ep", "tp", None),
            P("ep", "tp", None),
            P("ep", None, "tp"),
        ),
        check_vma=False,
    )
```

```python
import functools
import math

import jax
import jax.numpy as jnp
from jax import lax
from jax.experimental import pallas as pl
from jax.experimental.pallas import tpu as pltpu
from jax.sharding import PartitionSpec as P

MESH = pl.DeviceIdType.MESH
BF = jnp.bfloat16


def ring_order(chips):
    side_x = math.isqrt(chips)
    side_x = side_x if side_x * side_x == chips else chips // 2
    side_y = chips // side_x
    order = [x for x in range(side_x)]
    for y in range(1, side_y):
        xs = range(side_x - 1, 0, -1) if y % 2 else range(1, side_x)
        order += [y * side_x + x for x in xs]
    order += [y * side_x for y in range(side_y - 1, 0, -1)]
    return order


def pick(table, index):
    value = jnp.int32(table[0])
    for i in range(1, len(table)):
        value = jnp.where(index == i, jnp.int32(table[i]), value)
    return value


def remote(src, dst, send, recv, device):
    return pltpu.make_async_remote_copy(
        src_ref=src,
        dst_ref=dst,
        send_sem=send,
        recv_sem=recv,
        device_id={"tp": device},
        device_id_type=MESH,
    )


def greet(devices):
    barrier = pltpu.get_barrier_semaphore()
    for device in devices:
        pl.semaphore_signal(barrier, inc=1, device_id={"tp": device}, device_id_type=MESH)
    pl.semaphore_wait(barrier, len(devices))


def gather_kernel(count, chips, *refs):
    own, out = refs[:count], refs[count : 2 * count]
    ring_send, ring_recv, core_send, core_recv, keep = refs[2 * count :]
    order = ring_order(chips)
    place = [order.index(chip) for chip in range(chips)]
    me = lax.axis_index("tp")
    chip, core = me // 2, me % 2
    spot = pick(place, chip)
    partner = chip * 2 + 1 - core
    steps = chips // 2
    rows = own[0].shape[0]
    half = rows // 2

    def at(offset):
        return pick(order, (spot + offset + chips) % chips) * 2 + core

    right, left = at(1), at(-1)
    greet([right, left, partner])

    def part(ref, way, step):
        if step < steps - 1:
            return ref
        return ref.at[pl.ds(way * half, half)]

    def hop(k, way, step):
        index = at(-step if way == 0 else step)
        source = own[k] if step == 0 else out[k].at[index]
        return remote(
            part(source, way, step),
            part(out[k].at[index], way, step),
            ring_send.at[k, way, step],
            ring_recv.at[k, way, step],
            right if way == 0 else left,
        )

    def arrived(k, way, step):
        index = at(-(step + 1) if way == 0 else step + 1)
        block = part(out[k].at[index], way, step)
        return remote(
            block, block, ring_send.at[k, way, step], ring_recv.at[k, way, step], right if way == 0 else left
        ), remote(
            block, block, core_send.at[k, way, step], core_recv.at[k, way, step], partner
        )

    def own_pass(k):
        return remote(
            own[k], out[k].at[me], core_send.at[k, 2, 0], core_recv.at[k, 2, 0], partner
        )

    def own_keep(k):
        return pltpu.make_async_copy(own[k], out[k].at[me], keep.at[k])

    for k in range(count):
        for way in range(2):
            hop(k, way, 0).start()
    for k in range(count):
        own_pass(k).start()
        own_keep(k).start()
    for step in range(steps):
        for k in range(count):
            for way in range(2):
                landed, handed = arrived(k, way, step)
                landed.wait_recv()
                if step + 1 < steps:
                    hop(k, way, step + 1).start()
                handed.start()
    for k in range(count):
        own_keep(k).wait()
        own_pass(k).wait_send()
        other = remote(
            own[k], out[k].at[partner], core_send.at[k, 2, 0], core_recv.at[k, 2, 0], partner
        )
        other.wait_recv()
        for way in range(2):
            for step in range(steps):
                hop(k, way, step).wait_send()
                handed = arrived(k, way, step)[1]
                handed.wait_send()
                index = at(-(step + 1) if way == 0 else step + 1) // 2 * 2 + 1 - core
                block = part(out[k].at[index], way, step)
                remote(
                    block, block, core_send.at[k, way, step], core_recv.at[k, way, step], partner
                ).wait_recv()


def gather(arrays, ident):
    size = lax.axis_size("tp")
    chips, count = size // 2, len(arrays)
    ring = pltpu.SemaphoreType.DMA((count, 2, chips // 2))
    cores = pltpu.SemaphoreType.DMA((count, 3, chips // 2))
    return pl.pallas_call(
        functools.partial(gather_kernel, count, chips),
        out_shape=[jax.ShapeDtypeStruct((size,) + a.shape, a.dtype) for a in arrays],
        in_specs=[pl.BlockSpec(memory_space=pltpu.VMEM)] * count,
        out_specs=[pl.BlockSpec(memory_space=pl.ANY)] * count,
        scratch_shapes=[ring, ring, cores, cores, pltpu.SemaphoreType.DMA((count,))],
        compiler_params=pltpu.CompilerParams(collective_id=ident, has_side_effects=True),
        name=f"gather_{ident}",
    )(*arrays)


def reduce_kernel(count, chips, *refs):
    part, out = refs[:count], refs[count : 2 * count]
    pre, stage, got = refs[2 * count : 5 * count : 3], refs[2 * count + 1 : 5 * count : 3], refs[2 * count + 2 : 5 * count : 3]
    core_send, core_recv, chip_send, chip_recv = refs[5 * count :]
    me = lax.axis_index("tp")
    chip, core = me // 2, me % 2
    partner = chip * 2 + 1 - core
    away = [(chip + o) % chips for o in range(1, chips)]
    greet([partner] + [other * 2 + core for other in away])

    def swap(k):
        return remote(part[k].at[1 - core], pre[k], core_send.at[k], core_recv.at[k], partner)

    def ship(k, o):
        return remote(
            stage[k].at[away[o]], got[k].at[o], chip_send.at[k, o], chip_recv.at[k, o], away[o] * 2 + core
        )

    for k in range(count):
        swap(k).start()
    for k in range(count):
        swap(k).wait()

        def add(q, _):
            stage[k][q] = (
                part[k][core, q].astype(jnp.float32) + pre[k][q].astype(jnp.float32)
            ).astype(BF)
            return 0

        lax.fori_loop(0, chips, add, 0)
        for o in range(chips - 1):
            ship(k, o).start()
    for k in range(count):
        for o in range(chips - 1):
            ship(k, o).wait()
        total = stage[k][chip].astype(jnp.float32)
        for o in range(chips - 1):
            total = total + got[k][o].astype(jnp.float32)
        out[k][...] = total.astype(BF)


def reduce_pieces(partials, ident):
    size = lax.axis_size("tp")
    chips, count = size // 2, len(partials)
    rows, width = partials[0].shape[0], partials[0].shape[1] // size
    cut = [p.reshape(rows, chips, 2, width).transpose(2, 1, 0, 3) for p in partials]
    held = pltpu.VMEM((chips, rows, width), BF)
    got = pltpu.VMEM((chips - 1, rows, width), BF)
    return pl.pallas_call(
        functools.partial(reduce_kernel, count, chips),
        out_shape=[jax.ShapeDtypeStruct((rows, width), BF)] * count,
        in_specs=[pl.BlockSpec(memory_space=pltpu.VMEM)] * count,
        out_specs=[pl.BlockSpec(memory_space=pltpu.VMEM)] * count,
        scratch_shapes=[held, held, got] * count
        + [pltpu.SemaphoreType.DMA((count,))] * 2
        + [pltpu.SemaphoreType.DMA((count, chips - 1))] * 2,
        compiler_params=pltpu.CompilerParams(
            collective_id=ident, has_side_effects=True, vmem_limit_bytes=48 << 20
        ),
        name=f"reduce_{ident}",
    )(*cut)


def rows_kernel(x_ref, g_ref, o_ref):
    o_ref[...] = jnp.dot(x_ref[...], g_ref[0], preferred_element_type=jnp.float32).astype(BF)


def row_grads(x_turned, blocks):
    features, rows = x_turned.shape
    size, _, hidden = blocks.shape
    return pl.pallas_call(
        rows_kernel,
        grid=(size,),
        out_shape=jax.ShapeDtypeStruct((features, size * hidden), BF),
        in_specs=[
            pl.BlockSpec((features, rows), lambda n: (0, 0)),
            pl.BlockSpec((1, rows, hidden), lambda n: (n, 0, 0)),
        ],
        out_specs=pl.BlockSpec((features, hidden), lambda n: (0, n)),
        name="row_grads",
        cost_estimate=pl.CostEstimate(
            flops=2 * features * rows * size * hidden,
            bytes_accessed=2 * size * hidden * (rows + features),
            transcendentals=0,
        ),
    )(x_turned, blocks)


def side_by_side(blocks):
    size, rows, width = blocks.shape
    return blocks.transpose(1, 0, 2).reshape(rows, size * width)


def silu_parts(gate_pre):
    sigma = jax.nn.sigmoid(gate_pre)
    return (gate_pre * sigma, sigma * (1.0 + gate_pre * (1.0 - sigma)))


def contract_rows(left, right):
    return lax.dot_general(
        left, right, (((0,), (0,)), ((), ())), preferred_element_type=jnp.float32
    )


def contract_cols(left, right):
    return lax.dot_general(
        left, right, (((1,), (1,)), ((), ())), preferred_element_type=jnp.float32
    )


def general_body(tokens, cotangent, expert_ids, combine_weights, w_gate, w_up, w_down):
    groups = lax.axis_size("ep")
    tok_rows, piece_width = tokens.shape
    chosen = expert_ids.shape[1]
    capacity = tok_rows * chosen * 5 // (3 * groups)
    buffer_rows = groups * capacity
    gate_weight = w_gate[0]
    up_weight = w_up[0]
    down_weight = w_down[0]
    flat_ids = expert_ids.reshape(-1)
    onehot = (flat_ids[:, None] == jnp.arange(groups, dtype=jnp.int32)[None, :]).astype(jnp.int32)
    rank = jnp.sum((jnp.cumsum(onehot, axis=0) - onehot) * onehot, axis=1)
    slot_index = flat_ids * capacity + rank
    places = (jnp.arange(buffer_rows, dtype=jnp.int32)[:, None] == slot_index[None, :]).astype(
        jnp.bfloat16
    )
    placer = jnp.sum(
        places.reshape(buffer_rows, tok_rows, chosen).astype(jnp.float32), axis=2
    ).astype(jnp.bfloat16)
    scaled = (combine_weights[:, :, None] * cotangent[:, None, :].astype(jnp.float32)).astype(
        jnp.bfloat16
    )
    send_grad = jnp.dot(
        places, scaled.reshape(tok_rows * chosen, piece_width), preferred_element_type=jnp.float32
    ).astype(jnp.bfloat16)
    send_rows = jnp.dot(placer, tokens, preferred_element_type=jnp.float32).astype(jnp.bfloat16)
    recv_rows, recv_grad = (
        lax.all_to_all(
            send_rows.reshape(groups, capacity, piece_width),
            "ep",
            split_axis=0,
            concat_axis=0,
            tiled=True,
        ),
        lax.all_to_all(
            send_grad.reshape(groups, capacity, piece_width),
            "ep",
            split_axis=0,
            concat_axis=0,
            tiled=True,
        ),
    )
    recv_rows = recv_rows.reshape(buffer_rows, piece_width)
    recv_grad = recv_grad.reshape(buffer_rows, piece_width)
    x_blocks, dy_blocks = gather([recv_rows, recv_grad], 0)
    piece, dy_full = side_by_side(x_blocks), side_by_side(dy_blocks)
    gate_pre = jnp.dot(piece, gate_weight, preferred_element_type=jnp.float32)
    up_pre = jnp.dot(piece, up_weight, preferred_element_type=jnp.float32)
    active, slope = silu_parts(gate_pre)
    hidden = (active * up_pre).astype(jnp.bfloat16)
    partial_value = jnp.dot(hidden, down_weight, preferred_element_type=jnp.float32)
    grad_hidden = contract_cols(dy_full, down_weight)
    grad_gate_pre = (grad_hidden * up_pre * slope).astype(jnp.bfloat16)
    grad_up_pre = (grad_hidden * active).astype(jnp.bfloat16)
    input_partial = contract_cols(grad_gate_pre, gate_weight) + contract_cols(
        grad_up_pre, up_weight
    )
    out_piece, input_piece = reduce_pieces(
        [partial_value.astype(jnp.bfloat16), input_partial.astype(jnp.bfloat16)], 1
    )
    hidden_in, gate_in, up_in, out_piece, input_piece = lax.optimization_barrier(
        (hidden, grad_gate_pre, grad_up_pre, out_piece, input_piece)
    )
    hidden_blocks, gate_blocks, up_blocks = gather([hidden_in, gate_in, up_in], 2)
    out_back = lax.all_to_all(
        out_piece.reshape(groups, capacity, piece_width),
        "ep",
        split_axis=0,
        concat_axis=0,
        tiled=True,
    ).reshape(buffer_rows, piece_width)
    out_tokens = (
        jnp.take(out_back, slot_index, axis=0)
        .reshape(tok_rows, chosen, piece_width)
        .astype(jnp.float32)
    )
    mixed = jnp.sum(combine_weights[:, :, None] * out_tokens, axis=1).astype(jnp.bfloat16)
    local_products = jnp.sum(cotangent.astype(jnp.float32)[:, None, :] * out_tokens, axis=2)
    grad_combine = lax.psum(local_products, "tp")
    input_back = lax.all_to_all(
        input_piece.reshape(groups, capacity, piece_width),
        "ep",
        split_axis=0,
        concat_axis=0,
        tiled=True,
    ).reshape(buffer_rows, piece_width)
    grad_tokens = jnp.sum(
        jnp.take(input_back, slot_index, axis=0)
        .reshape(tok_rows, chosen, piece_width)
        .astype(jnp.float32),
        axis=1,
    ).astype(jnp.bfloat16)
    down_cols_out = (
        jnp.einsum("nrh,rd->nhd", hidden_blocks, recv_grad, preferred_element_type=jnp.float32)
        .astype(jnp.bfloat16)
        .reshape(-1, piece_width)
    )
    x_turned = recv_rows.T
    gate_rows_out = row_grads(x_turned, gate_blocks)
    up_rows_out = row_grads(x_turned, up_blocks)
    return (
        mixed,
        grad_tokens,
        grad_combine,
        gate_rows_out[None],
        up_rows_out[None],
        down_cols_out[None],
    )


CHUNK = 256
LANES = 128


def fast_form(tokens, expert_ids, w_gate):
    groups, size = lax.axis_size("ep"), lax.axis_size("tp")
    tok_rows, width = tokens.shape
    hidden = w_gate.shape[2]
    capacity = tok_rows * expert_ids.shape[1] * 5 // (3 * groups)
    return (
        size == 8
        and expert_ids.shape[1] == 2
        and 3 <= groups <= 8
        and width % LANES == 0
        and hidden % CHUNK == 0
        and capacity % 16 == 0
        and capacity <= LANES
        and groups * capacity % 32 == 0
        and tok_rows <= LANES
        and tok_rows % 16 == 0
    )


def far_copy(src, dst, send, recv, device):
    return pltpu.make_async_remote_copy(
        src_ref=src, dst_ref=dst, send_sem=send, recv_sem=recv, device_id=device, device_id_type=MESH
    )


def layer_kernel(
    chips,
    groups,
    capacity,
    ids_hbm,
    weights_hbm,
    tokens_hbm,
    cotangent_hbm,
    wg_hbm,
    wu_hbm,
    wd_hbm,
    gate_buf,
    up_buf,
    down_buf,
    mixed,
    grad_tokens,
    grad_combine,
    blocks,
    both,
    out_rows,
    dy_rows,
    cots,
    factors,
    part,
    pre,
    stage,
    back,
    ready,
    got,
    turned,
    inner_sum,
    inner_out,
    inner_in,
    products,
    table,
    ids_t,
    weights_t,
    tokens,
    cotangent,
    in_sem,
    w_sem,
    z_recv,
    x_side,
    x_far,
    x_pass,
    a_side,
    a_far,
    a_own,
    a_pass,
    s_recv,
    recv,
    send,
):
    size = 2 * chips
    tok_rows, width = tokens.shape
    rows = groups * capacity
    model = size * width
    hidden = wg_hbm.shape[1]
    chunks = hidden // CHUNK
    wide = 2 * width
    order = ring_order(chips)
    place = [order.index(chip) for chip in range(chips)]
    me = lax.axis_index("tp")
    group = lax.axis_index("ep")
    chip, core = me // 2, me % 2
    spot = pick(place, chip)
    partner = chip * 2 + 1 - core

    def at(offset):
        return pick(order, (spot + offset + chips) % chips) * 2 + core

    right, left, across = at(1), at(-1), at(2)
    sides = (right, left)

    def other(device):
        return device // 2 * 2 + 1 - core

    near = [sorted(range(groups), key=lambda s: (abs(s - g), s)) for g in range(groups)]
    planes = [pick([near[g][k] for g in range(groups)], group) for k in range(groups)]

    def rows_of(s):
        return pl.ds(pl.multiple_of(s * capacity, 16), capacity)

    def cols_of(device):
        return pl.ds(pl.multiple_of(device * width, LANES), width)

    def take(block, sem, device):
        far_copy(block, block, send.at[0], sem, device).wait_recv()

    barrier = pltpu.get_barrier_semaphore()
    for k in range(1, groups):
        pl.semaphore_signal(barrier, inc=1, device_id={"ep": planes[k]}, device_id_type=MESH)
    for d in range(1, size):
        pl.semaphore_signal(barrier, inc=1, device_id={"tp": (me + d) % size}, device_id_type=MESH)

    inputs = (
        (ids_hbm, ids_t),
        (weights_hbm, weights_t),
        (tokens_hbm, tokens),
        (cotangent_hbm, cotangent),
    )
    inputs = [pltpu.make_async_copy(a, b, in_sem.at[n]) for n, (a, b) in enumerate(inputs)]
    for copy in inputs:
        copy.start()
    for copy in inputs:
        copy.wait()
    row_id = lax.broadcasted_iota(jnp.int32, (8, tok_rows), 0)
    member_t = jnp.where((ids_t[0:1, :] == row_id) | (ids_t[1:2, :] == row_id), 1.0, 0.0)
    first = lax.broadcasted_iota(jnp.int32, (tok_rows, tok_rows), 0)
    second = lax.broadcasted_iota(jnp.int32, (tok_rows, tok_rows), 1)
    before_t = jnp.dot(
        member_t.astype(BF),
        jnp.where(first < second, 1.0, 0.0).astype(BF),
        preferred_element_type=jnp.float32,
    )
    table[...] = jnp.zeros((LANES, LANES), jnp.float32)
    table[0:2, 0:tok_rows] = ids_t[...].astype(jnp.float32)
    table[2:4, 0:tok_rows] = weights_t[...]
    columns = jnp.transpose(table[...])[0:tok_rows, :]
    choice = (columns[:, 0:1], columns[:, 1:2])
    weight = (columns[:, 2:3], columns[:, 3:4])
    slot_t = lax.broadcasted_iota(jnp.int32, (capacity, tok_rows), 0).astype(jnp.float32)
    for p in range(groups):
        placer = (
            jnp.where(slot_t == before_t[p : p + 1, :], 1.0, 0.0) * member_t[p : p + 1, :]
        ).astype(BF)
        out_rows[p] = jnp.dot(placer, tokens[...], preferred_element_type=jnp.float32).astype(BF)

    pl.semaphore_wait(barrier, size + groups - 2)


    for k in range(groups - 1, 0, -1):
        far_copy(
            out_rows.at[planes[k]],
            both.at[0, rows_of(group), cols_of(me)],
            send.at[0],
            z_recv.at[0, group],
            {"ep": planes[k]},
        ).start()
    for target in (across, right, left):
        far_copy(cotangent, cots.at[chip], send.at[8], recv.at[4], {"tp": target}).start()
    cots[chip] = cotangent[...]

    def x_block(a, k, device):
        return both.at[a, rows_of(planes[k]), cols_of(device)]

    def x_send(a, k, device, sem, target):
        block = x_block(a, k, device)
        far_copy(block, block, send.at[1], sem, {"tp": target}).start()

    def side_of(k):
        return 0 if k < 2 else 2

    def x_first(k):
        if k == 0:
            both[0, rows_of(group), cols_of(me)] = out_rows[group]
        else:
            take(x_block(0, k, me), z_recv.at[0, planes[k]], {"ep": planes[k]})
        for way in range(2):
            x_send(0, k, me, x_side.at[way, k], sides[way])
        if k > 0:
            x_send(0, k, me, x_far.at[k], across)
        x_send(0, k, me, x_pass.at[side_of(k)], partner)

    def x_relay(k):
        for way in range(2):
            origin = sides[1 - way]
            take(x_block(0, k, origin), x_side.at[way, k], {"tp": origin})
            if k == 0 and way == 0:
                x_send(0, k, origin, x_far.at[k], sides[way])
            x_send(0, k, origin, x_pass.at[side_of(k)], partner)

    def x_last(k):
        take(x_block(0, k, across), x_far.at[k], {"tp": across})
        x_send(0, k, across, x_pass.at[side_of(k)], partner)

    def dy_pass(k):
        for q in range(chips):
            x_send(1, k, q * 2 + core, x_pass.at[1], partner)

    def dy_first():
        take(cots.at[pl.ds(0, chips - 1)], recv.at[4], {"tp": across})
        for p in range(groups):
            placer = (
                jnp.where(slot_t == before_t[p : p + 1, :], 1.0, 0.0) * member_t[p : p + 1, :]
            ).astype(BF)
            own_weight = jnp.where(choice[0] == p, weight[0], 0.0) + jnp.where(
                choice[1] == p, weight[1], 0.0
            )
            for q in range(chips):
                scaled = (own_weight * cots[q].astype(jnp.float32)).astype(BF)
                dy_rows[p, q] = jnp.dot(placer, scaled, preferred_element_type=jnp.float32).astype(BF)
        for k in range(1, groups):
            for q in range(chips):
                far_copy(
                    dy_rows.at[planes[k], q],
                    both.at[1, rows_of(group), cols_of(q * 2 + core)],
                    send.at[9],
                    z_recv.at[1, group],
                    {"ep": planes[k]},
                ).start()
        for q in range(chips):
            both[1, rows_of(group), cols_of(q * 2 + core)] = dy_rows[group, q]
        dy_pass(0)

    def dy_next(k):
        take(
            both.at[1, rows_of(planes[k]), pl.ds(0, chips * width)],
            z_recv.at[1, planes[k]],
            {"ep": planes[k]},
        )
        dy_pass(k)

    def x_whole(a, n, count):
        block = both.at[a, pl.ds(0, count * capacity), pl.ds(0, chips * width)]
        take(block, x_pass.at[n], {"tp": partner})

    def fetch(n):
        source, target = ((wg_hbm, gate_buf), (wu_hbm, up_buf), (wd_hbm, down_buf))[n]
        if n < 2:
            for c in range(chunks):
                pltpu.make_async_copy(
                    source.at[:, pl.ds(c * CHUNK, CHUNK)],
                    target.at[pl.ds(c * model, model), :],
                    w_sem.at[n],
                ).start()
        else:
            for q in range(chips):
                pltpu.make_async_copy(
                    source.at[:, pl.ds(q * wide, wide)],
                    target.at[pl.ds(q * hidden, hidden), :],
                    w_sem.at[n],
                ).start()

    def fetched(n):
        target = (gate_buf, up_buf, down_buf)[n]
        pltpu.make_async_copy(target, target, w_sem.at[n]).wait()

    x_first(0)
    for n in range(3):
        fetch(n)
    x_relay(0)
    x_first(1)
    x_last(0)
    dy_first()
    x_first(2)
    x_relay(1)
    x_last(1)
    for k in range(3, groups):
        x_first(k)
    x_whole(0, 0, 2)
    for n in range(3):
        fetched(n)

    half = rows // 2
    kinds = ((0, 1), (1, 2))

    def a_block(b, c, device, way=None):
        start, count = kinds[b]
        if way is None:
            return blocks.at[device, c, pl.ds(start, count)]
        return blocks.at[device, c, pl.ds(start, count), pl.ds(way * half, half), :]

    def a_send(b, c, device, sem, target, way=None):
        block = a_block(b, c, device, way)
        far_copy(block, block, send.at[2], sem, {"tp": target}).start()

    def a_first(b, c):
        for way in range(2):
            a_send(b, c, me, a_side.at[b, way, c], sides[way])
        a_send(b, c, me, a_own.at[b], partner)

    def a_relay(b, c):
        for way in range(2):
            origin = sides[1 - way]
            take(a_block(b, c, origin), a_side.at[b, way, c], {"tp": origin})
            a_send(b, c, origin, a_far.at[b, c], sides[way], way)
            a_send(b, c, origin, a_pass.at[b, 0, c], partner)

    def a_relayed(b, c):
        start, count = kinds[b]
        take(blocks.at[pl.ds(0, 2), c, pl.ds(start, count)], a_pass.at[b, 0, c], {"tp": partner})

    def a_last(b, c):
        take(a_block(b, c, across), a_far.at[b, c], {"tp": left})
        a_send(b, c, across, a_pass.at[b, 1, c], partner)

    def a_lasted(b, c):
        take(a_block(b, c, other(across)), a_pass.at[b, 1, c], {"tp": partner})

    def hidden_rows(c, k):
        spread = pl.ds(c * model, model)
        cut = rows_of(planes[k])
        held = both[0, cut, :]
        gate_pre = jnp.dot(held, gate_buf[spread, :], preferred_element_type=jnp.float32)
        up_pre = jnp.dot(held, up_buf[spread, :], preferred_element_type=jnp.float32)
        active, slope = silu_parts(gate_pre)
        blocks[me, c, 0, cut, :] = (active * up_pre).astype(BF)
        block = blocks.at[me, c, pl.ds(0, 1), cut, :]
        for way in range(2):
            far_copy(block, block, send.at[2], a_side.at[0, way, c], {"tp": sides[way]}).start()
        far_copy(block, block, send.at[2], a_own.at[0], {"tp": partner}).start()
        factors[0, c, cut, :] = up_pre * slope
        factors[1, c, cut, :] = active

    turns = [2, 1, chips - 1, 0]

    def swap(a, o, value):
        part[a, 0, o] = value[:, :width].astype(BF)
        part[a, 1, o] = value[:, width:].astype(BF)
        far_copy(
            part.at[a, 1 - core, o], pre.at[a, o], send.at[3], s_recv.at[a, o], {"tp": partner}
        ).start()

    def out_part(o, _):
        q = pick(order, (spot + pick(turns, o)) % chips)
        value = None
        for c in range(chunks):
            cut = pl.ds(pl.multiple_of(q * hidden + c * CHUNK, CHUNK), CHUNK)
            term = jnp.dot(blocks[me, c, 0], down_buf[cut, :], preferred_element_type=jnp.float32)
            value = term if c == 0 else value + term
        swap(0, o, value)
        return 0

    def in_part(o, _):
        q = pick(order, (spot + pick(turns, o)) % chips)
        value = None
        for c in range(chunks):
            cut = pl.ds(pl.multiple_of(c * model + q * wide, LANES), wide)
            term = contract_cols(blocks[me, c, 1], gate_buf[cut, :]) + contract_cols(
                blocks[me, c, 2], up_buf[cut, :]
            )
            value = term if c == 0 else value + term
        swap(1, o, value)
        return 0

    def spread_parts(a):
        for o in range(chips):
            take(pre.at[a, o], s_recv.at[a, o], {"tp": partner})

            def add(s, _):
                cut = rows_of(s)
                stage[a, o, cut, :] = (
                    part[a, core, o, cut, :].astype(jnp.float32) + pre[a, o, cut, :].astype(jnp.float32)
                ).astype(BF)
                return 0

            lax.fori_loop(0, groups, add, 0)
            for k in range(groups - 1, 0, -1):
                far_copy(
                    stage.at[a, o, rows_of(planes[k]), :],
                    back.at[a, rows_of(group), pl.ds(o * width, width)],
                    send.at[4],
                    recv.at[0],
                    {"ep": planes[k]},
                ).start()
            back[a, rows_of(group), o * width : (o + 1) * width] = stage[a, o, rows_of(group), :]

    rest = [(x_relay, k) for k in range(2, groups)] + [(x_last, k) for k in range(2, groups)]
    done = 0
    for c in range(chunks):
        for k in range(2):
            hidden_rows(c, k)
        upto = len(rest) * (c + 1) // chunks
        for step, k in rest[done:upto]:
            step(k)
        done = upto
    x_whole(0, 2, groups - 2)
    for c in range(chunks):
        for k in range(2, groups):
            hidden_rows(c, k)
    lax.fori_loop(0, chips, out_part, 0)
    a_relay(0, 0)
    for k in range(1, groups):
        if k < chunks - 1:
            a_relay(0, k)
        dy_next(k)
    x_whole(1, 1, groups)
    spread_parts(0)
    inner_sum[...] = jnp.zeros((rows, LANES), jnp.float32)

    def grad_chunk(c, _):
        grad_hidden = None
        for q in range(chips):
            cut = pl.ds(pl.multiple_of(q * hidden + c * CHUNK, CHUNK), CHUNK)
            term = contract_cols(both[1, :, q * wide : (q + 1) * wide], down_buf[cut, :])
            grad_hidden = term if q == 0 else grad_hidden + term
        blocks[me, c, 1] = (grad_hidden * factors[0, c]).astype(BF)
        blocks[me, c, 2] = (grad_hidden * factors[1, c]).astype(BF)
        a_first(1, c)
        product = blocks[me, c, 0].astype(jnp.float32) * grad_hidden
        total = inner_sum[...]
        for n in range(CHUNK // LANES):
            total = total + product[:, n * LANES : (n + 1) * LANES]
        inner_sum[...] = total
        return 0

    lax.fori_loop(0, chunks, grad_chunk, 0)
    for c in range(max(1, min(groups, chunks - 1)), chunks):
        a_relay(0, c)

    lax.fori_loop(0, chips, in_part, 0)
    spread_parts(1)

    for p in range(groups):
        value = inner_sum[p * capacity : (p + 1) * capacity, :]
        if capacity < LANES:
            value = jnp.concatenate(
                [value, jnp.zeros((LANES - capacity, LANES), jnp.float32)], axis=0
            )
        value = jnp.sum(jnp.transpose(value), axis=0, keepdims=True)
        inner_out[p] = jnp.broadcast_to(value, (8, LANES))
    for k in range(1, groups):
        far_copy(
            inner_out.at[planes[k]], inner_in.at[group], send.at[5], recv.at[1], {"ep": planes[k]}
        ).start()
    inner_in[group] = inner_out[group]

    turned[...] = jnp.transpose(both[0, :, cols_of(me)].astype(jnp.float32)).astype(BF)

    def down_grads(device, c):
        place_of = device * chunks + c
        down_buf[
            pl.ds(pl.multiple_of(place_of // 2 * CHUNK, CHUNK), CHUNK),
            pl.ds(pl.multiple_of(place_of % 2 * width, LANES), width),
        ] = contract_rows(blocks[device, c, 0], both[1, :, cols_of(me)]).astype(BF)

    def side_grads(device, c):
        spread = pl.ds(pl.multiple_of((device * chunks + c) * width, LANES), width)
        gate_buf[spread, :] = jnp.dot(
            turned[...], blocks[device, c, 1], preferred_element_type=jnp.float32
        ).astype(BF)
        up_buf[spread, :] = jnp.dot(
            turned[...], blocks[device, c, 2], preferred_element_type=jnp.float32
        ).astype(BF)

    def grads_for(b, found):
        devices, chunk = [d for d, _ in found], [c for _, c in found]

        def step(n, _):
            (down_grads, side_grads)[b](pick(devices, n), pick(chunk, n))
            return 0

        lax.fori_loop(0, len(found), step, 0)

    def relays(b):
        for c in range(chunks):
            a_relay(b, c)
            found = [(left, c), (right, c)]
            if c > 0:
                a_relayed(b, c - 1)
                found += [(other(left), c - 1), (other(right), c - 1)]
            grads_for(b, found)
        a_relayed(b, chunks - 1)
        grads_for(b, [(other(left), chunks - 1), (other(right), chunks - 1)])

    take(blocks.at[partner, :, pl.ds(0, 1)], a_own.at[0], {"tp": partner})
    take(blocks.at[partner, :, pl.ds(1, 2)], a_own.at[1], {"tp": partner})
    for b in range(2):
        grads_for(b, [(d, c) for c in range(chunks) for d in (me, partner)])
    for c in range(chunks):
        a_relayed(0, c)
    grads_for(0, [(d, c) for c in range(chunks) for d in (left, right, other(left), other(right))])
    relays(1)

    def across_grads(b, first, end):
        for c in range(first, end):
            a_last(b, c)
            found = [(across, c)]
            if c > 0:
                a_lasted(b, c - 1)
                found.append((other(across), c - 1))
            grads_for(b, found)
        if end == chunks:
            a_lasted(b, chunks - 1)
            grads_for(b, [(other(across), chunks - 1)])

    across_grads(0, 0, chunks)
    across_grads(1, 0, max(0, chunks - 2))

    take(inner_in.at[pl.ds(0, groups - 1)], recv.at[1], {"ep": planes[1]})
    lane = lax.broadcasted_iota(jnp.int32, (tok_rows, LANES), 1)
    lane_value = lane.astype(jnp.float32)
    columns = jnp.transpose(table[...])[0:tok_rows, :]
    choice = (columns[:, 0:1], columns[:, 1:2])
    weight = (columns[:, 2:3], columns[:, 3:4])
    member = jnp.where((choice[0] == lane_value) | (choice[1] == lane_value), 1.0, 0.0)
    first = lax.broadcasted_iota(jnp.int32, (tok_rows, tok_rows), 0)
    second = lax.broadcasted_iota(jnp.int32, (tok_rows, tok_rows), 1)
    before = jnp.dot(
        jnp.where(second < first, 1.0, 0.0).astype(BF),
        member.astype(BF),
        preferred_element_type=jnp.float32,
    )
    inner = jnp.zeros((tok_rows, LANES), jnp.float32)
    takers = []
    slot = lax.broadcasted_iota(jnp.int32, (tok_rows, rows), 1).astype(jnp.float32)
    for k in range(2):
        rank = jnp.sum(jnp.where(lane_value == choice[k], before, 0.0), axis=1, keepdims=True)
        takers.append(jnp.where(slot == choice[k] * capacity + rank, 1.0, 0.0).astype(BF))
        value = jnp.zeros((tok_rows, LANES), jnp.float32)
        for p in range(groups):
            value = value + jnp.where((lane_value == rank) & (choice[k] == p), inner_in[p][0:1, :], 0.0)
        value = jnp.sum(value, axis=1, keepdims=True) / weight[k]
        inner = inner + jnp.where(lane == k, value, 0.0)
    if tok_rows < LANES:
        inner = jnp.concatenate([inner, jnp.zeros((LANES - tok_rows, LANES), jnp.float32)], axis=0)
    products[me] = jnp.transpose(inner)[0:8, :]
    for d in range(1, size):
        far_copy(
            products.at[me], products.at[me], send.at[6], recv.at[2], {"tp": (me + d) % size}
        ).start()

    take(back.at[:, pl.ds(0, rows - capacity), :], recv.at[0], {"ep": planes[1]})
    for n in range(chips // 2):
        cut = slice(n * wide, (n + 1) * wide)
        mix = weight[0] * jnp.dot(takers[0], back[0, :, cut], preferred_element_type=jnp.float32)
        mix = mix + weight[1] * jnp.dot(
            takers[1], back[0, :, cut], preferred_element_type=jnp.float32
        )
        grads = jnp.dot(takers[0] + takers[1], back[1, :, cut], preferred_element_type=jnp.float32)
        for j in range(2):
            o = 2 * n + j
            ready[o, 0] = mix[:, j * width : (j + 1) * width].astype(BF)
            ready[o, 1] = grads[:, j * width : (j + 1) * width].astype(BF)
            if o < chips - 1:
                far_copy(
                    ready.at[o], got.at[o], send.at[7], recv.at[3], {"tp": at(turns[o])}
                ).start()

    across_grads(1, max(0, chunks - 2), chunks)

    take(products.at[pl.ds(0, size - 1)], recv.at[2], {"tp": partner})
    summed = products[0]
    for d in range(1, size):
        summed = summed + products[d]
    grad_combine[...] = summed[0:2, 0:tok_rows]

    take(got, recv.at[3], {"tp": right})
    for a, out in ((0, mixed), (1, grad_tokens)):
        value = ready[chips - 1, a].astype(jnp.float32)
        for o in range(chips - 1):
            value = value + got[o, a].astype(jnp.float32)
        out[...] = value.astype(BF)

    def sent(block, n):
        far_copy(block, block, send.at[n], recv.at[0], {"tp": partner}).wait_send()

    sent(out_rows.at[pl.ds(0, groups - 1)], 0)
    sent(both.at[0, :, pl.ds(0, (chips + 3) * width)], 1)
    sent(both.at[1, :, pl.ds(0, chips * width)], 1)
    sent(cots.at[pl.ds(0, chips - 1)], 8)
    sent(dy_rows.at[pl.ds(0, groups - 1)], 9)
    sent(blocks.at[pl.ds(0, chips + 3)], 2)
    sent(part.at[:, 0], 3)
    sent(back.at[:, pl.ds(0, rows - capacity), :], 4)
    sent(inner_out.at[pl.ds(0, groups - 1)], 5)
    sent(products.at[pl.ds(0, size - 1)], 6)
    sent(ready.at[pl.ds(0, chips - 1)], 7)


def layer(ids_t, weights_t, tokens, cotangent, w_gate, w_up, w_down, capacity):
    size, groups = lax.axis_size("tp"), lax.axis_size("ep")
    chips = size // 2
    tok_rows, width = tokens.shape
    model, hidden = w_gate.shape
    chunks = hidden // CHUNK
    rows = groups * capacity
    whole, any_place = pl.BlockSpec(memory_space=pltpu.VMEM), pl.BlockSpec(memory_space=pl.ANY)
    dma = pltpu.SemaphoreType.DMA
    return pl.pallas_call(
        functools.partial(layer_kernel, chips, groups, capacity),
        out_shape=[
            pltpu.VMEM((chunks * model, CHUNK), BF),
            pltpu.VMEM((chunks * model, CHUNK), BF),
            pltpu.VMEM((chips * hidden, 2 * width), BF),
            pltpu.VMEM((tok_rows, width), BF),
            pltpu.VMEM((tok_rows, width), BF),
            pltpu.VMEM((2, tok_rows), jnp.float32),
        ],
        in_specs=[any_place] * 7,
        out_specs=[whole] * 6,
        scratch_shapes=[
            pltpu.VMEM((size, chunks, 3, rows, CHUNK), BF),
            pltpu.VMEM((2, rows, model), BF),
            pltpu.VMEM((groups, capacity, width), BF),
            pltpu.VMEM((groups, chips, capacity, width), BF),
            pltpu.VMEM((chips, tok_rows, width), BF),
            pltpu.VMEM((2, chunks, rows, CHUNK), jnp.float32),
            pltpu.VMEM((2, 2, chips, rows, width), BF),
            pltpu.VMEM((2, chips, rows, width), BF),
            pltpu.VMEM((2, chips, rows, width), BF),
            pltpu.VMEM((2, rows, chips * width), BF),
            pltpu.VMEM((chips, 2, tok_rows, width), BF),
            pltpu.VMEM((chips - 1, 2, tok_rows, width), BF),
            pltpu.VMEM((width, rows), BF),
            pltpu.VMEM((rows, LANES), jnp.float32),
            pltpu.VMEM((groups, 8, LANES), jnp.float32),
            pltpu.VMEM((groups, 8, LANES), jnp.float32),
            pltpu.VMEM((size, 8, LANES), jnp.float32),
            pltpu.VMEM((LANES, LANES), jnp.float32),
            pltpu.VMEM((2, tok_rows), jnp.int32),
            pltpu.VMEM((2, tok_rows), jnp.float32),
            pltpu.VMEM((tok_rows, width), BF),
            pltpu.VMEM((tok_rows, width), BF),
            dma((4,)),
            dma((3,)),
            dma((2, groups)),
            dma((2, groups)),
            dma((groups,)),
            dma((3,)),
            dma((2, 2, chunks)),
            dma((2, chunks)),
            dma((2,)),
            dma((2, 2, chunks)),
            dma((2, chips)),
            dma((5,)),
            dma((10,)),
        ],
        compiler_params=pltpu.CompilerParams(
            collective_id=0, has_side_effects=True, vmem_limit_bytes=44 << 20
        ),
        name="layer",
    )(ids_t, weights_t, tokens, cotangent, w_gate, w_up, w_down)


def place_kernel(gate_buf, up_buf, down_buf, *refs):
    small, (gate, up, down), outs, sems = refs[:3], refs[3:6], refs[6:9], refs[9]
    width = gate.shape[0]
    count = gate.shape[1] // CHUNK
    for n in range(count):
        cut, spread = pl.ds(n * CHUNK, CHUNK), pl.ds(n * width, width)
        pltpu.make_async_copy(gate_buf.at[spread, :], gate.at[:, cut], sems.at[0]).start()
        pltpu.make_async_copy(up_buf.at[spread, :], up.at[:, cut], sems.at[1]).start()
        block = down_buf.at[pl.ds(n // 2 * CHUNK, CHUNK), pl.ds(n % 2 * width, width)]
        pltpu.make_async_copy(block, down.at[cut, :], sems.at[2]).start()
    for n in range(3):
        pltpu.make_async_copy(small[n], outs[n], sems.at[3 + n]).start()
    for n in range(3):
        pltpu.make_async_copy(small[n], outs[n], sems.at[3 + n]).wait()
    for n, result in enumerate((gate, up, down)):
        pltpu.make_async_copy(result, result, sems.at[n]).wait()


def place_results(gate_buf, up_buf, down_buf, mixed, grad_tokens, grad_combine):
    tok_rows, width = mixed.shape
    hidden = gate_buf.shape[0] // width * CHUNK
    whole, any_place = pl.BlockSpec(memory_space=pltpu.VMEM), pl.BlockSpec(memory_space=pl.ANY)
    return pl.pallas_call(
        place_kernel,
        out_shape=[
            jax.ShapeDtypeStruct((width, hidden), BF),
            jax.ShapeDtypeStruct((width, hidden), BF),
            jax.ShapeDtypeStruct((hidden, width), BF),
            jax.ShapeDtypeStruct((tok_rows, width), BF),
            jax.ShapeDtypeStruct((tok_rows, width), BF),
            jax.ShapeDtypeStruct((2, tok_rows), jnp.float32),
        ],
        in_specs=[whole] * 6,
        out_specs=[any_place] * 6,
        scratch_shapes=[pltpu.SemaphoreType.DMA((6,))],
        compiler_params=pltpu.CompilerParams(vmem_limit_bytes=4 << 20),
        name="place_results",
    )(gate_buf, up_buf, down_buf, mixed, grad_tokens, grad_combine)


def body(tokens, cotangent, expert_ids, combine_weights, w_gate, w_up, w_down):
    if not fast_form(tokens, expert_ids, w_gate):
        return general_body(tokens, cotangent, expert_ids, combine_weights, w_gate, w_up, w_down)
    tok_rows, chosen = expert_ids.shape
    capacity = tok_rows * chosen * 5 // (3 * lax.axis_size("ep"))
    held = layer(
        expert_ids.T, combine_weights.T, tokens, cotangent, w_gate[0], w_up[0], w_down[0], capacity
    )
    gate, up, down, mixed, grad_tokens, grad_combine = place_results(*held)
    return mixed, grad_tokens, grad_combine.T, gate[None], up[None], down[None]


def solution(mesh):
    placed = (
        P("ep", "tp"),
        P("ep", "tp"),
        P("ep", None),
        P("ep", None),
        P("ep", None, "tp"),
        P("ep", None, "tp"),
        P("ep", "tp", None),
    )
    return jax.shard_map(
        body,
        mesh=mesh,
        in_specs=placed,
        out_specs=(
            P("ep", "tp"),
            P("ep", "tp"),
            P("ep", None),
            P("ep", "tp", None),
            P("ep", "tp", None),
            P("ep", None, "tp"),
        ),
        check_vma=False,
    )
```
